128 devices in a mesh: section: 4 (over z), rows: 32 (over y, x, core).
Axes of the slice: x: 4, y: 4, z: 4, core: 2. Of those that a mesh axis runs over, the one named last changes fastest.
Arguments:
- rows_data: float32 [16, 32768, 128], P('section', 'rows'), may hold values from -6 to 6
- row_keys: int32 [16, 32768], P('section', 'rows'), may hold values from 0 to 8191
- valid_counts: int32 [16, 32], P('section', 'rows'), may hold values from 256 to 1024
- predicates: int32 [4, 16, 1024], P('section', None, 'rows'), may hold values from -2147483648 to 2147483647, as said below
- section_weight: float32 [4, 128, 128], P('section'), may hold values from -0.5 to 0.5
- section_bias: float32 [4, 128], P('section'), may hold values from -3 to 3
Outputs:
- key_means: float32 [8192, 128], P(('section', 'rows'))
- key_counts: float32 [8192], P(('section', 'rows'))
The draws below stay inside these ranges and needn't reach their ends.
Inputs may be any that keep to these rules, and one draw needn't show every extreme that they name: Bit j of predicates[s, m, w] is the flag of row 32 w + j of micro-batch m for section s; about three flags in four are 1. `row_keys`: keys are drawn from a skewed distribution: a few keys are very frequent and most are rare.
All inputs are finite; a program needn't handle non-finite values.
Results may differ from the reference program's by a relative error of at most 0.0001.
Values sent between devices are 32-bit elements; how exact they have to be, the bound alone decides.
A program may use at most 64 MiB of HBM per device.

```python
import math
import jax
import jax.numpy as jnp
import numpy as np
from jax import lax

D = 128
KEYS = 8192
SECTIONS = 4
B_DEV = 1024
MICRO = 16
BROWS = 32768
N_ROWS = 32


def draw_predicates(key, part):
    shape = (SECTIONS, MICRO, BROWS // 32)
    first_key = jax.random.fold_in(key, 11)
    second_key = jax.random.fold_in(key, 23)
    lowest = -2147483647 - 1
    first = jax.random.randint(first_key, shape, lowest, 2147483647, dtype=jnp.int32)
    second = jax.random.randint(second_key, shape, lowest, 2147483647, dtype=jnp.int32)
    return first | second


def set_ends(result, key, least, high):
    index_at = [jax.random.randint(jax.random.fold_in(key, axis), (), 0, length) for axis, length in enumerate(result.shape)]
    widest = result.shape.index(max(result.shape))
    neighbour = index_at[:widest] + [(index_at[widest] + 1) % result.shape[widest]] + index_at[widest + 1:]
    return result.at[tuple(index_at)].set(least).at[tuple(neighbour)].set(high)


def block_scale(rng, extent, cuts, low, largest):
    def one(dim, blocks):
        steps = jax.random.uniform(jax.random.fold_in(jax.random.fold_in(rng, 6), dim), (blocks,), jnp.float32, low / len(cuts), largest / len(cuts))
        return jnp.repeat(jnp.exp(steps), extent[dim] // blocks).reshape((-1,) + (1,) * (len(extent) - dim - 1))

    factor_of = one(*cuts[0])
    for cut in cuts[1:]:
        factor_of = factor_of * one(*cut)
    return factor_of


def cumulative_ranks(count, slope):
    loads = [(1 << 20) // math.isqrt(rank ** slope) + 1 for rank in range(1, count + 1)]
    deviation = 1 + sum(loads) // (1 << 30)
    return np.cumsum(np.array([max(1, weight // deviation) for weight in loads]))


def ranked_ids(stream_key, extent, count, lean):
    table = cumulative_ranks(count, lean)
    ticket = jax.random.randint(jax.random.fold_in(stream_key, 1), extent, 0, int(table[count - 1]))
    rank = jnp.searchsorted(jnp.asarray(table, jnp.int32), ticket, side="right")
    return jax.random.permutation(jax.random.fold_in(stream_key, 2), count)[rank].astype(jnp.int32)


def noise(rng, extent, scale, limit, split=(), kind=jnp.bfloat16):
    entries = jax.random.normal(rng, extent, jnp.float32) * scale
    if len(split) > 0:
        entries = block_scale(rng, extent, split, -0.22, 0.18) * entries
    return jnp.clip(entries, min=-limit, max=limit).astype(kind)


def setup_inputs(seed: int = 0) -> dict:
    key_of = jax.random.split(jax.random.key(seed), 7)
    return {
        "rows_data": noise(key_of[0], (MICRO, BROWS, D), 1.0, 6.0, ((0, 4), (1, 32)), jnp.float32),
        "row_keys": set_ends(ranked_ids(key_of[1], (MICRO, BROWS), KEYS, 2), jax.random.fold_in(key_of[1], 3), 0, KEYS - 1).astype(jnp.int32),
        "valid_counts": set_ends(jax.random.randint(key_of[2], (MICRO, N_ROWS), B_DEV // 4, B_DEV + 1), jax.random.fold_in(key_of[2], 1), B_DEV // 4, B_DEV).astype(jnp.int32),
        "predicates": draw_predicates(jax.random.fold_in(key_of[6], 71), 0),
        "section_weight": noise(key_of[4], (SECTIONS, D, D), D ** -0.5, 0.5, ((0, 4),), jnp.float32),
        "section_bias": noise(key_of[5], (SECTIONS, D), 0.5, 3.0, ((0, 4),), jnp.float32),
    }


def advance(h, weight, bias):
    return h + jnp.tanh(jnp.dot(h, weight, precision=lax.Precision.HIGHEST, preferred_element_type=jnp.float32) + bias)


def unpack_flags(words):
    shifts = lax.broadcasted_iota(jnp.int32, (32,), 0)
    flags = jnp.right_shift(words[..., None], shifts) & 1
    return flags.reshape(words.shape[:-1] + (words.shape[-1] * 32,))


def reference(rows_data, row_keys, valid_counts, predicates, section_weight, section_bias):
    micro = rows_data.shape[0]
    brows = rows_data.shape[1]
    width = rows_data.shape[2]
    position = jnp.arange(brows, dtype=jnp.int32) % B_DEV
    limits = jnp.repeat(valid_counts, B_DEV, axis=1)
    alive = (position[None, :] < limits).reshape(-1)
    hidden = rows_data.reshape(micro * brows, width)
    keys = row_keys.reshape(-1)
    sums = jnp.zeros((KEYS, width), jnp.float32)
    counts = jnp.zeros((KEYS,), jnp.float32)
    for section in range(SECTIONS):
        alive = alive & (unpack_flags(predicates[section]).reshape(-1) == 1)
        hidden = advance(hidden, section_weight[section], section_bias[section])
        sums = sums + jax.ops.segment_sum(jnp.where(alive[:, None], hidden, 0.0), keys, num_segments=KEYS)
        counts = counts + jax.ops.segment_sum(alive.astype(jnp.float32), keys, num_segments=KEYS)
    key_means = sums / jnp.maximum(counts, 1.0)[:, None]
    return key_means, counts
```

```python
import functools

import jax
import jax.numpy as jnp
from jax import lax
from jax.experimental import pallas as pl
from jax.experimental.pallas import tpu as pltpu
from jax.sharding import PartitionSpec as P

KEYS = 8192
SECTIONS = 4
D = 128
MICRO = 4
BLOCK = 1024
ROWS = MICRO * BLOCK
GROUP = 16
STEP = 256
f32, bf16, i32 = jnp.float32, jnp.bfloat16, jnp.int32
MESH = pl.DeviceIdType.MESH
VM, SM, HB = pltpu.VMEM, pltpu.SMEM, pltpu.HBM


def spec(space):
    return pl.BlockSpec(memory_space=space)


def high_low(x):
    high = x.astype(bf16)
    return high, (x - high.astype(f32)).astype(bf16)


def exchange_kernel(w_in, b_in, p_in, keys, valid, w_all, b_all, same, level, counts, words_v, words, send, recv, local):
    me = lax.axis_index("section")
    row = lax.axis_index("rows")
    barrier = pltpu.get_barrier_semaphore()
    for k in range(1, 4):
        pl.semaphore_signal(barrier, inc=1, device_id=(lax.rem(me + k, 4), row), device_id_type=MESH)
    pl.semaphore_wait(barrier, 3)
    copies = []
    for n, k in enumerate((2, 1, 3)):
        to = lax.rem(me + k, 4)
        for a, (src, dst) in enumerate(
            ((p_in.at[to], words_v.at[me]), (b_in.at[0], b_all.at[me]), (w_in.at[0], w_all.at[me]))
        ):
            copies.append((a, pltpu.make_async_remote_copy(
                src_ref=src, dst_ref=dst, send_sem=send.at[n, a], recv_sem=recv.at[n, a],
                device_id=(to, row), device_id_type=MESH)))
    for a in range(3):
        for which, copy in copies:
            if which == a:
                copy.start()
    own = [
        pltpu.make_async_copy(p_in.at[me], words_v.at[me], local.at[0]),
        pltpu.make_async_copy(b_in.at[0], b_all.at[me], local.at[1]),
        pltpu.make_async_copy(w_in.at[0], w_all.at[me], local.at[2]),
    ]
    for copy in own:
        copy.start()
    group_i = (lax.broadcasted_iota(i32, (1, 128), 1) // GROUP) * KEYS

    def sameness(j, carry):
        key_row = keys[pl.ds(j, 1), :] + group_i
        key_col = jnp.transpose(jnp.broadcast_to(key_row, (128, 128)))
        same[j] = jnp.where(key_col == key_row, 1.0, 0.0).astype(bf16)
        return carry

    lax.fori_loop(0, 32, sameness, 0)
    own[0].wait()
    for which, copy in copies:
        if which == 0:
            copy.wait()
    to_scalar = pltpu.make_async_copy(words_v, words, local.at[3])
    to_scalar.start()
    to_scalar.wait()
    counts[...] = jnp.zeros_like(counts)
    lane = lax.broadcasted_iota(i32, (64, 128), 1)
    sub64 = lax.broadcasted_iota(i32, (64, 128), 0)
    sub128 = lax.broadcasted_iota(i32, (128, 128), 0)

    def tally(j, carry):
        m = j // 8
        first = (j % 8) * 4
        nv = valid[m, 0]
        total = jnp.zeros((64, 128), i32)
        alive = []
        for w in range(4):
            n = nv - (first + w) * 32
            alive.append(jnp.where(n >= 32, jnp.int32(-1), (jnp.int32(1) << jnp.clip(n, 0, 31)) - 1))
        for s in range(SECTIONS):
            alive = [a & words[s, m, first + w] for w, a in enumerate(alive)]
            v = jnp.where(lane < 64, jnp.where(lane < 32, alive[0], alive[1]), jnp.where(lane < 96, alive[2], alive[3]))
            total = total + ((v >> (lane & 31)) & 1)
        key_row = keys[pl.ds(j, 1), :]
        high = jnp.where((key_row >> 7) == sub64, total.astype(f32), 0.0).astype(bf16)
        low = jnp.where((key_row & 127) == sub128, 1.0, 0.0).astype(bf16)
        counts[...] += lax.dot_general(high, low, (((1,), (1,)), ((), ())), preferred_element_type=f32)
        level[j] = jnp.transpose(jnp.concatenate([total, total], axis=0))
        return carry

    lax.fori_loop(0, 32, tally, 0)
    own[1].wait()
    own[2].wait()
    for which, copy in copies:
        if which != 0:
            copy.wait()


def exchange(weight, bias, predicates, keys, valid):
    return pl.pallas_call(
        exchange_kernel,
        out_shape=(
            jax.ShapeDtypeStruct((4, D, D), f32),
            jax.ShapeDtypeStruct((4, 1, D), f32),
            jax.ShapeDtypeStruct((32, 128, 128), bf16),
            jax.ShapeDtypeStruct((32, 128, 128), i32),
            jax.ShapeDtypeStruct((64, 128), f32),
        ),
        in_specs=[spec(HB), spec(HB), spec(HB), spec(VM), spec(SM)],
        out_specs=(spec(VM),) * 5,
        scratch_shapes=[
            pltpu.VMEM((4, 4, 32), i32),
            pltpu.SMEM((4, 4, 32), i32),
            pltpu.SemaphoreType.DMA((3, 3)),
            pltpu.SemaphoreType.DMA((3, 3)),
            pltpu.SemaphoreType.DMA((4,)),
        ],
        compiler_params=pltpu.CompilerParams(collective_id=0, has_side_effects=True, vmem_limit_bytes=8 << 20),
    )(weight, bias, predicates, keys, valid)


def sections_kernel(rows_in, keys, w, b, same, level, table, rows, w2, ready, sem):
    fetch = pltpu.make_async_copy(rows_in, rows, sem)
    fetch.start()
    for s in range(SECTIONS):
        top = jnp.concatenate(high_low(w[s]), axis=1)
        w2[s] = jnp.concatenate([top, top], axis=0)

    def clear(i, carry):
        table[pl.ds(pl.multiple_of(i * 256, 256), 256), :] = jnp.zeros((256, D), f32)
        return carry

    lax.fori_loop(0, KEYS // 256, clear, 0)
    fetch.wait()

    def compute(t, slot):
        h = rows[pl.ds(pl.multiple_of(t * STEP, STEP), STEP), :]
        lev = level[pl.ds(t * (STEP // 128), STEP // 128)].reshape(STEP, 128)
        acc = jnp.zeros((STEP, D), f32)
        for s in range(SECTIONS):
            p = jnp.dot(jnp.concatenate(high_low(h), axis=1), w2[s], preferred_element_type=f32)
            h = h + jnp.tanh(p[:, :D] + (p[:, D:] + b[s]))
            acc = acc + jnp.where(lev > s, h, 0.0)
        both = jnp.concatenate(high_low(acc), axis=1)
        for j in range(STEP // 128):
            p = jnp.dot(same[t * (STEP // 128) + j], both[j * 128 : (j + 1) * 128], preferred_element_type=f32)
            ready[slot, j * 128 : (j + 1) * 128, :] = p[:, :D] + p[:, D:]

    def scatter(t, slot):
        for g in range(STEP // GROUP):
            at = [keys[t * (STEP // 128) + (g * GROUP + i) // 128, (g * GROUP + i) % 128] for i in range(GROUP)]
            held = [table[pl.ds(k, 1), :] for k in at]
            new = [held[i] + ready[slot, g * GROUP + i : g * GROUP + i + 1, :] for i in range(GROUP)]
            for i in range(GROUP):
                table[pl.ds(at[i], 1), :] = new[i]

    compute(0, 0)

    def body(t, carry):
        compute(t, t % 2)
        scatter(t - 1, (t - 1) % 2)
        return carry

    lax.fori_loop(1, ROWS // STEP, body, 0)
    scatter(ROWS // STEP - 1, (ROWS // STEP - 1) % 2)


def sections(rows, keys, w, b, same, level):
    return pl.pallas_call(
        sections_kernel,
        out_shape=jax.ShapeDtypeStruct((KEYS, D), f32),
        in_specs=[spec(HB), spec(SM)] + [spec(VM)] * 4,
        out_specs=spec(VM),
        scratch_shapes=[
            pltpu.VMEM((ROWS, D), f32),
            pltpu.VMEM((SECTIONS, 256, 256), bf16),
            pltpu.VMEM((2, STEP, D), f32),
            pltpu.SemaphoreType.DMA,
        ],
        compiler_params=pltpu.CompilerParams(vmem_limit_bytes=16 << 20),
    )(rows, keys, w, b, same, level)


PARTS = ((0, 24), (24, 24), (48, 16))
ORDER = ((0, 1, 2), (1, 2, 0), (2, 0, 1), (2, 0, 1))


def reduce_kernel(table, counts, means, count_out, *scratch):
    held = scratch[0:4]
    first = scratch[4:8]
    middle = scratch[8:12]
    second = scratch[12:16]
    last = scratch[16:20]
    third = scratch[20:24]
    core_sems, send, recv = scratch[24:27]
    z = lax.axis_index("section")
    row = lax.axis_index("rows")
    y, x, c = row // 8, (row // 2) % 4, row % 2
    place = (z, y, x)

    def peer(axis, k):
        at = list(place)
        at[axis] = lax.rem(at[axis] + k, 4)
        return at[axis], (at[0], at[1] * 8 + at[2] * 2 + c)

    other = (z, y * 8 + x * 2 + (1 - c))
    barrier = pltpu.get_barrier_semaphore()
    pl.semaphore_signal(barrier, inc=1, device_id=other, device_id_type=MESH)
    for axis in range(3):
        for k in range(1, 4):
            pl.semaphore_signal(barrier, inc=1, device_id=peer(axis, k)[1], device_id_type=MESH)
    pl.semaphore_wait(barrier, 10)

    core = []
    for n in (3, 0, 1, 2):
        if n < 3:
            src = table.at[:, :, :, 1 - c, pl.ds(PARTS[n][0], PARTS[n][1]), :]
        else:
            src = counts
        copy = pltpu.make_async_remote_copy(
            src_ref=src, dst_ref=held[n], send_sem=core_sems.at[0, n], recv_sem=core_sems.at[1, n],
            device_id=other, device_id_type=MESH)
        copy.start()
        core.append((n, copy))

    def piece(ref, axes, axis, index):
        where = [slice(None)] * len(axes)
        where[axes.index(axis)] = index
        return ref.at[tuple(where)]

    def send_stage(n, stage, source, axes, target):
        axis = ORDER[n][stage]
        copies = []
        for k in (2, 1, 3):
            index, device = peer(axis, k)
            copy = pltpu.make_async_remote_copy(
                src_ref=piece(source, axes, axis, index), dst_ref=target.at[k - 1],
                send_sem=send.at[n, stage, k - 1], recv_sem=recv.at[n, stage, k - 1],
                device_id=device, device_id_type=MESH)
            copy.start()
            copies.append(copy)
        return copies

    def summed(n, stage, source, axes, target):
        mine = piece(source, axes, ORDER[n][stage], place[ORDER[n][stage]])[...]
        return (mine + target[0]) + (target[1] + target[2])

    axes = [[0, 1, 2] for _ in range(4)]
    flying = {}
    for n, copy in core:
        copy.wait()
        if n < 3:
            for a in range(4):
                held[n][a] += table[a, :, :, c, PARTS[n][0] : PARTS[n][0] + PARTS[n][1], :]
        else:
            held[n][...] += counts[...]
        flying[n] = send_stage(n, 0, held[n], axes[n], first[n])
    for stage, (source, target, result) in enumerate(((held, first, middle), (middle, second, last))):
        for n in (3, 0, 1, 2) if stage else (3, 2, 0, 1):
            for copy in flying[n]:
                copy.wait()
            result[n][...] = summed(n, stage, source[n], axes[n], target[n])
            axes[n] = [a for a in axes[n] if a != ORDER[n][stage]]
            flying[n] = send_stage(n, stage + 1, result[n], axes[n], (second, third)[stage][n])
    total = None
    for n in (3, 0, 1, 2):
        for copy in flying[n]:
            copy.wait()
        value = summed(n, 2, last[n], axes[n], third[n])
        if n == 3:
            wide = jnp.transpose(jnp.broadcast_to(value, (128, 128)))
            total = jnp.where(c == 0, wide[:64], wide[64:])
            count_out[...] = jnp.broadcast_to(jnp.where(c == 0, value, pltpu.roll(value, 64, 1)), (8, 128))
            total = jnp.maximum(total, 1.0)
        else:
            lo, size = PARTS[n]
            means[lo : lo + size, :] = value / total[lo : lo + size]


def reduce_to_owner(table, counts):
    sizes = [24, 24, 16, 1]
    buffers = []
    for lead in ((4, 4, 4), (3, 4, 4), (4, 4), (3, 4), (4,), (3,)):
        buffers += [pltpu.VMEM((*lead, n, D), f32) for n in sizes]
    return pl.pallas_call(
        reduce_kernel,
        out_shape=(jax.ShapeDtypeStruct((64, D), f32), jax.ShapeDtypeStruct((8, D), f32)),
        in_specs=[spec(VM), spec(VM)],
        out_specs=(spec(VM), spec(VM)),
        scratch_shapes=buffers + [
            pltpu.SemaphoreType.DMA((2, 4)),
            pltpu.SemaphoreType.DMA((4, 3, 3)),
            pltpu.SemaphoreType.DMA((4, 3, 3)),
        ],
        compiler_params=pltpu.CompilerParams(collective_id=1, has_side_effects=True, vmem_limit_bytes=16 << 20),
    )(table.reshape(4, 4, 4, 2, 64, D), counts.reshape(4, 4, 4, 1, D))


def shards(rows_data, row_keys, valid_counts, predicates, section_weight, section_bias):
    keys = row_keys.reshape(32, 128)
    w, b, same, level, counts = exchange(
        section_weight, section_bias.reshape(1, 1, D), predicates.reshape(4, MICRO, 32), keys, valid_counts)
    table = sections(rows_data.reshape(ROWS, D), keys, w, b, same, level)
    means, total = reduce_to_owner(table, counts)
    return means, total[0, :64]


def solution(mesh):
    placed = (
        P("section", "rows", None),
        P("section", "rows"),
        P("section", "rows"),
        P("section", None, "rows"),
        P("section", None, None),
        P("section", None),
    )
    return jax.shard_map(
        shards,
        mesh=mesh,
        in_specs=placed,
        out_specs=(P(("section", "rows"), None), P(("section", "rows"))),
        check_vma=False,
    )
```

```python
import functools

import jax
import jax.numpy as jnp
from jax import lax
from jax.experimental import pallas as pl
from jax.experimental.pallas import tpu as pltpu
from jax.sharding import PartitionSpec as P

KEYS = 8192
SECTIONS = 4
D = 128
MICRO = 4
BLOCK = 1024
ROWS = MICRO * BLOCK
GROUP = 8
CHUNK = 256
f32, bf16, i32 = jnp.float32, jnp.bfloat16, jnp.int32
MESH = pl.DeviceIdType.MESH
VM, SM, HB = pltpu.VMEM, pltpu.SMEM, pltpu.HBM


def spec(space):
    return pl.BlockSpec(memory_space=space)


def pinned(x):
    return pltpu.with_memory_space_constraint(x, HB)


def high_low(x):
    high = x.astype(bf16)
    return high, (x - high.astype(f32)).astype(bf16)


def exchange_kernel(
    w_in, b_in, p_in, k_in, v_in,
    w_all, b_all, same, level, counts, table_a, table_b,
    keys, key_rows, valid, words_v, words, send, recv, local,
):
    me = lax.axis_index("section")
    row = lax.axis_index("rows")
    own = [
        pltpu.make_async_copy(src, dst, local.at[n])
        for n, (src, dst) in enumerate((
            (k_in, keys), (v_in, valid), (p_in.at[me], words_v.at[me]),
            (b_in.at[0], b_all.at[me]), (w_in.at[0], w_all.at[me])))
    ]
    for copy in own:
        copy.start()
    barrier = pltpu.get_barrier_semaphore()
    for k in range(1, 4):
        pl.semaphore_signal(barrier, inc=1, device_id=(lax.rem(me + k, 4), row), device_id_type=MESH)

    def clear(i, carry):
        at = pl.ds(pl.multiple_of(i * 512, 512), 512)
        table_a[at, :] = jnp.zeros((512, D), f32)
        table_b[at, :] = jnp.zeros((512, D), f32)
        return carry

    lax.fori_loop(0, KEYS // 512, clear, 0)
    pl.semaphore_wait(barrier, 3)
    copies = []
    for n, k in enumerate((2, 1, 3)):
        to = lax.rem(me + k, 4)
        for a, (src, dst) in enumerate(
            ((p_in.at[to], words_v.at[me]), (b_in.at[0], b_all.at[me]), (w_in.at[0], w_all.at[me]))
        ):
            copies.append((a, pltpu.make_async_remote_copy(
                src_ref=src, dst_ref=dst, send_sem=send.at[n, a], recv_sem=recv.at[n, a],
                device_id=(to, row), device_id_type=MESH)))
    for a in range(3):
        for which, copy in copies:
            if which == a:
                copy.start()
    own[0].wait()
    own[1].wait()
    group_i = (lax.broadcasted_iota(i32, (1, 128), 1) // GROUP) * KEYS

    for m in range(MICRO):
        for j in range(8):
            key_rows[m * 8 + j : m * 8 + j + 1, :] = keys[m : m + 1, j * 128 : (j + 1) * 128]

    def key_row_at(m, j):
        return key_rows[pl.ds(m * 8 + j, 1), :]

    def sameness(i, carry):
        for u in range(4):
            key_row = key_row_at(i // 2, (i % 2) * 4 + u) + group_i
            key_col = jnp.transpose(jnp.broadcast_to(key_row, (128, 128)))
            same[i * 4 + u] = jnp.where(key_col == key_row, 1.0, 0.0).astype(bf16)
        return carry

    lax.fori_loop(0, 8, sameness, 0)
    own[2].wait()
    for which, copy in copies:
        if which == 0:
            copy.wait()
    to_scalar = pltpu.make_async_copy(words_v, words, local.at[5])
    to_scalar.start()
    to_scalar.wait()
    counts[...] = jnp.zeros_like(counts)
    lane = lax.broadcasted_iota(i32, (64, 128), 1)
    sub64 = lax.broadcasted_iota(i32, (64, 128), 0)
    sub128 = lax.broadcasted_iota(i32, (128, 128), 0)

    def tally(i, carry):
        m = i // 2
        nv = valid[0, m]
        found = jnp.zeros((64, 128), f32)
        for u in range(4):
            j = (i % 2) * 4 + u
            total = jnp.zeros((8, 128), i32)
            alive = []
            for w in range(4):
                n = nv - (j * 4 + w) * 32
                alive.append(jnp.where(n >= 32, jnp.int32(-1), (jnp.int32(1) << jnp.clip(n, 0, 31)) - 1))
            for s in range(SECTIONS):
                alive = [a & words[s, m, j * 4 + w] for w, a in enumerate(alive)]
                v = jnp.where(
                    lane[:8] < 64,
                    jnp.where(lane[:8] < 32, alive[0], alive[1]),
                    jnp.where(lane[:8] < 96, alive[2], alive[3]))
                total = total + ((v >> (lane[:8] & 31)) & 1)
            key_row = key_row_at(m, j)
            lives = jnp.concatenate([total] * 8, axis=0).astype(f32)
            high = jnp.where((key_row >> 7) == sub64, lives, 0.0).astype(bf16)
            low = jnp.where((key_row & 127) == sub128, 1.0, 0.0).astype(bf16)
            found = found + lax.dot_general(high, low, (((1,), (1,)), ((), ())), preferred_element_type=f32)
            level[i * 4 + u] = jnp.transpose(jnp.concatenate([total] * 16, axis=0))
        counts[...] += found
        return carry

    lax.fori_loop(0, 8, tally, 0)
    own[3].wait()
    own[4].wait()
    for which, copy in copies:
        if which != 0:
            copy.wait()


def exchange(weight, bias, predicates, keys, valid):
    return pl.pallas_call(
        exchange_kernel,
        out_shape=(
            jax.ShapeDtypeStruct((4, D, D), f32),
            jax.ShapeDtypeStruct((4, 1, D), f32),
            jax.ShapeDtypeStruct((32, 128, 128), bf16),
            jax.ShapeDtypeStruct((32, 128, 128), i32),
            jax.ShapeDtypeStruct((64, 128), f32),
            jax.ShapeDtypeStruct((KEYS, D), f32),
            jax.ShapeDtypeStruct((KEYS, D), f32),
        ),
        in_specs=[spec(HB)] * 5,
        out_specs=(spec(VM),) * 7,
        scratch_shapes=[
            pltpu.VMEM((MICRO, BLOCK), i32),
            pltpu.VMEM((32, 128), i32),
            pltpu.SMEM((1, MICRO), i32),
            pltpu.VMEM((4, 4, 32), i32),
            pltpu.SMEM((4, 4, 32), i32),
            pltpu.SemaphoreType.DMA((3, 3)),
            pltpu.SemaphoreType.DMA((3, 3)),
            pltpu.SemaphoreType.DMA((6,)),
        ],
        compiler_params=pltpu.CompilerParams(collective_id=0, has_side_effects=True, vmem_limit_bytes=8 << 20),
        cost_estimate=pl.CostEstimate(flops=40_000_000_000, bytes_accessed=1 << 20, transcendentals=0),
    )(pinned(weight), pinned(bias), pinned(predicates), pinned(keys), pinned(valid))


def sections_kernel(rows, keys_in, w, b, same, level, clear_a, clear_b, table_a, table_b, w2, ready, keys, sem):
    fetch = pltpu.make_async_copy(keys_in, keys, sem)
    fetch.start()
    for s in range(SECTIONS):
        top = jnp.concatenate(high_low(w[s]), axis=1)
        w2[s] = jnp.concatenate([top, top], axis=0)

    def batch(m, carry):
        h = rows[m]
        alive = level[pl.ds(m * 8, 8)].reshape(BLOCK, 128)
        total = jnp.zeros((BLOCK, D), f32)
        for s in range(SECTIONS):
            p = jnp.dot(jnp.concatenate(high_low(h), axis=1), w2[s], preferred_element_type=f32)
            h = h + jnp.tanh(p[:, :D] + (p[:, D:] + b[s]))
            total = total + jnp.where(alive > s, h, 0.0)
        both = jnp.concatenate(high_low(total), axis=1)
        for j in range(8):
            p = jnp.dot(same[m * 8 + j], both[j * 128 : (j + 1) * 128], preferred_element_type=f32)
            ready[m, j * 128 : (j + 1) * 128, :] = p[:, :D] + p[:, D:]
        return carry

    lax.fori_loop(0, MICRO, batch, 0)
    fetch.wait()
    tables = (table_a, table_b)
    groups = CHUNK // GROUP

    def scatter(u, carry):
        m, base = u // (BLOCK // CHUNK), (u % (BLOCK // CHUNK)) * CHUNK

        def load(g):
            at = [keys[m, base + g * GROUP + i] for i in range(GROUP)]
            return at, [tables[g % 2][pl.ds(k, 1), :] for k in at]

        def store(g, at, held):
            for i, k in enumerate(at):
                tables[g % 2][pl.ds(k, 1), :] = held[i] + ready[m, pl.ds(base + g * GROUP + i, 1), :]

        flying = {g: load(g) for g in range(2)}
        for g in range(groups):
            store(g, *flying.pop(g))
            if g + 2 < groups:
                flying[g + 2] = load(g + 2)
        return carry

    lax.fori_loop(0, ROWS // CHUNK, scatter, 0)

    def join(i, carry):
        at = pl.ds(pl.multiple_of(i * 512, 512), 512)
        table_a[at, :] += table_b[at, :]
        return carry

    lax.fori_loop(0, KEYS // 512, join, 0)


def sections(rows, keys, w, b, same, level, clear_a, clear_b):
    return pl.pallas_call(
        sections_kernel,
        out_shape=(jax.ShapeDtypeStruct((KEYS, D), f32),) * 2,
        in_specs=[spec(VM), spec(HB)] + [spec(VM)] * 6,
        out_specs=(spec(VM),) * 2,
        scratch_shapes=[
            pltpu.VMEM((SECTIONS, 256, 256), bf16),
            pltpu.VMEM((MICRO, BLOCK, D), f32),
            pltpu.SMEM((MICRO, BLOCK), i32),
            pltpu.SemaphoreType.DMA,
        ],
        input_output_aliases={6: 0, 7: 1},
        compiler_params=pltpu.CompilerParams(vmem_limit_bytes=12 << 20),
    )(rows, pinned(keys), w, b, same, level, clear_a, clear_b)[0]


PARTS = ((0, 24), (24, 24), (48, 16))
ORDER = ((0, 1, 2), (1, 2, 0), (2, 0, 1), (2, 0, 1))


def reduce_kernel(table, counts, means, count_out, *scratch):
    held = scratch[0:4]
    first = scratch[4:8]
    middle = scratch[8:12]
    second = scratch[12:16]
    last = scratch[16:20]
    third = scratch[20:24]
    core_sems, send, recv = scratch[24:27]
    z = lax.axis_index("section")
    row = lax.axis_index("rows")
    y, x, c = row // 8, (row // 2) % 4, row % 2
    place = (z, y, x)

    def peer(axis, k):
        at = list(place)
        at[axis] = lax.rem(at[axis] + k, 4)
        return at[axis], (at[0], at[1] * 8 + at[2] * 2 + c)

    other = (z, y * 8 + x * 2 + (1 - c))
    barrier = pltpu.get_barrier_semaphore()
    pl.semaphore_signal(barrier, inc=1, device_id=other, device_id_type=MESH)
    for axis in range(3):
        for k in range(1, 4):
            pl.semaphore_signal(barrier, inc=1, device_id=peer(axis, k)[1], device_id_type=MESH)
    pl.semaphore_wait(barrier, 10)

    core = []
    for n in (3, 0, 1, 2):
        if n < 3:
            src = table.at[:, :, :, 1 - c, pl.ds(PARTS[n][0], PARTS[n][1]), :]
        else:
            src = counts
        copy = pltpu.make_async_remote_copy(
            src_ref=src, dst_ref=held[n], send_sem=core_sems.at[0, n], recv_sem=core_sems.at[1, n],
            device_id=other, device_id_type=MESH)
        copy.start()
        core.append((n, copy))

    def piece(ref, axes, axis, index):
        where = [slice(None)] * len(axes)
        where[axes.index(axis)] = index
        return ref.at[tuple(where)]

    def send_stage(n, stage, source, axes, target):
        axis = ORDER[n][stage]
        copies = []
        for k in (2, 1, 3):
            index, device = peer(axis, k)
            copy = pltpu.make_async_remote_copy(
                src_ref=piece(source, axes, axis, index), dst_ref=target.at[k - 1],
                send_sem=send.at[n, stage, k - 1], recv_sem=recv.at[n, stage, k - 1],
                device_id=device, device_id_type=MESH)
            copy.start()
            copies.append(copy)
        return copies

    def summed(n, stage, source, axes, target):
        mine = piece(source, axes, ORDER[n][stage], place[ORDER[n][stage]])[...]
        return (mine + target[0]) + (target[1] + target[2])

    axes = [[0, 1, 2] for _ in range(4)]
    flying = {}
    for n, copy in core:
        copy.wait()
        if n < 3:
            for a in range(4):
                held[n][a] += table[a, :, :, c, PARTS[n][0] : PARTS[n][0] + PARTS[n][1], :]
        else:
            held[n][...] += counts[...]
        flying[n] = send_stage(n, 0, held[n], axes[n], first[n])
    for stage, (source, target, result) in enumerate(((held, first, middle), (middle, second, last))):
        for n in (3, 0, 1, 2) if stage else (3, 2, 0, 1):
            for copy in flying[n]:
                copy.wait()
            result[n][...] = summed(n, stage, source[n], axes[n], target[n])
            axes[n] = [a for a in axes[n] if a != ORDER[n][stage]]
            flying[n] = send_stage(n, stage + 1, result[n], axes[n], (second, third)[stage][n])
    total = None
    for n in (3, 0, 1, 2):
        for copy in flying[n]:
            copy.wait()
        value = summed(n, 2, last[n], axes[n], third[n])
        if n == 3:
            wide = jnp.transpose(jnp.broadcast_to(value, (128, 128)))
            total = jnp.where(c == 0, wide[:64], wide[64:])
            count_out[...] = jnp.broadcast_to(jnp.where(c == 0, value, pltpu.roll(value, 64, 1)), (8, 128))
            total = jnp.maximum(total, 1.0)
        else:
            lo, size = PARTS[n]
            means[lo : lo + size, :] = value / total[lo : lo + size]


def reduce_to_owner(table, counts):
    sizes = [24, 24, 16, 1]
    buffers = []
    for lead in ((4, 4, 4), (3, 4, 4), (4, 4), (3, 4), (4,), (3,)):
        buffers += [pltpu.VMEM((*lead, n, D), f32) for n in sizes]
    return pl.pallas_call(
        reduce_kernel,
        out_shape=(jax.ShapeDtypeStruct((64, D), f32), jax.ShapeDtypeStruct((8, D), f32)),
        in_specs=[spec(VM), spec(VM)],
        out_specs=(spec(VM), spec(VM)),
        scratch_shapes=buffers + [
            pltpu.SemaphoreType.DMA((2, 4)),
            pltpu.SemaphoreType.DMA((4, 3, 3)),
            pltpu.SemaphoreType.DMA((4, 3, 3)),
        ],
        compiler_params=pltpu.CompilerParams(collective_id=1, has_side_effects=True, vmem_limit_bytes=16 << 20),
    )(table.reshape(4, 4, 4, 2, 64, D), counts.reshape(4, 4, 4, 1, D))


def shards(rows_data, row_keys, valid_counts, predicates, section_weight, section_bias):
    w, b, same, level, counts, clear_a, clear_b = exchange(
        section_weight, section_bias.reshape(1, 1, D), predicates.reshape(4, MICRO, 32), row_keys, valid_counts.T)
    table = sections(rows_data, row_keys, w, b, same, level, clear_a, clear_b)
    means, total = reduce_to_owner(table, counts)
    return means, total[0, :64]


def solution(mesh):
    placed = (
        P("section", "rows", None),
        P("section", "rows"),
        P("section", "rows"),
        P("section", None, "rows"),
        P("section", None, None),
        P("section", None),
    )
    return jax.shard_map(
        shards,
        mesh=mesh,
        in_specs=placed,
        out_specs=(P(("section", "rows"), None), P(("section", "rows"))),
        check_vma=False,
    )
```

```python
import functools

import jax
import jax.numpy as jnp
from jax import lax
from jax.experimental import pallas as pl
from jax.experimental.pallas import tpu as pltpu
from jax.sharding import PartitionSpec as P

KEYS = 8192
SECTIONS = 4
D = 128
MICRO = 4
BLOCK = 1024
ROWS = MICRO * BLOCK
GROUP = 8
CHUNK = 256
f32, bf16, i32 = jnp.float32, jnp.bfloat16, jnp.int32
MESH = pl.DeviceIdType.MESH
VM, SM, HB = pltpu.VMEM, pltpu.SMEM, pltpu.HBM


def spec(space):
    return pl.BlockSpec(memory_space=space)


def pinned(x):
    return pltpu.with_memory_space_constraint(x, HB)


def high_low(x):
    high = x.astype(bf16)
    return high, (x - high.astype(f32)).astype(bf16)


def exchange_kernel(
    w_in, b_in, p_in, k_in, v_in,
    w_all, b_all, same, level, counts, table_a, table_b, key_rows,
    keys, valid, words_v, words, send, recv, local,
):
    me = lax.axis_index("section")
    row = lax.axis_index("rows")
    own = [
        pltpu.make_async_copy(src, dst, local.at[n])
        for n, (src, dst) in enumerate((
            (k_in, keys), (v_in, valid), (p_in.at[me], words_v.at[me]),
            (b_in.at[0], b_all.at[me]), (w_in.at[0], w_all.at[me])))
    ]
    for copy in own:
        copy.start()
    barrier = pltpu.get_barrier_semaphore()
    for k in range(1, 4):
        pl.semaphore_signal(barrier, inc=1, device_id=(lax.rem(me + k, 4), row), device_id_type=MESH)

    def clear(i, carry):
        at = pl.ds(pl.multiple_of(i * 512, 512), 512)
        table_a[at, :] = jnp.zeros((512, D), f32)
        table_b[at, :] = jnp.zeros((512, D), f32)
        return carry

    lax.fori_loop(0, KEYS // 512, clear, 0)
    pl.semaphore_wait(barrier, 3)
    copies = []
    for n, k in enumerate((2, 1, 3)):
        to = lax.rem(me + k, 4)
        for a, (src, dst) in enumerate(
            ((p_in.at[to], words_v.at[me]), (b_in.at[0], b_all.at[me]), (w_in.at[0], w_all.at[me]))
        ):
            copies.append((a, pltpu.make_async_remote_copy(
                src_ref=src, dst_ref=dst, send_sem=send.at[n, a], recv_sem=recv.at[n, a],
                device_id=(to, row), device_id_type=MESH)))
    for a in range(3):
        for which, copy in copies:
            if which == a:
                copy.start()
    own[0].wait()
    own[1].wait()
    group_i = (lax.broadcasted_iota(i32, (1, 128), 1) // GROUP) * KEYS

    for m in range(MICRO):
        for j in range(8):
            key_rows[m * 8 + j : m * 8 + j + 1, :] = keys[m : m + 1, j * 128 : (j + 1) * 128]

    def key_row_at(m, j):
        return key_rows[pl.ds(m * 8 + j, 1), :]

    def sameness(i, carry):
        for u in range(4):
            key_row = key_row_at(i // 2, (i % 2) * 4 + u) + group_i
            key_col = jnp.transpose(jnp.broadcast_to(key_row, (128, 128)))
            same[i * 4 + u] = jnp.where(key_col == key_row, 1.0, 0.0).astype(bf16)
        return carry

    lax.fori_loop(0, 8, sameness, 0)
    own[2].wait()
    for which, copy in copies:
        if which == 0:
            copy.wait()
    to_scalar = pltpu.make_async_copy(words_v, words, local.at[5])
    to_scalar.start()
    to_scalar.wait()
    counts[...] = jnp.zeros_like(counts)
    lane = lax.broadcasted_iota(i32, (64, 128), 1)
    sub64 = lax.broadcasted_iota(i32, (64, 128), 0)
    sub128 = lax.broadcasted_iota(i32, (128, 128), 0)

    def tally(i, carry):
        m = i // 2
        nv = valid[0, m]
        found = jnp.zeros((64, 128), f32)
        for u in range(4):
            j = (i % 2) * 4 + u
            total = jnp.zeros((8, 128), i32)
            alive = []
            for w in range(4):
                n = nv - (j * 4 + w) * 32
                alive.append(jnp.where(n >= 32, jnp.int32(-1), (jnp.int32(1) << jnp.clip(n, 0, 31)) - 1))
            for s in range(SECTIONS):
                alive = [a & words[s, m, j * 4 + w] for w, a in enumerate(alive)]
                v = jnp.where(
                    lane[:8] < 64,
                    jnp.where(lane[:8] < 32, alive[0], alive[1]),
                    jnp.where(lane[:8] < 96, alive[2], alive[3]))
                total = total + ((v >> (lane[:8] & 31)) & 1)
            key_row = key_row_at(m, j)
            lives = jnp.concatenate([total] * 8, axis=0).astype(f32)
            high = jnp.where((key_row >> 7) == sub64, lives, 0.0).astype(bf16)
            low = jnp.where((key_row & 127) == sub128, 1.0, 0.0).astype(bf16)
            found = found + lax.dot_general(high, low, (((1,), (1,)), ((), ())), preferred_element_type=f32)
            level[i * 4 + u] = jnp.transpose(jnp.concatenate([total] * 16, axis=0))
        counts[...] += found
        return carry

    lax.fori_loop(0, 8, tally, 0)
    own[3].wait()
    own[4].wait()
    for which, copy in copies:
        if which != 0:
            copy.wait()


def exchange(weight, bias, predicates, keys, valid):
    return pl.pallas_call(
        exchange_kernel,
        out_shape=(
            jax.ShapeDtypeStruct((4, D, D), f32),
            jax.ShapeDtypeStruct((4, 1, D), f32),
            jax.ShapeDtypeStruct((32, 128, 128), bf16),
            jax.ShapeDtypeStruct((32, 128, 128), i32),
            jax.ShapeDtypeStruct((64, 128), f32),
            jax.ShapeDtypeStruct((KEYS, D), f32),
            jax.ShapeDtypeStruct((KEYS, D), f32),
            jax.ShapeDtypeStruct((32, 128), i32),
        ),
        in_specs=[spec(HB)] * 5,
        out_specs=(spec(VM),) * 8,
        scratch_shapes=[
            pltpu.VMEM((MICRO, BLOCK), i32),
            pltpu.SMEM((1, MICRO), i32),
            pltpu.VMEM((4, 4, 32), i32),
            pltpu.SMEM((4, 4, 32), i32),
            pltpu.SemaphoreType.DMA((3, 3)),
            pltpu.SemaphoreType.DMA((3, 3)),
            pltpu.SemaphoreType.DMA((6,)),
        ],
        compiler_params=pltpu.CompilerParams(collective_id=0, has_side_effects=True, vmem_limit_bytes=8 << 20),
        cost_estimate=pl.CostEstimate(flops=40_000_000_000, bytes_accessed=1 << 20, transcendentals=0),
    )(pinned(weight), pinned(bias), pinned(predicates), pinned(keys), pinned(valid))


def sections_kernel(rows, keys_in, w, b, same, level, clear_a, clear_b, table_a, table_b, w2, ready, keys, sem):
    fetch = pltpu.make_async_copy(keys_in, keys, sem)
    fetch.start()
    for s in range(SECTIONS):
        top = jnp.concatenate(high_low(w[s]), axis=1)
        w2[s] = jnp.concatenate([top, top], axis=0)

    def batch(m, carry):
        h = rows[m]
        alive = level[pl.ds(m * 8, 8)].reshape(BLOCK, 128)
        total = jnp.zeros((BLOCK, D), f32)
        for s in range(SECTIONS):
            p = jnp.dot(jnp.concatenate(high_low(h), axis=1), w2[s], preferred_element_type=f32)
            h = h + jnp.tanh(p[:, :D] + (p[:, D:] + b[s]))
            total = total + jnp.where(alive > s, h, 0.0)
        both = jnp.concatenate(high_low(total), axis=1)
        for j in range(8):
            p = jnp.dot(same[m * 8 + j], both[j * 128 : (j + 1) * 128], preferred_element_type=f32)
            ready[pl.ds(pl.multiple_of(m * BLOCK + j * 128, 128), 128), :] = p[:, :D] + p[:, D:]
        return carry

    lax.fori_loop(0, MICRO, batch, 0)
    fetch.wait()
    tables = (table_a, table_b)
    groups = CHUNK // GROUP

    def scatter(u, carry):
        def load(g):
            at = [keys[u * (CHUNK // 128) + (g * GROUP + i) // 128, (g * GROUP + i) % 128] for i in range(GROUP)]
            return at, [tables[g % 2][pl.ds(k, 1), :] for k in at]

        def store(g, at, held):
            for i, k in enumerate(at):
                tables[g % 2][pl.ds(k, 1), :] = held[i] + ready[pl.ds(u * CHUNK + g * GROUP + i, 1), :]

        flying = {g: load(g) for g in range(2)}
        for g in range(groups):
            store(g, *flying.pop(g))
            if g + 2 < groups:
                flying[g + 2] = load(g + 2)
        return carry

    lax.fori_loop(0, ROWS // CHUNK, scatter, 0)

    def join(i, carry):
        at = pl.ds(pl.multiple_of(i * 512, 512), 512)
        table_a[at, :] += table_b[at, :]
        return carry

    lax.fori_loop(0, KEYS // 512, join, 0)


def sections(rows, keys, w, b, same, level, clear_a, clear_b):
    return pl.pallas_call(
        sections_kernel,
        out_shape=(jax.ShapeDtypeStruct((KEYS, D), f32),) * 2,
        in_specs=[spec(VM)] * 8,
        out_specs=(spec(VM),) * 2,
        scratch_shapes=[
            pltpu.VMEM((SECTIONS, 256, 256), bf16),
            pltpu.VMEM((ROWS, D), f32),
            pltpu.SMEM((32, 128), i32),
            pltpu.SemaphoreType.DMA,
        ],
        input_output_aliases={6: 0, 7: 1},
        compiler_params=pltpu.CompilerParams(vmem_limit_bytes=12 << 20),
    )(rows, keys, w, b, same, level, clear_a, clear_b)[0]


PARTS = ((0, 1, (2, 0, 1)), (0, 24, (0, 1, 2)), (24, 24, (1, 2, 0)), (48, 16, (2, 0, 1)))
N = len(PARTS)


def reduce_kernel(table, counts, means, count_out, *scratch):
    held, near, middle, second, last, third = (scratch[i * N : (i + 1) * N] for i in range(6))
    core_sems, near_send, near_recv, send, recv = scratch[6 * N :]
    z = lax.axis_index("section")
    row = lax.axis_index("rows")
    y, x, c = row // 8, (row // 2) % 4, row % 2
    place = (z, y, x)

    def position(axis, k):
        return lax.rem(place[axis] + k, 4)

    def device(axis, k):
        at = list(place)
        at[axis] = position(axis, k)
        return (at[0], at[1] * 8 + at[2] * 2 + c)

    other = (z, y * 8 + x * 2 + (1 - c))
    barrier = pltpu.get_barrier_semaphore()
    pl.semaphore_signal(barrier, inc=1, device_id=other, device_id_type=MESH)
    for axis in range(3):
        for k in range(1, 4):
            pl.semaphore_signal(barrier, inc=1, device_id=device(axis, k), device_id_type=MESH)
    pl.semaphore_wait(barrier, 10)

    def remote(src, dst, send_sem, recv_sem, to):
        copy = pltpu.make_async_remote_copy(
            src_ref=src, dst_ref=dst, send_sem=send_sem, recv_sem=recv_sem, device_id=to, device_id_type=MESH)
        copy.start()
        return copy

    def piece(ref, axes, axis, index, half=None):
        where = [slice(None)] * len(axes)
        where[axes.index(axis)] = index
        if half is not None:
            where[1 if axes[0] == axis else 0] = pl.ds(2 * half, 2)
        return ref.at[tuple(where)]

    every = [0, 1, 2]
    core = []
    for n, (start, size, order) in enumerate(PARTS):
        src = counts if n == 0 else table.at[:, :, :, 1 - c, pl.ds(start, size), :]
        core.append(remote(src, held[n], core_sems.at[0, n], core_sems.at[1, n], other))

    sent = [[] for _ in PARTS]
    relay = [None] * N
    for n, (start, size, order) in enumerate(PARTS):
        core[n].wait()
        if n == 0:
            held[n][...] += counts[...]
        else:
            for a in range(4):
                held[n][a] += table[a, :, :, c, start : start + size, :]
        axis = order[0]

        def hop(slot, index, half, k):
            return remote(
                piece(held[n], every, axis, index, half), near[n].at[slot],
                near_send.at[n, slot], near_recv.at[n, slot], device(axis, k))

        relay[n] = [hop(0, position(axis, 2), 0, 1), hop(1, position(axis, 2), 1, 3)]
        sent[n] = [hop(2, position(axis, 1), 1, 1), hop(3, position(axis, 3), 0, 3)]
    for n, (start, size, order) in enumerate(PARTS):
        axis = order[0]
        for half, k in ((0, 1), (1, 3)):
            relay[n][half].wait()
            block = piece(held[n], every, axis, position(axis, k), half)
            block[...] += near[n][half]
            sent[n].append(remote(
                block, near[n].at[4 + half], near_send.at[n, 4 + half], near_recv.at[n, 4 + half], device(axis, k)))

    def spread(n, stage, source, axes, target):
        axis = PARTS[n][2][stage]
        return [
            remote(
                piece(source, axes, axis, position(axis, k)), target.at[k - 1],
                send.at[n, stage - 1, k - 1], recv.at[n, stage - 1, k - 1], device(axis, k))
            for k in (2, 1, 3)
        ]

    def summed(n, stage, source, axes, target):
        axis = PARTS[n][2][stage]
        return (piece(source, axes, axis, place[axis])[...] + target[0]) + (target[1] + target[2])

    for n, (start, size, order) in enumerate(PARTS):
        for copy in sent[n]:
            copy.wait()
        axis = order[0]
        middle[n][0:2] = (piece(held[n], every, axis, place[axis], 0)[...] + near[n][3]) + near[n][4]
        middle[n][2:4] = (piece(held[n], every, axis, place[axis], 1)[...] + near[n][2]) + near[n][5]
        sent[n] = spread(n, 1, middle[n], [a for a in every if a != axis], second[n])
    for n, (start, size, order) in enumerate(PARTS):
        for copy in sent[n]:
            copy.wait()
        axes = [a for a in every if a != order[0]]
        last[n][...] = summed(n, 1, middle[n], axes, second[n])
        sent[n] = spread(n, 2, last[n], [order[2]], third[n])
    for n, (start, size, order) in enumerate(PARTS):
        for copy in sent[n]:
            copy.wait()
        value = summed(n, 2, last[n], [order[2]], third[n])
        if n == 0:
            wide = jnp.transpose(jnp.broadcast_to(value, (128, 128)))
            total = jnp.maximum(jnp.where(c == 0, wide[:64], wide[64:]), 1.0)
            count_out[...] = jnp.broadcast_to(jnp.where(c == 0, value, pltpu.roll(value, 64, 1)), (8, 128))
        else:
            means[start : start + size, :] = value / total[start : start + size]


def reduce_to_owner(table, counts):
    buffers = []
    for lead in ((4, 4, 4), (6, 2, 4), (4, 4), (3, 4), (4,), (3,)):
        buffers += [pltpu.VMEM((*lead, size, D), f32) for _, size, _ in PARTS]
    return pl.pallas_call(
        reduce_kernel,
        out_shape=(jax.ShapeDtypeStruct((64, D), f32), jax.ShapeDtypeStruct((8, D), f32)),
        in_specs=[spec(VM), spec(VM)],
        out_specs=(spec(VM), spec(VM)),
        scratch_shapes=buffers + [
            pltpu.SemaphoreType.DMA((2, N)),
            pltpu.SemaphoreType.DMA((N, 6)),
            pltpu.SemaphoreType.DMA((N, 6)),
            pltpu.SemaphoreType.DMA((N, 2, 3)),
            pltpu.SemaphoreType.DMA((N, 2, 3)),
        ],
        compiler_params=pltpu.CompilerParams(collective_id=1, has_side_effects=True, vmem_limit_bytes=16 << 20),
    )(table.reshape(4, 4, 4, 2, 64, D), counts.reshape(4, 4, 4, 1, D))


def shards(rows_data, row_keys, valid_counts, predicates, section_weight, section_bias):
    w, b, same, level, counts, clear_a, clear_b, key_rows = exchange(
        section_weight, section_bias.reshape(1, 1, D), predicates.reshape(4, MICRO, 32), row_keys, valid_counts.T)
    table = sections(rows_data, key_rows, w, b, same, level, clear_a, clear_b)
    means, total = reduce_to_owner(table, counts)
    return means, total[0, :64]


def solution(mesh):
    placed = (
        P("section", "rows", None),
        P("section", "rows"),
        P("section", "rows"),
        P("section", None, "rows"),
        P("section", None, None),
        P("section", None),
    )
    return jax.shard_map(
        shards,
        mesh=mesh,
        in_specs=placed,
        out_specs=(P(("section", "rows"), None), P(("section", "rows"))),
        check_vma=False,
    )
```

```python
import functools

import jax
import jax.numpy as jnp
from jax import lax
from jax.experimental import pallas as pl
from jax.experimental.pallas import tpu as pltpu
from jax.sharding import PartitionSpec as P

KEYS = 8192
SECTIONS = 4
D = 128
MICRO = 4
BLOCK = 1024
ROWS = MICRO * BLOCK
GROUP = 8
CHUNK = 256
f32, bf16, i32 = jnp.float32, jnp.bfloat16, jnp.int32
MESH = pl.DeviceIdType.MESH
VM, SM, HB = pltpu.VMEM, pltpu.SMEM, pltpu.HBM


def spec(space):
    return pl.BlockSpec(memory_space=space)


def pinned(x):
    return pltpu.with_memory_space_constraint(x, HB)


def high_low(x):
    high = x.astype(bf16)
    return high, (x - high.astype(f32)).astype(bf16)


def exchange_kernel(
    w_in, b_in, p_in, k_in, v_in,
    w_all, b_all, same, level, counts, table_a, table_b, key_rows,
    keys, valid, words_v, words, send, recv, local,
):
    me = lax.axis_index("section")
    row = lax.axis_index("rows")
    own = [
        pltpu.make_async_copy(src, dst, local.at[n])
        for n, (src, dst) in enumerate((
            (k_in, keys), (v_in, valid), (p_in.at[me], words_v.at[me]),
            (b_in.at[0], b_all.at[me]), (w_in.at[0], w_all.at[me])))
    ]
    for copy in own:
        copy.start()
    barrier = pltpu.get_barrier_semaphore()
    for k in range(1, 4):
        pl.semaphore_signal(barrier, inc=1, device_id=(lax.rem(me + k, 4), row), device_id_type=MESH)

    def clear(i, carry):
        at = pl.ds(pl.multiple_of(i * 512, 512), 512)
        table_a[at, :] = jnp.zeros((512, D), f32)
        table_b[at, :] = jnp.zeros((512, D), f32)
        return carry

    lax.fori_loop(0, KEYS // 512, clear, 0)
    pl.semaphore_wait(barrier, 3)
    copies = []
    for n, k in enumerate((2, 1, 3)):
        to = lax.rem(me + k, 4)
        for a, (src, dst) in enumerate(
            ((p_in.at[to], words_v.at[me]), (b_in.at[0], b_all.at[me]), (w_in.at[0], w_all.at[me]))
        ):
            copies.append((a, pltpu.make_async_remote_copy(
                src_ref=src, dst_ref=dst, send_sem=send.at[n, a], recv_sem=recv.at[n, a],
                device_id=(to, row), device_id_type=MESH)))
    for a in range(3):
        for which, copy in copies:
            if which == a:
                copy.start()
    own[0].wait()
    own[1].wait()
    group_i = (lax.broadcasted_iota(i32, (1, 128), 1) // GROUP) * KEYS

    for m in range(MICRO):
        for j in range(8):
            key_rows[m * 8 + j : m * 8 + j + 1, :] = keys[m : m + 1, j * 128 : (j + 1) * 128]

    def key_row_at(m, j):
        return key_rows[pl.ds(m * 8 + j, 1), :]

    def sameness(i, carry):
        for u in range(4):
            key_row = key_row_at(i // 2, (i % 2) * 4 + u) + group_i
            key_col = jnp.transpose(jnp.broadcast_to(key_row, (128, 128)))
            same[i * 4 + u] = jnp.where(key_col == key_row, 1.0, 0.0).astype(bf16)
        return carry

    lax.fori_loop(0, 8, sameness, 0)
    own[2].wait()
    for which, copy in copies:
        if which == 0:
            copy.wait()
    to_scalar = pltpu.make_async_copy(words_v, words, local.at[5])
    to_scalar.start()
    to_scalar.wait()
    counts[...] = jnp.zeros_like(counts)
    lane = lax.broadcasted_iota(i32, (64, 128), 1)
    sub64 = lax.broadcasted_iota(i32, (64, 128), 0)
    sub128 = lax.broadcasted_iota(i32, (128, 128), 0)

    def tally(i, carry):
        m = i // 2
        nv = valid[0, m]
        found = jnp.zeros((64, 128), f32)
        for u in range(4):
            j = (i % 2) * 4 + u
            total = jnp.zeros((8, 128), i32)
            alive = []
            for w in range(4):
                n = nv - (j * 4 + w) * 32
                alive.append(jnp.where(n >= 32, jnp.int32(-1), (jnp.int32(1) << jnp.clip(n, 0, 31)) - 1))
            for s in range(SECTIONS):
                alive = [a & words[s, m, j * 4 + w] for w, a in enumerate(alive)]
                v = jnp.where(
                    lane[:8] < 64,
                    jnp.where(lane[:8] < 32, alive[0], alive[1]),
                    jnp.where(lane[:8] < 96, alive[2], alive[3]))
                total = total + ((v >> (lane[:8] & 31)) & 1)
            key_row = key_row_at(m, j)
            lives = jnp.concatenate([total] * 8, axis=0).astype(f32)
            high = jnp.where((key_row >> 7) == sub64, lives, 0.0).astype(bf16)
            low = jnp.where((key_row & 127) == sub128, 1.0, 0.0).astype(bf16)
            found = found + lax.dot_general(high, low, (((1,), (1,)), ((), ())), preferred_element_type=f32)
            level[i * 4 + u] = jnp.transpose(jnp.concatenate([total] * 16, axis=0))
        counts[...] += found
        return carry

    lax.fori_loop(0, 8, tally, 0)
    own[3].wait()
    own[4].wait()
    for which, copy in copies:
        if which != 0:
            copy.wait()


def exchange(weight, bias, predicates, keys, valid):
    return pl.pallas_call(
        exchange_kernel,
        out_shape=(
            jax.ShapeDtypeStruct((4, D, D), f32),
            jax.ShapeDtypeStruct((4, 1, D), f32),
            jax.ShapeDtypeStruct((32, 128, 128), bf16),
            jax.ShapeDtypeStruct((32, 128, 128), i32),
            jax.ShapeDtypeStruct((64, 128), f32),
            jax.ShapeDtypeStruct((KEYS, D), f32),
            jax.ShapeDtypeStruct((KEYS, D), f32),
            jax.ShapeDtypeStruct((32, 128), i32),
        ),
        in_specs=[spec(HB)] * 5,
        out_specs=(spec(VM),) * 8,
        scratch_shapes=[
            pltpu.VMEM((MICRO, BLOCK), i32),
            pltpu.SMEM((1, MICRO), i32),
            pltpu.VMEM((4, 4, 32), i32),
            pltpu.SMEM((4, 4, 32), i32),
            pltpu.SemaphoreType.DMA((3, 3)),
            pltpu.SemaphoreType.DMA((3, 3)),
            pltpu.SemaphoreType.DMA((6,)),
        ],
        compiler_params=pltpu.CompilerParams(collective_id=0, has_side_effects=True, vmem_limit_bytes=8 << 20),
        cost_estimate=pl.CostEstimate(flops=40_000_000_000, bytes_accessed=1 << 20, transcendentals=0),
    )(pinned(weight), pinned(bias), pinned(predicates), pinned(keys), pinned(valid))


def sections_kernel(rows, keys_in, w, b, same, level, clear_a, clear_b, table_a, table_b, w2, ready, keys, sem):
    fetch = pltpu.make_async_copy(keys_in, keys, sem)
    fetch.start()
    for s in range(SECTIONS):
        top = jnp.concatenate(high_low(w[s]), axis=1)
        w2[s] = jnp.concatenate([top, top], axis=0)

    def batch(m, carry):
        h = rows[m]
        alive = level[pl.ds(m * 8, 8)].reshape(BLOCK, 128)
        total = jnp.zeros((BLOCK, D), f32)
        for s in range(SECTIONS):
            p = jnp.dot(jnp.concatenate(high_low(h), axis=1), w2[s], preferred_element_type=f32)
            h = h + jnp.tanh(p[:, :D] + (p[:, D:] + b[s]))
            total = total + jnp.where(alive > s, h, 0.0)
        both = jnp.concatenate(high_low(total), axis=1)
        for j in range(8):
            p = jnp.dot(same[m * 8 + j], both[j * 128 : (j + 1) * 128], preferred_element_type=f32)
            ready[pl.ds(pl.multiple_of(m * BLOCK + j * 128, 128), 128), :] = p[:, :D] + p[:, D:]
        return carry

    lax.fori_loop(0, MICRO, batch, 0)
    fetch.wait()
    tables = (table_a, table_b)
    groups = CHUNK // GROUP

    def scatter(u, carry):
        def load(g):
            at = [keys[u * (CHUNK // 128) + (g * GROUP + i) // 128, (g * GROUP + i) % 128] for i in range(GROUP)]
            return at, [tables[g % 2][pl.ds(k, 1), :] for k in at]

        def store(g, at, held):
            for i, k in enumerate(at):
                tables[g % 2][pl.ds(k, 1), :] = held[i] + ready[pl.ds(u * CHUNK + g * GROUP + i, 1), :]

        flying = {g: load(g) for g in range(2)}
        for g in range(groups):
            store(g, *flying.pop(g))
            if g + 2 < groups:
                flying[g + 2] = load(g + 2)
        return carry

    lax.fori_loop(0, ROWS // CHUNK, scatter, 0)

    def join(i, carry):
        at = pl.ds(pl.multiple_of(i * 512, 512), 512)
        table_a[at, :] += table_b[at, :]
        return carry

    lax.fori_loop(0, KEYS // 512, join, 0)


def sections(rows, keys, w, b, same, level, clear_a, clear_b):
    return pl.pallas_call(
        sections_kernel,
        out_shape=(jax.ShapeDtypeStruct((KEYS, D), f32),) * 2,
        in_specs=[spec(VM)] * 8,
        out_specs=(spec(VM),) * 2,
        scratch_shapes=[
            pltpu.VMEM((SECTIONS, 256, 256), bf16),
            pltpu.VMEM((ROWS, D), f32),
            pltpu.SMEM((32, 128), i32),
            pltpu.SemaphoreType.DMA,
        ],
        input_output_aliases={6: 0, 7: 1},
        compiler_params=pltpu.CompilerParams(vmem_limit_bytes=12 << 20),
    )(rows, keys, w, b, same, level, clear_a, clear_b)[0]


PARTS = (
    (0, 1, (2, 0, 1)),
    (0, 8, (0, 1, 2)), (8, 8, (1, 2, 0)), (16, 8, (2, 0, 1)),
    (24, 16, (0, 1, 2)), (40, 16, (1, 2, 0)), (56, 8, (2, 0, 1)),
)
N = len(PARTS)


def reduce_kernel(table, counts, means, count_out, *scratch):
    held, near, middle, second, last, third = (scratch[i * N : (i + 1) * N] for i in range(6))
    core_sems, near_send, near_recv, send, recv = scratch[6 * N :]
    z = lax.axis_index("section")
    row = lax.axis_index("rows")
    y, x, c = row // 8, (row // 2) % 4, row % 2
    place = (z, y, x)

    def position(axis, k):
        return lax.rem(place[axis] + k, 4)

    def device(axis, k):
        at = list(place)
        at[axis] = position(axis, k)
        return (at[0], at[1] * 8 + at[2] * 2 + c)

    other = (z, y * 8 + x * 2 + (1 - c))
    barrier = pltpu.get_barrier_semaphore()
    pl.semaphore_signal(barrier, inc=1, device_id=other, device_id_type=MESH)
    for axis in range(3):
        for k in range(1, 4):
            pl.semaphore_signal(barrier, inc=1, device_id=device(axis, k), device_id_type=MESH)
    pl.semaphore_wait(barrier, 10)

    def remote(src, dst, send_sem, recv_sem, to):
        copy = pltpu.make_async_remote_copy(
            src_ref=src, dst_ref=dst, send_sem=send_sem, recv_sem=recv_sem, device_id=to, device_id_type=MESH)
        copy.start()
        return copy

    def piece(ref, axes, axis, index, half=None):
        where = [slice(None)] * len(axes)
        where[axes.index(axis)] = index
        if half is not None:
            where[1 if axes[0] == axis else 0] = pl.ds(2 * half, 2)
        return ref.at[tuple(where)]

    every = [0, 1, 2]
    core = []
    for n, (start, size, order) in enumerate(PARTS):
        src = counts if n == 0 else table.at[:, :, :, 1 - c, pl.ds(start, size), :]
        core.append(remote(src, held[n], core_sems.at[0, n], core_sems.at[1, n], other))

    sent = [[] for _ in PARTS]
    relay = [None] * N
    for n, (start, size, order) in enumerate(PARTS):
        core[n].wait()
        if n == 0:
            held[n][...] += counts[...]
        else:
            for a in range(4):
                held[n][a] += table[a, :, :, c, start : start + size, :]
        axis = order[0]

        def hop(slot, index, half, k):
            return remote(
                piece(held[n], every, axis, index, half), near[n].at[slot],
                near_send.at[n, slot], near_recv.at[n, slot], device(axis, k))

        relay[n] = [hop(0, position(axis, 2), 0, 1), hop(1, position(axis, 2), 1, 3)]
        sent[n] = [hop(2, position(axis, 1), 1, 1), hop(3, position(axis, 3), 0, 3)]
    for n, (start, size, order) in enumerate(PARTS):
        axis = order[0]
        for half, k in ((0, 1), (1, 3)):
            relay[n][half].wait()
            block = piece(held[n], every, axis, position(axis, k), half)
            block[...] += near[n][half]
            sent[n].append(remote(
                block, near[n].at[4 + half], near_send.at[n, 4 + half], near_recv.at[n, 4 + half], device(axis, k)))

    def spread(n, stage, source, axes, target):
        axis = PARTS[n][2][stage]
        return [
            remote(
                piece(source, axes, axis, position(axis, k)), target.at[k - 1],
                send.at[n, stage - 1, k - 1], recv.at[n, stage - 1, k - 1], device(axis, k))
            for k in (2, 1, 3)
        ]

    def summed(n, stage, source, axes, target):
        axis = PARTS[n][2][stage]
        return (piece(source, axes, axis, place[axis])[...] + target[0]) + (target[1] + target[2])

    for n, (start, size, order) in enumerate(PARTS):
        for copy in sent[n]:
            copy.wait()
        axis = order[0]
        middle[n][0:2] = (piece(held[n], every, axis, place[axis], 0)[...] + near[n][3]) + near[n][4]
        middle[n][2:4] = (piece(held[n], every, axis, place[axis], 1)[...] + near[n][2]) + near[n][5]
        sent[n] = spread(n, 1, middle[n], [a for a in every if a != axis], second[n])
    for n, (start, size, order) in enumerate(PARTS):
        for copy in sent[n]:
            copy.wait()
        axes = [a for a in every if a != order[0]]
        last[n][...] = summed(n, 1, middle[n], axes, second[n])
        sent[n] = spread(n, 2, last[n], [order[2]], third[n])
    for n, (start, size, order) in enumerate(PARTS):
        for copy in sent[n]:
            copy.wait()
        value = summed(n, 2, last[n], [order[2]], third[n])
        if n == 0:
            wide = jnp.transpose(jnp.broadcast_to(value, (128, 128)))
            total = jnp.maximum(jnp.where(c == 0, wide[:64], wide[64:]), 1.0)
            count_out[...] = jnp.broadcast_to(jnp.where(c == 0, value, pltpu.roll(value, 64, 1)), (8, 128))
        else:
            means[start : start + size, :] = value / total[start : start + size]


def reduce_to_owner(table, counts):
    buffers = []
    for lead in ((4, 4, 4), (6, 2, 4), (4, 4), (3, 4), (4,), (3,)):
        buffers += [pltpu.VMEM((*lead, size, D), f32) for _, size, _ in PARTS]
    return pl.pallas_call(
        reduce_kernel,
        out_shape=(jax.ShapeDtypeStruct((64, D), f32), jax.ShapeDtypeStruct((8, D), f32)),
        in_specs=[spec(VM), spec(VM)],
        out_specs=(spec(VM), spec(VM)),
        scratch_shapes=buffers + [
            pltpu.SemaphoreType.DMA((2, N)),
            pltpu.SemaphoreType.DMA((N, 6)),
            pltpu.SemaphoreType.DMA((N, 6)),
            pltpu.SemaphoreType.DMA((N, 2, 3)),
            pltpu.SemaphoreType.DMA((N, 2, 3)),
        ],
        compiler_params=pltpu.CompilerParams(collective_id=1, has_side_effects=True, vmem_limit_bytes=16 << 20),
    )(table.reshape(4, 4, 4, 2, 64, D), counts.reshape(4, 4, 4, 1, D))


def shards(rows_data, row_keys, valid_counts, predicates, section_weight, section_bias):
    w, b, same, level, counts, clear_a, clear_b, key_rows = exchange(
        section_weight, section_bias.reshape(1, 1, D), predicates.reshape(4, MICRO, 32), row_keys, valid_counts.T)
    table = sections(rows_data, key_rows, w, b, same, level, clear_a, clear_b)
    means, total = reduce_to_owner(table, counts)
    return means, total[0, :64]


def solution(mesh):
    placed = (
        P("section", "rows", None),
        P("section", "rows"),
        P("section", "rows"),
        P("section", None, "rows"),
        P("section", None, None),
        P("section", None),
    )
    return jax.shard_map(
        shards,
        mesh=mesh,
        in_specs=placed,
        out_specs=(P(("section", "rows"), None), P(("section", "rows"))),
        check_vma=False,
    )
```

```python
import functools

import jax
import jax.numpy as jnp
from jax import lax
from jax.experimental import pallas as pl
from jax.experimental.pallas import tpu as pltpu
from jax.sharding import PartitionSpec as P

KEYS = 8192
SECTIONS = 4
D = 128
MICRO = 4
BLOCK = 1024
ROWS = MICRO * BLOCK
GROUP = 8
CHUNK = 256
f32, bf16, i32 = jnp.float32, jnp.bfloat16, jnp.int32
MESH = pl.DeviceIdType.MESH
VM, SM, HB = pltpu.VMEM, pltpu.SMEM, pltpu.HBM


def spec(space):
    return pl.BlockSpec(memory_space=space)


def pinned(x):
    return pltpu.with_memory_space_constraint(x, HB)


def high_low(x):
    high = x.astype(bf16)
    return high, (x - high.astype(f32)).astype(bf16)


def exchange_kernel(
    w_in, b_in, p_in, k_in, v_in,
    w_all, b_all, same, level, lives, table_a, table_b, key_rows,
    keys, valid, words_v, words, send, recv, local,
):
    me = lax.axis_index("section")
    row = lax.axis_index("rows")
    own = [
        pltpu.make_async_copy(src, dst, local.at[n])
        for n, (src, dst) in enumerate((
            (k_in, keys), (v_in, valid), (p_in.at[me], words_v.at[me]),
            (b_in.at[0], b_all.at[me]), (w_in.at[0], w_all.at[me])))
    ]
    for copy in own:
        copy.start()
    barrier = pltpu.get_barrier_semaphore()
    for k in range(1, 4):
        pl.semaphore_signal(barrier, inc=1, device_id=(lax.rem(me + k, 4), row), device_id_type=MESH)

    def clear(i, carry):
        at = pl.ds(pl.multiple_of(i * 512, 512), 512)
        table_a[at, :] = jnp.zeros((512, D), f32)
        table_b[at, :] = jnp.zeros((512, D), f32)
        return carry

    lax.fori_loop(0, KEYS // 512, clear, 0)
    pl.semaphore_wait(barrier, 3)
    copies = []
    for n, k in enumerate((2, 1, 3)):
        to = lax.rem(me + k, 4)
        for a, (src, dst) in enumerate(
            ((p_in.at[to], words_v.at[me]), (b_in.at[0], b_all.at[me]), (w_in.at[0], w_all.at[me]))
        ):
            copies.append((a, pltpu.make_async_remote_copy(
                src_ref=src, dst_ref=dst, send_sem=send.at[n, a], recv_sem=recv.at[n, a],
                device_id=(to, row), device_id_type=MESH)))
    for a in range(3):
        for which, copy in copies:
            if which == a:
                copy.start()
    own[0].wait()
    own[1].wait()
    group_i = (lax.broadcasted_iota(i32, (1, 128), 1) // GROUP) * KEYS

    for m in range(MICRO):
        for j in range(8):
            key_rows[m * 8 + j : m * 8 + j + 1, :] = keys[m : m + 1, j * 128 : (j + 1) * 128]

    def key_row_at(m, j):
        return key_rows[pl.ds(m * 8 + j, 1), :]

    def sameness(i, carry):
        for u in range(4):
            key_row = key_row_at(i // 2, (i % 2) * 4 + u) + group_i
            key_col = jnp.transpose(jnp.broadcast_to(key_row, (128, 128)))
            same[i * 4 + u] = jnp.where(key_col == key_row, 1.0, 0.0).astype(bf16)
        return carry

    lax.fori_loop(0, 8, sameness, 0)
    own[2].wait()
    for which, copy in copies:
        if which == 0:
            copy.wait()
    to_scalar = pltpu.make_async_copy(words_v, words, local.at[5])
    to_scalar.start()
    to_scalar.wait()
    lane = lax.broadcasted_iota(i32, (8, 128), 1)

    def tally(i, carry):
        m = i // 2
        nv = valid[0, m]
        for u in range(4):
            j = (i % 2) * 4 + u
            total = jnp.zeros((8, 128), i32)
            alive = []
            for w in range(4):
                n = nv - (j * 4 + w) * 32
                alive.append(jnp.where(n >= 32, jnp.int32(-1), (jnp.int32(1) << jnp.clip(n, 0, 31)) - 1))
            for s in range(SECTIONS):
                alive = [a & words[s, m, j * 4 + w] for w, a in enumerate(alive)]
                v = jnp.where(
                    lane < 64,
                    jnp.where(lane < 32, alive[0], alive[1]),
                    jnp.where(lane < 96, alive[2], alive[3]))
                total = total + ((v >> (lane & 31)) & 1)
            lives[pl.ds(i * 4 + u, 1), :] = total[:1]
            level[i * 4 + u] = jnp.transpose(jnp.concatenate([total] * 16, axis=0))
        return carry

    lax.fori_loop(0, 8, tally, 0)
    own[3].wait()
    own[4].wait()
    for which, copy in copies:
        if which != 0:
            copy.wait()


def exchange(weight, bias, predicates, keys, valid):
    return pl.pallas_call(
        exchange_kernel,
        out_shape=(
            jax.ShapeDtypeStruct((4, D, D), f32),
            jax.ShapeDtypeStruct((4, 1, D), f32),
            jax.ShapeDtypeStruct((32, 128, 128), bf16),
            jax.ShapeDtypeStruct((32, 128, 128), i32),
            jax.ShapeDtypeStruct((32, 128), i32),
            jax.ShapeDtypeStruct((KEYS, D), f32),
            jax.ShapeDtypeStruct((KEYS, D), f32),
            jax.ShapeDtypeStruct((32, 128), i32),
        ),
        in_specs=[spec(HB)] * 5,
        out_specs=(spec(VM),) * 8,
        scratch_shapes=[
            pltpu.VMEM((MICRO, BLOCK), i32),
            pltpu.SMEM((1, MICRO), i32),
            pltpu.VMEM((4, 4, 32), i32),
            pltpu.SMEM((4, 4, 32), i32),
            pltpu.SemaphoreType.DMA((3, 3)),
            pltpu.SemaphoreType.DMA((3, 3)),
            pltpu.SemaphoreType.DMA((6,)),
        ],
        compiler_params=pltpu.CompilerParams(collective_id=0, has_side_effects=True, vmem_limit_bytes=8 << 20),
        cost_estimate=pl.CostEstimate(flops=40_000_000_000, bytes_accessed=1 << 20, transcendentals=0),
    )(pinned(weight), pinned(bias), pinned(predicates), pinned(keys), pinned(valid))


def sections_kernel(rows, keys_in, w, b, same, level, clear_a, clear_b, table_a, table_b, w2, ready, keys, sem):
    fetch = pltpu.make_async_copy(keys_in, keys, sem)
    fetch.start()
    for s in range(SECTIONS):
        top = jnp.concatenate(high_low(w[s]), axis=1)
        w2[s] = jnp.concatenate([top, top], axis=0)

    def batch(m, carry):
        h = rows[m]
        alive = level[pl.ds(m * 8, 8)].reshape(BLOCK, 128)
        total = jnp.zeros((BLOCK, D), f32)
        for s in range(SECTIONS):
            p = jnp.dot(jnp.concatenate(high_low(h), axis=1), w2[s], preferred_element_type=f32)
            h = h + jnp.tanh(p[:, :D] + (p[:, D:] + b[s]))
            total = total + jnp.where(alive > s, h, 0.0)
        both = jnp.concatenate(high_low(total), axis=1)
        for j in range(8):
            p = jnp.dot(same[m * 8 + j], both[j * 128 : (j + 1) * 128], preferred_element_type=f32)
            ready[pl.ds(pl.multiple_of(m * BLOCK + j * 128, 128), 128), :] = p[:, :D] + p[:, D:]
        return carry

    lax.fori_loop(0, MICRO, batch, 0)
    fetch.wait()
    tables = (table_a, table_b)
    groups = CHUNK // GROUP

    def scatter(u, carry):
        def load(g):
            at = [keys[u * (CHUNK // 128) + (g * GROUP + i) // 128, (g * GROUP + i) % 128] for i in range(GROUP)]
            return at, [tables[g % 2][pl.ds(k, 1), :] for k in at]

        def store(g, at, held):
            for i, k in enumerate(at):
                tables[g % 2][pl.ds(k, 1), :] = held[i] + ready[pl.ds(u * CHUNK + g * GROUP + i, 1), :]

        flying = {g: load(g) for g in range(2)}
        for g in range(groups):
            store(g, *flying.pop(g))
            if g + 2 < groups:
                flying[g + 2] = load(g + 2)
        return carry

    lax.fori_loop(0, ROWS // CHUNK, scatter, 0)


def sections(rows, keys, w, b, same, level, clear_a, clear_b):
    return pl.pallas_call(
        sections_kernel,
        out_shape=(jax.ShapeDtypeStruct((KEYS, D), f32),) * 2,
        in_specs=[spec(VM)] * 8,
        out_specs=(spec(VM),) * 2,
        scratch_shapes=[
            pltpu.VMEM((SECTIONS, 256, 256), bf16),
            pltpu.VMEM((ROWS, D), f32),
            pltpu.SMEM((32, 128), i32),
            pltpu.SemaphoreType.DMA,
        ],
        input_output_aliases={6: 0, 7: 1},
        compiler_params=pltpu.CompilerParams(vmem_limit_bytes=12 << 20),
    )(rows, keys, w, b, same, level, clear_a, clear_b)


PARTS = (
    (0, 1, (2, 0, 1)),
    (0, 8, (0, 1, 2)), (8, 8, (1, 2, 0)), (16, 8, (2, 0, 1)),
    (24, 8, (0, 1, 2)), (32, 8, (1, 2, 0)), (40, 8, (2, 0, 1)),
    (48, 8, (0, 1, 2)), (56, 8, (1, 2, 0)),
)
TURNS = (
    (0, 0), (0, 1), (0, 2), (0, 3), (0, 4), (0, 5), (0, 6), (0, 7), (0, 8), (1, 0), (1, 1), (1, 2),
    (1, 3), (1, 4), (1, 5), (1, 6), (1, 7), (1, 8), (2, 0), (2, 1), (2, 2), (2, 3), (2, 4), (2, 5),
    (2, 6), (2, 7), (2, 8), (3, 0), (3, 1), (3, 2), (3, 3), (3, 4), (3, 5), (3, 6), (3, 7), (3, 8),
    (4, 0), (4, 1), (4, 2), (4, 3), (4, 4), (4, 5), (4, 6), (4, 7), (4, 8),
)
N = len(PARTS)


def reduce_kernel(table_a, table_b, keys, lives, means, count_out, table, counts, *scratch):
    held, near, middle, second, last, third = (scratch[i * N : (i + 1) * N] for i in range(6))
    core_sems, near_send, near_recv, send, recv = scratch[6 * N :]
    z = lax.axis_index("section")
    row = lax.axis_index("rows")
    y, x, c = row // 8, (row // 2) % 4, row % 2
    place = (z, y, x)

    def position(axis, k):
        return lax.rem(place[axis] + k, 4)

    def device(axis, k):
        at = list(place)
        at[axis] = position(axis, k)
        return (at[0], at[1] * 8 + at[2] * 2 + c)

    other = (z, y * 8 + x * 2 + (1 - c))
    peers = [device(axis, k) for axis in range(3) for k in (1, 3)] + [other]
    barrier = pltpu.get_barrier_semaphore()
    for peer in peers:
        pl.semaphore_signal(barrier, inc=1, device_id=peer, device_id_type=MESH)

    def join(i, carry):
        at = (i // 16, (i // 4) % 4, i % 4)
        table[at] = table_a[at] + table_b[at]
        return carry

    lax.fori_loop(0, 64, join, 0)
    sub64 = lax.broadcasted_iota(i32, (64, 128), 0)
    sub128 = lax.broadcasted_iota(i32, (128, 128), 0)

    def tally(i, found):
        for u in range(4):
            key_row = keys[pl.ds(i * 4 + u, 1), :]
            alive = lives[pl.ds(i * 4 + u, 1), :].astype(f32)
            high = jnp.where((key_row >> 7) == sub64, alive, 0.0).astype(bf16)
            low = jnp.where((key_row & 127) == sub128, 1.0, 0.0).astype(bf16)
            found = found + lax.dot_general(high, low, (((1,), (1,)), ((), ())), preferred_element_type=f32)
        return found

    found = lax.fori_loop(0, 8, tally, jnp.zeros((64, 128), f32))
    for i in range(64):
        counts[i // 16, (i // 4) % 4, i % 4] = found[i : i + 1]
    pl.semaphore_wait(barrier, len(peers))

    def remote(src, dst, send_sem, recv_sem, to):
        copy = pltpu.make_async_remote_copy(
            src_ref=src, dst_ref=dst, send_sem=send_sem, recv_sem=recv_sem, device_id=to, device_id_type=MESH)
        copy.start()
        return copy

    def piece(ref, axes, axis, index, half=None):
        where = [slice(None)] * len(axes)
        where[axes.index(axis)] = index
        if half is not None:
            where[1 if axes[0] == axis else 0] = pl.ds(2 * half, 2)
        return ref.at[tuple(where)]

    def spread(n, stage, source, axes, target):
        axis = PARTS[n][2][stage]
        return [
            remote(
                piece(source, axes, axis, position(axis, k)), target.at[k - 1],
                send.at[n, stage - 1, k - 1], recv.at[n, stage - 1, k - 1], device(axis, k))
            for k in (2, 1, 3)
        ]

    def summed(n, stage, source, axes, target):
        axis = PARTS[n][2][stage]
        return (piece(source, axes, axis, place[axis])[...] + target[0]) + (target[1] + target[2])

    every = [0, 1, 2]
    core = []
    for n, (start, size, order) in enumerate(PARTS):
        src = counts if n == 0 else table.at[:, :, :, 1 - c, pl.ds(start, size), :]
        core.append(remote(src, held[n], core_sems.at[0, n], core_sems.at[1, n], other))
    sent = [[] for _ in PARTS]
    relay = [None] * N
    total = None
    for turn, n in TURNS:
        start, size, order = PARTS[n]
        axis = order[0]

        def hop(slot, index, half, k):
            return remote(
                piece(held[n], every, axis, index, half), near[n].at[slot],
                near_send.at[n, slot], near_recv.at[n, slot], device(axis, k))

        if turn == 0:
            core[n].wait()
            if n == 0:
                held[n][...] += counts[...]
            else:
                for i in range(4):
                    held[n][i] += table[i, :, :, c, start : start + size, :]
            relay[n] = [hop(0, position(axis, 2), 0, 1), hop(1, position(axis, 2), 1, 3)]
            sent[n] = [hop(2, position(axis, 1), 1, 1), hop(3, position(axis, 3), 0, 3)]
        elif turn == 1:
            for half, k in ((0, 1), (1, 3)):
                relay[n][half].wait()
                block = piece(held[n], every, axis, position(axis, k), half)
                block[...] += near[n][half]
                sent[n].append(hop(4 + half, position(axis, k), half, k))
        else:
            for copy in sent[n]:
                copy.wait()
            axes = [i for i in every if i != axis]
            if turn == 2:
                middle[n][0:2] = (piece(held[n], every, axis, place[axis], 0)[...] + near[n][3]) + near[n][4]
                middle[n][2:4] = (piece(held[n], every, axis, place[axis], 1)[...] + near[n][2]) + near[n][5]
                sent[n] = spread(n, 1, middle[n], axes, second[n])
            elif turn == 3:
                last[n][...] = summed(n, 1, middle[n], axes, second[n])
                sent[n] = spread(n, 2, last[n], [order[2]], third[n])
            else:
                value = summed(n, 2, last[n], [order[2]], third[n])
                if n == 0:
                    wide = jnp.transpose(jnp.broadcast_to(value, (128, 128)))
                    total = jnp.maximum(jnp.where(c == 0, wide[:64], wide[64:]), 1.0)
                    count_out[...] = jnp.broadcast_to(jnp.where(c == 0, value, pltpu.roll(value, 64, 1)), (8, 128))
                else:
                    means[start : start + size, :] = value / total[start : start + size]


def reduce_to_owner(table_a, table_b, keys, lives):
    buffers = [pltpu.VMEM((4, 4, 4, 2, 64, D), f32), pltpu.VMEM((4, 4, 4, 1, D), f32)]
    for lead in ((4, 4, 4), (6, 2, 4), (4, 4), (3, 4), (4,), (3,)):
        buffers += [pltpu.VMEM((*lead, size, D), f32) for _, size, _ in PARTS]
    return pl.pallas_call(
        reduce_kernel,
        out_shape=(jax.ShapeDtypeStruct((64, D), f32), jax.ShapeDtypeStruct((8, D), f32)),
        in_specs=[spec(VM)] * 4,
        out_specs=(spec(VM), spec(VM)),
        scratch_shapes=buffers + [
            pltpu.SemaphoreType.DMA((2, N)),
            pltpu.SemaphoreType.DMA((N, 6)),
            pltpu.SemaphoreType.DMA((N, 6)),
            pltpu.SemaphoreType.DMA((N, 2, 3)),
            pltpu.SemaphoreType.DMA((N, 2, 3)),
        ],
        compiler_params=pltpu.CompilerParams(collective_id=1, has_side_effects=True, vmem_limit_bytes=20 << 20),
    )(table_a.reshape(4, 4, 4, 2, 64, D), table_b.reshape(4, 4, 4, 2, 64, D), keys, lives)


def shards(rows_data, row_keys, valid_counts, predicates, section_weight, section_bias):
    w, b, same, level, lives, clear_a, clear_b, key_rows = exchange(
        section_weight, section_bias.reshape(1, 1, D), predicates.reshape(4, MICRO, 32), row_keys, valid_counts.T)
    tables = sections(rows_data, key_rows, w, b, same, level, clear_a, clear_b)
    means, total = reduce_to_owner(*tables, key_rows, lives)
    return means, total[0, :64]


def solution(mesh):
    placed = (
        P("section", "rows", None),
        P("section", "rows"),
        P("section", "rows"),
        P("section", None, "rows"),
        P("section", None, None),
        P("section", None),
    )
    return jax.shard_map(
        shards,
        mesh=mesh,
        in_specs=placed,
        out_specs=(P(("section", "rows"), None), P(("section", "rows"))),
        check_vma=False,
    )
```

```python
import functools

import jax
import jax.numpy as jnp
from jax import lax
from jax.experimental import pallas as pl
from jax.experimental.pallas import tpu as pltpu
from jax.sharding import PartitionSpec as P

KEYS = 8192
SECTIONS = 4
D = 128
MICRO = 4
BLOCK = 1024
ROWS = MICRO * BLOCK
GROUP = 8
CHUNK = 256
f32, bf16, i32 = jnp.float32, jnp.bfloat16, jnp.int32
MESH = pl.DeviceIdType.MESH
VM, SM, HB = pltpu.VMEM, pltpu.SMEM, pltpu.HBM


def spec(space):
    return pl.BlockSpec(memory_space=space)


def pinned(x):
    return pltpu.with_memory_space_constraint(x, HB)


def high_low(x):
    high = x.astype(bf16)
    return high, (x - high.astype(f32)).astype(bf16)


def exchange_kernel(
    w_in, b_in, p_in, k_in, v_in,
    w_all, b_all, same, level, lives, table_a, table_b, key_rows,
    keys, valid, flags, words_v, words, send, recv, pair_send, pair_recv, local,
):
    me = lax.axis_index("section")
    row = lax.axis_index("rows")
    c = row % 2
    other = (me, row + 1 - 2 * c)
    own = [
        pltpu.make_async_copy(src, dst, local.at[n])
        for n, (src, dst) in enumerate((
            (p_in, flags), (p_in.at[me], words_v.at[me]), (b_in.at[0], b_all.at[me]), (w_in.at[0], w_all.at[me]),
            (k_in, keys), (v_in, valid)))
    ]
    for copy in own:
        copy.start()
    barrier = pltpu.get_barrier_semaphore()
    for k in range(1, 4):
        pl.semaphore_signal(barrier, inc=1, device_id=(lax.rem(me + k, 4), row), device_id_type=MESH)
    pl.semaphore_signal(barrier, inc=1, device_id=other, device_id_type=MESH)

    def clear(i, carry):
        at = pl.ds(pl.multiple_of(i * 512, 512), 512)
        table_a[at, :] = jnp.zeros((512, D), f32)
        table_b[at, :] = jnp.zeros((512, D), f32)
        return carry

    lax.fori_loop(0, KEYS // 512, clear, 0)
    for copy in own[:4]:
        copy.wait()
    pl.semaphore_wait(barrier, 4)
    half = pl.ds(pl.multiple_of(c * 64, 64), 64)
    copies = []
    for n, k in enumerate((2, 1, 3)):
        to = lax.rem(me + k, 4)
        for a, (src, dst) in enumerate((
            (flags.at[to], words_v.at[me]), (w_all.at[me, half], w_all.at[me, half]), (b_all.at[me], b_all.at[me]),
        )):
            copies.append((a, pltpu.make_async_remote_copy(
                src_ref=src, dst_ref=dst, send_sem=send.at[n, a], recv_sem=recv.at[n, a],
                device_id=(to, row), device_id_type=MESH)))
    for a in range(3):
        for which, copy in copies:
            if which == a:
                copy.start()
    own[4].wait()
    own[5].wait()
    group_i = (lax.broadcasted_iota(i32, (1, 128), 1) // GROUP) * KEYS

    for m in range(MICRO):
        for j in range(8):
            key_rows[m * 8 + j : m * 8 + j + 1, :] = keys[m : m + 1, j * 128 : (j + 1) * 128]

    def key_row_at(m, j):
        return key_rows[pl.ds(m * 8 + j, 1), :]

    def sameness(i, carry):
        for u in range(4):
            key_row = key_row_at(i // 2, (i % 2) * 4 + u) + group_i
            key_col = jnp.transpose(jnp.broadcast_to(key_row, (128, 128)))
            same[i * 4 + u] = jnp.where(key_col == key_row, 1.0, 0.0).astype(bf16)
        return carry

    lax.fori_loop(0, 8, sameness, 0)
    for which, copy in copies:
        if which == 0:
            copy.wait()
    to_scalar = pltpu.make_async_copy(words_v, words, local.at[6])
    to_scalar.start()
    passed = []
    for n, k in enumerate((2, 1, 3)):
        origin = lax.rem(me + 4 - k, 4)
        copies[3 * n + 1][1].wait()
        block = w_all.at[origin, half]
        copy = pltpu.make_async_remote_copy(
            src_ref=block, dst_ref=block, send_sem=pair_send.at[n], recv_sem=pair_recv.at[n],
            device_id=other, device_id_type=MESH)
        copy.start()
        passed.append(copy)
    to_scalar.wait()
    lane = lax.broadcasted_iota(i32, (8, 128), 1)

    def tally(i, carry):
        m = i // 2
        nv = valid[0, m]
        for u in range(4):
            j = (i % 2) * 4 + u
            total = jnp.zeros((8, 128), i32)
            alive = []
            for w in range(4):
                n = nv - (j * 4 + w) * 32
                alive.append(jnp.where(n >= 32, jnp.int32(-1), (jnp.int32(1) << jnp.clip(n, 0, 31)) - 1))
            for s in range(SECTIONS):
                alive = [a & words[s, m, j * 4 + w] for w, a in enumerate(alive)]
                v = jnp.where(
                    lane < 64,
                    jnp.where(lane < 32, alive[0], alive[1]),
                    jnp.where(lane < 96, alive[2], alive[3]))
                total = total + ((v >> (lane & 31)) & 1)
            lives[pl.ds(i * 4 + u, 1), :] = total[:1]
            level[i * 4 + u] = jnp.transpose(jnp.concatenate([total] * 16, axis=0))
        return carry

    lax.fori_loop(0, 8, tally, 0)
    for which, copy in copies:
        if which == 2:
            copy.wait()
    for copy in passed:
        copy.wait()


def exchange(weight, bias, predicates, keys, valid):
    return pl.pallas_call(
        exchange_kernel,
        out_shape=(
            jax.ShapeDtypeStruct((4, D, D), f32),
            jax.ShapeDtypeStruct((4, 1, D), f32),
            jax.ShapeDtypeStruct((32, 128, 128), bf16),
            jax.ShapeDtypeStruct((32, 128, 128), i32),
            jax.ShapeDtypeStruct((32, 128), i32),
            jax.ShapeDtypeStruct((KEYS, D), f32),
            jax.ShapeDtypeStruct((KEYS, D), f32),
            jax.ShapeDtypeStruct((32, 128), i32),
        ),
        in_specs=[spec(HB)] * 5,
        out_specs=(spec(VM),) * 8,
        scratch_shapes=[
            pltpu.VMEM((MICRO, BLOCK), i32),
            pltpu.SMEM((1, MICRO), i32),
            pltpu.VMEM((4, 4, 32), i32),
            pltpu.VMEM((4, 4, 32), i32),
            pltpu.SMEM((4, 4, 32), i32),
            pltpu.SemaphoreType.DMA((3, 3)),
            pltpu.SemaphoreType.DMA((3, 3)),
            pltpu.SemaphoreType.DMA((3,)),
            pltpu.SemaphoreType.DMA((3,)),
            pltpu.SemaphoreType.DMA((7,)),
        ],
        compiler_params=pltpu.CompilerParams(collective_id=0, has_side_effects=True, vmem_limit_bytes=8 << 20),
        cost_estimate=pl.CostEstimate(flops=40_000_000_000, bytes_accessed=1 << 20, transcendentals=0),
    )(pinned(weight), pinned(bias), pinned(predicates), pinned(keys), pinned(valid))


def sections_kernel(
    rows, keys_in, w, b, same, level, clear_a, clear_b, v_in, table_a, table_b, w2, ready, keys, valid, sems
):
    fetch = [pltpu.make_async_copy(keys_in, keys, sems.at[0]), pltpu.make_async_copy(v_in, valid, sems.at[1])]
    for copy in fetch:
        copy.start()
    for s in range(SECTIONS):
        top = jnp.concatenate(high_low(w[s]), axis=1)
        w2[s] = jnp.concatenate([top, top], axis=0)

    def batch(m, carry):
        h = rows[m]
        alive = level[pl.ds(m * 8, 8)].reshape(BLOCK, 128)
        total = jnp.zeros((BLOCK, D), f32)
        for s in range(SECTIONS):
            p = jnp.dot(jnp.concatenate(high_low(h), axis=1), w2[s], preferred_element_type=f32)
            h = h + jnp.tanh(p[:, :D] + (p[:, D:] + b[s]))
            total = total + jnp.where(alive > s, h, 0.0)
        both = jnp.concatenate(high_low(total), axis=1)
        for j in range(8):
            p = jnp.dot(same[m * 8 + j], both[j * 128 : (j + 1) * 128], preferred_element_type=f32)
            ready[pl.ds(pl.multiple_of(m * BLOCK + j * 128, 128), 128), :] = p[:, :D] + p[:, D:]
        return carry

    lax.fori_loop(0, MICRO, batch, 0)
    for copy in fetch:
        copy.wait()
    tables = (table_a, table_b)
    groups = CHUNK // GROUP

    def scatter(first, i, carry):
        u = first + i
        def load(g):
            at = [keys[u * (CHUNK // 128) + (g * GROUP + i) // 128, (g * GROUP + i) % 128] for i in range(GROUP)]
            return at, [tables[g % 2][pl.ds(k, 1), :] for k in at]

        def store(g, at, held):
            for i, k in enumerate(at):
                tables[g % 2][pl.ds(k, 1), :] = held[i] + ready[pl.ds(u * CHUNK + g * GROUP + i, 1), :]

        flying = {g: load(g) for g in range(2)}
        for g in range(groups):
            store(g, *flying.pop(g))
            if g + 2 < groups:
                flying[g + 2] = load(g + 2)
        return carry

    for m in range(MICRO):
        chunks = (valid[0, m] + CHUNK - 1) // CHUNK
        lax.fori_loop(0, chunks, functools.partial(scatter, m * (BLOCK // CHUNK)), 0)


def sections(rows, keys, w, b, same, level, clear_a, clear_b, valid):
    return pl.pallas_call(
        sections_kernel,
        out_shape=(jax.ShapeDtypeStruct((KEYS, D), f32),) * 2,
        in_specs=[spec(VM)] * 8 + [spec(HB)],
        out_specs=(spec(VM),) * 2,
        scratch_shapes=[
            pltpu.VMEM((SECTIONS, 256, 256), bf16),
            pltpu.VMEM((ROWS, D), f32),
            pltpu.SMEM((32, 128), i32),
            pltpu.SMEM((1, MICRO), i32),
            pltpu.SemaphoreType.DMA((2,)),
        ],
        input_output_aliases={6: 0, 7: 1},
        compiler_params=pltpu.CompilerParams(vmem_limit_bytes=12 << 20),
    )(rows, keys, w, b, same, level, clear_a, clear_b, pinned(valid))


PARTS = (
    (0, 1, (2, 0, 1)),
    (0, 8, (0, 1, 2)), (8, 8, (1, 2, 0)), (16, 8, (2, 0, 1)),
    (24, 8, (0, 1, 2)), (32, 8, (1, 2, 0)), (40, 8, (2, 0, 1)),
    (48, 8, (0, 1, 2)), (56, 8, (1, 2, 0)),
)
TURNS = (
    (0, 0), (0, 1), (0, 2), (0, 3), (0, 4), (0, 5), (0, 6), (0, 7), (0, 8), (1, 0), (1, 1), (1, 2),
    (1, 3), (1, 4), (1, 5), (1, 6), (1, 7), (1, 8), (2, 0), (2, 1), (2, 2), (2, 3), (2, 4), (2, 5),
    (2, 6), (2, 7), (2, 8), (3, 0), (3, 1), (3, 2), (3, 3), (3, 4), (3, 5), (3, 6), (3, 7), (3, 8),
    (4, 0), (4, 1), (4, 2), (4, 3), (4, 4), (4, 5), (4, 6), (4, 7), (4, 8),
)
N = len(PARTS)


def reduce_kernel(table_a, table_b, keys, lives, means, count_out, table, counts, *scratch):
    held, near, middle, second, last, third = (scratch[i * N : (i + 1) * N] for i in range(6))
    core_sems, near_send, near_recv, send, recv = scratch[6 * N :]
    z = lax.axis_index("section")
    row = lax.axis_index("rows")
    y, x, c = row // 8, (row // 2) % 4, row % 2
    place = (z, y, x)

    def position(axis, k):
        return lax.rem(place[axis] + k, 4)

    def device(axis, k):
        at = list(place)
        at[axis] = position(axis, k)
        return (at[0], at[1] * 8 + at[2] * 2 + c)

    other = (z, y * 8 + x * 2 + (1 - c))
    peers = [device(axis, k) for axis in range(3) for k in (1, 3)] + [other]
    barrier = pltpu.get_barrier_semaphore()
    for peer in peers:
        pl.semaphore_signal(barrier, inc=1, device_id=peer, device_id_type=MESH)

    def join(i, carry):
        at = (i // 16, (i // 4) % 4, i % 4)
        table[at] = table_a[at] + table_b[at]
        return carry

    lax.fori_loop(0, 64, join, 0)
    sub64 = lax.broadcasted_iota(i32, (64, 128), 0)
    sub128 = lax.broadcasted_iota(i32, (128, 128), 0)

    def tally(i, found):
        for u in range(4):
            key_row = keys[pl.ds(i * 4 + u, 1), :]
            alive = lives[pl.ds(i * 4 + u, 1), :].astype(f32)
            high = jnp.where((key_row >> 7) == sub64, alive, 0.0).astype(bf16)
            low = jnp.where((key_row & 127) == sub128, 1.0, 0.0).astype(bf16)
            found = found + lax.dot_general(high, low, (((1,), (1,)), ((), ())), preferred_element_type=f32)
        return found

    found = lax.fori_loop(0, 8, tally, jnp.zeros((64, 128), f32))
    for i in range(64):
        counts[i // 16, (i // 4) % 4, i % 4] = found[i : i + 1]
    pl.semaphore_wait(barrier, len(peers))

    def remote(src, dst, send_sem, recv_sem, to):
        copy = pltpu.make_async_remote_copy(
            src_ref=src, dst_ref=dst, send_sem=send_sem, recv_sem=recv_sem, device_id=to, device_id_type=MESH)
        copy.start()
        return copy

    def piece(ref, axes, axis, index, half=None):
        where = [slice(None)] * len(axes)
        where[axes.index(axis)] = index
        if half is not None:
            where[1 if axes[0] == axis else 0] = pl.ds(2 * half, 2)
        return ref.at[tuple(where)]

    def spread(n, stage, source, axes, target):
        axis = PARTS[n][2][stage]
        return [
            remote(
                piece(source, axes, axis, position(axis, k)), target.at[k - 1],
                send.at[n, stage - 1, k - 1], recv.at[n, stage - 1, k - 1], device(axis, k))
            for k in (2, 1, 3)
        ]

    def summed(n, stage, source, axes, target):
        axis = PARTS[n][2][stage]
        return (piece(source, axes, axis, place[axis])[...] + target[0]) + (target[1] + target[2])

    every = [0, 1, 2]
    core = []
    for n, (start, size, order) in enumerate(PARTS):
        src = counts if n == 0 else table.at[:, :, :, 1 - c, pl.ds(start, size), :]
        core.append(remote(src, held[n], core_sems.at[0, n], core_sems.at[1, n], other))
    sent = [[] for _ in PARTS]
    relay = [None] * N
    total = None
    for turn, n in TURNS:
        start, size, order = PARTS[n]
        axis = order[0]

        def hop(slot, index, half, k):
            return remote(
                piece(held[n], every, axis, index, half), near[n].at[slot],
                near_send.at[n, slot], near_recv.at[n, slot], device(axis, k))

        if turn == 0:
            core[n].wait()
            if n == 0:
                held[n][...] += counts[...]
            else:
                for i in range(4):
                    held[n][i] += table[i, :, :, c, start : start + size, :]
            relay[n] = [hop(0, position(axis, 2), 0, 1), hop(1, position(axis, 2), 1, 3)]
            sent[n] = [hop(2, position(axis, 1), 1, 1), hop(3, position(axis, 3), 0, 3)]
        elif turn == 1:
            for half, k in ((0, 1), (1, 3)):
                relay[n][half].wait()
                block = piece(held[n], every, axis, position(axis, k), half)
                block[...] += near[n][half]
                sent[n].append(hop(4 + half, position(axis, k), half, k))
        else:
            for copy in sent[n]:
                copy.wait()
            axes = [i for i in every if i != axis]
            if turn == 2:
                middle[n][0:2] = (piece(held[n], every, axis, place[axis], 0)[...] + near[n][3]) + near[n][4]
                middle[n][2:4] = (piece(held[n], every, axis, place[axis], 1)[...] + near[n][2]) + near[n][5]
                sent[n] = spread(n, 1, middle[n], axes, second[n])
            elif turn == 3:
                last[n][...] = summed(n, 1, middle[n], axes, second[n])
                sent[n] = spread(n, 2, last[n], [order[2]], third[n])
            else:
                value = summed(n, 2, last[n], [order[2]], third[n])
                if n == 0:
                    wide = jnp.transpose(jnp.broadcast_to(value, (128, 128)))
                    total = jnp.maximum(jnp.where(c == 0, wide[:64], wide[64:]), 1.0)
                    count_out[...] = jnp.broadcast_to(jnp.where(c == 0, value, pltpu.roll(value, 64, 1)), (8, 128))
                else:
                    means[start : start + size, :] = value / total[start : start + size]


def reduce_to_owner(table_a, table_b, keys, lives):
    buffers = [pltpu.VMEM((4, 4, 4, 2, 64, D), f32), pltpu.VMEM((4, 4, 4, 1, D), f32)]
    for lead in ((4, 4, 4), (6, 2, 4), (4, 4), (3, 4), (4,), (3,)):
        buffers += [pltpu.VMEM((*lead, size, D), f32) for _, size, _ in PARTS]
    return pl.pallas_call(
        reduce_kernel,
        out_shape=(jax.ShapeDtypeStruct((64, D), f32), jax.ShapeDtypeStruct((8, D), f32)),
        in_specs=[spec(VM)] * 4,
        out_specs=(spec(VM), spec(VM)),
        scratch_shapes=buffers + [
            pltpu.SemaphoreType.DMA((2, N)),
            pltpu.SemaphoreType.DMA((N, 6)),
            pltpu.SemaphoreType.DMA((N, 6)),
            pltpu.SemaphoreType.DMA((N, 2, 3)),
            pltpu.SemaphoreType.DMA((N, 2, 3)),
        ],
        compiler_params=pltpu.CompilerParams(collective_id=1, has_side_effects=True, vmem_limit_bytes=20 << 20),
    )(table_a.reshape(4, 4, 4, 2, 64, D), table_b.reshape(4, 4, 4, 2, 64, D), keys, lives)


def shards(rows_data, row_keys, valid_counts, predicates, section_weight, section_bias):
    w, b, same, level, lives, clear_a, clear_b, key_rows = exchange(
        section_weight, section_bias.reshape(1, 1, D), predicates.reshape(4, MICRO, 32), row_keys, valid_counts.T)
    tables = sections(rows_data, key_rows, w, b, same, level, clear_a, clear_b, valid_counts.T)
    means, total = reduce_to_owner(*tables, key_rows, lives)
    return means, total[0, :64]


def solution(mesh):
    placed = (
        P("section", "rows", None),
        P("section", "rows"),
        P("section", "rows"),
        P("section", None, "rows"),
        P("section", None, None),
        P("section", None),
    )
    return jax.shard_map(
        shards,
        mesh=mesh,
        in_specs=placed,
        out_specs=(P(("section", "rows"), None), P(("section", "rows"))),
        check_vma=False,
    )
```

```python
import functools

import jax
import jax.numpy as jnp
from jax import lax
from jax.experimental import pallas as pl
from jax.experimental.pallas import tpu as pltpu
from jax.sharding import PartitionSpec as P

KEYS = 8192
SECTIONS = 4
D = 128
MICRO = 4
BLOCK = 1024
ROWS = MICRO * BLOCK
GROUP = 8
CHUNK = 256
f32, bf16, i32 = jnp.float32, jnp.bfloat16, jnp.int32
MESH = pl.DeviceIdType.MESH
VM, SM, HB = pltpu.VMEM, pltpu.SMEM, pltpu.HBM


def spec(space):
    return pl.BlockSpec(memory_space=space)


def pinned(x):
    return pltpu.with_memory_space_constraint(x, HB)


def high_low(x):
    high = x.astype(bf16)
    return high, (x - high.astype(f32)).astype(bf16)


def exchange_kernel(
    w_in, b_in, p_in, k_in, v_in,
    w_all, b_all, same, level, lives, table_a, table_b, key_rows,
    keys, valid, flags, words_v, words, send, recv, pair_send, pair_recv, local,
):
    me = lax.axis_index("section")
    row = lax.axis_index("rows")
    c = row % 2
    other = (me, row + 1 - 2 * c)
    own = [
        pltpu.make_async_copy(src, dst, local.at[n])
        for n, (src, dst) in enumerate((
            (p_in, flags), (p_in.at[me], words_v.at[me]), (b_in.at[0], b_all.at[me]), (w_in.at[0], w_all.at[me]),
            (k_in, keys), (v_in, valid)))
    ]
    for copy in own:
        copy.start()
    barrier = pltpu.get_barrier_semaphore()
    for k in range(1, 4):
        pl.semaphore_signal(barrier, inc=1, device_id=(lax.rem(me + k, 4), row), device_id_type=MESH)
    pl.semaphore_signal(barrier, inc=1, device_id=other, device_id_type=MESH)

    def clear(i, carry):
        at = pl.ds(pl.multiple_of(i * 512, 512), 512)
        table_a[at, :] = jnp.zeros((512, D), f32)
        table_b[at, :] = jnp.zeros((512, D), f32)
        return carry

    lax.fori_loop(0, KEYS // 512, clear, 0)
    for copy in own[:4]:
        copy.wait()
    pl.semaphore_wait(barrier, 4)
    half = pl.ds(pl.multiple_of(c * 64, 64), 64)
    copies = []
    for n, k in enumerate((2, 1, 3)):
        to = lax.rem(me + k, 4)
        for a, (src, dst) in enumerate((
            (flags.at[to], words_v.at[me]), (w_all.at[me, half], w_all.at[me, half]), (b_all.at[me], b_all.at[me]),
        )):
            copies.append((a, pltpu.make_async_remote_copy(
                src_ref=src, dst_ref=dst, send_sem=send.at[n, a], recv_sem=recv.at[n, a],
                device_id=(to, row), device_id_type=MESH)))
    for a in range(3):
        for which, copy in copies:
            if which == a:
                copy.start()
    own[4].wait()
    own[5].wait()
    group_i = (lax.broadcasted_iota(i32, (1, 128), 1) // GROUP) * KEYS

    for m in range(MICRO):
        for j in range(8):
            key_rows[m * 8 + j : m * 8 + j + 1, :] = keys[m : m + 1, j * 128 : (j + 1) * 128]

    def key_row_at(m, j):
        return key_rows[pl.ds(m * 8 + j, 1), :]

    def sameness(i, carry):
        for u in range(4):
            key_row = key_row_at(i // 2, (i % 2) * 4 + u) + group_i
            key_col = jnp.transpose(jnp.broadcast_to(key_row, (128, 128)))
            same[i * 4 + u] = jnp.where(key_col == key_row, 1.0, 0.0).astype(bf16)
        return carry

    lax.fori_loop(0, 8, sameness, 0)
    for which, copy in copies:
        if which == 0:
            copy.wait()
    to_scalar = pltpu.make_async_copy(words_v, words, local.at[6])
    to_scalar.start()
    passed = []
    for n, k in enumerate((2, 1, 3)):
        origin = lax.rem(me + 4 - k, 4)
        copies[3 * n + 1][1].wait()
        block = w_all.at[origin, half]
        copy = pltpu.make_async_remote_copy(
            src_ref=block, dst_ref=block, send_sem=pair_send.at[n], recv_sem=pair_recv.at[n],
            device_id=other, device_id_type=MESH)
        copy.start()
        passed.append(copy)
    to_scalar.wait()
    lane = lax.broadcasted_iota(i32, (8, 128), 1)

    def tally(i, carry):
        m = i // 2
        nv = valid[0, m]
        for u in range(4):
            j = (i % 2) * 4 + u
            total = jnp.zeros((8, 128), i32)
            alive = []
            for w in range(4):
                n = nv - (j * 4 + w) * 32
                alive.append(jnp.where(n >= 32, jnp.int32(-1), (jnp.int32(1) << jnp.clip(n, 0, 31)) - 1))
            for s in range(SECTIONS):
                alive = [a & words[s, m, j * 4 + w] for w, a in enumerate(alive)]
                v = jnp.where(
                    lane < 64,
                    jnp.where(lane < 32, alive[0], alive[1]),
                    jnp.where(lane < 96, alive[2], alive[3]))
                total = total + ((v >> (lane & 31)) & 1)
            lives[pl.ds(i * 4 + u, 1), :] = total[:1]
            level[i * 4 + u] = jnp.transpose(jnp.concatenate([total] * 16, axis=0))
        return carry

    lax.fori_loop(0, 8, tally, 0)
    for which, copy in copies:
        if which == 2:
            copy.wait()
    for copy in passed:
        copy.wait()


def exchange(weight, bias, predicates, keys, valid):
    return pl.pallas_call(
        exchange_kernel,
        out_shape=(
            jax.ShapeDtypeStruct((4, D, D), f32),
            jax.ShapeDtypeStruct((4, 1, D), f32),
            jax.ShapeDtypeStruct((32, 128, 128), bf16),
            jax.ShapeDtypeStruct((32, 128, 128), i32),
            jax.ShapeDtypeStruct((32, 128), i32),
            jax.ShapeDtypeStruct((KEYS, D), f32),
            jax.ShapeDtypeStruct((KEYS, D), f32),
            jax.ShapeDtypeStruct((32, 128), i32),
        ),
        in_specs=[spec(HB)] * 5,
        out_specs=(spec(VM),) * 8,
        scratch_shapes=[
            pltpu.VMEM((MICRO, BLOCK), i32),
            pltpu.SMEM((1, MICRO), i32),
            pltpu.VMEM((4, 4, 32), i32),
            pltpu.VMEM((4, 4, 32), i32),
            pltpu.SMEM((4, 4, 32), i32),
            pltpu.SemaphoreType.DMA((3, 3)),
            pltpu.SemaphoreType.DMA((3, 3)),
            pltpu.SemaphoreType.DMA((3,)),
            pltpu.SemaphoreType.DMA((3,)),
            pltpu.SemaphoreType.DMA((7,)),
        ],
        compiler_params=pltpu.CompilerParams(collective_id=0, has_side_effects=True, vmem_limit_bytes=8 << 20),
        cost_estimate=pl.CostEstimate(flops=40_000_000_000, bytes_accessed=1 << 20, transcendentals=0),
    )(pinned(weight), pinned(bias), pinned(predicates), pinned(keys), pinned(valid))


def sections_kernel(
    rows, keys_in, w, b, same, level, clear_a, clear_b, v_in, table_a, table_b, w2, ready, keys, valid, sems
):
    fetch = [pltpu.make_async_copy(keys_in, keys, sems.at[0]), pltpu.make_async_copy(v_in, valid, sems.at[1])]
    for copy in fetch:
        copy.start()
    for s in range(SECTIONS):
        top = jnp.concatenate(high_low(w[s]), axis=1)
        w2[s] = jnp.concatenate([top, top], axis=0)

    def batch(m, carry):
        h = rows[m]
        alive = level[pl.ds(m * 8, 8)].reshape(BLOCK, 128)
        total = jnp.zeros((BLOCK, D), f32)
        for s in range(SECTIONS):
            p = jnp.dot(jnp.concatenate(high_low(h), axis=1), w2[s], preferred_element_type=f32)
            h = h + jnp.tanh(p[:, :D] + (p[:, D:] + b[s]))
            total = total + jnp.where(alive > s, h, 0.0)
        both = jnp.concatenate(high_low(total), axis=1)
        for j in range(8):
            p = jnp.dot(same[m * 8 + j], both[j * 128 : (j + 1) * 128], preferred_element_type=f32)
            ready[pl.ds(pl.multiple_of(m * BLOCK + j * 128, 128), 128), :] = p[:, :D] + p[:, D:]
        return carry

    lax.fori_loop(0, MICRO, batch, 0)
    for copy in fetch:
        copy.wait()
    tables = (table_a, table_b)
    groups = CHUNK // GROUP

    def scatter(first, i, carry):
        u = first + i
        def load(g):
            at = [keys[u * (CHUNK // 128) + (g * GROUP + i) // 128, (g * GROUP + i) % 128] for i in range(GROUP)]
            return at, [tables[g % 2][pl.ds(k, 1), :] for k in at]

        def store(g, at, held):
            for i, k in enumerate(at):
                tables[g % 2][pl.ds(k, 1), :] = held[i] + ready[pl.ds(u * CHUNK + g * GROUP + i, 1), :]

        flying = {g: load(g) for g in range(2)}
        for g in range(groups):
            store(g, *flying.pop(g))
            if g + 2 < groups:
                flying[g + 2] = load(g + 2)
        return carry

    for m in range(MICRO):
        chunks = (valid[0, m] + CHUNK - 1) // CHUNK
        lax.fori_loop(0, chunks, functools.partial(scatter, m * (BLOCK // CHUNK)), 0)


def sections(rows, keys, w, b, same, level, clear_a, clear_b, valid):
    return pl.pallas_call(
        sections_kernel,
        out_shape=(jax.ShapeDtypeStruct((KEYS, D), f32),) * 2,
        in_specs=[spec(VM)] * 8 + [spec(HB)],
        out_specs=(spec(VM),) * 2,
        scratch_shapes=[
            pltpu.VMEM((SECTIONS, 256, 256), bf16),
            pltpu.VMEM((ROWS, D), f32),
            pltpu.SMEM((32, 128), i32),
            pltpu.SMEM((1, MICRO), i32),
            pltpu.SemaphoreType.DMA((2,)),
        ],
        input_output_aliases={6: 0, 7: 1},
        compiler_params=pltpu.CompilerParams(vmem_limit_bytes=12 << 20),
    )(rows, keys, w, b, same, level, clear_a, clear_b, pinned(valid))


PARTS = (
    (0, 8, (0, 1, 2)),
    (24, 8, (1, 2, 0)),
    (64, 8, (2, 0, 1)),
    (8, 8, (0, 1, 2)),
    (32, 8, (1, 2, 0)),
    (48, 8, (2, 0, 1)),
    (16, 8, (0, 1, 2)),
    (40, 8, (1, 2, 0)),
    (56, 8, (2, 0, 1)),
)
TURNS = (
    (0, 0), (5, 0), (0, 1), (5, 1), (0, 2), (5, 2), (0, 3), (5, 3), (0, 4), (5, 4), (0, 5), (5, 5),
    (0, 6), (5, 6), (0, 7), (5, 7), (0, 8), (5, 8), (1, 0), (1, 1), (1, 2), (1, 3), (1, 4), (1, 5),
    (1, 6), (1, 7), (1, 8), (2, 0), (2, 1), (2, 2), (2, 3), (2, 4), (2, 5), (2, 6), (2, 7), (2, 8),
    (3, 0), (3, 1), (3, 2), (3, 3), (3, 4), (3, 5), (3, 6), (3, 7), (3, 8), (4, 0), (4, 1), (4, 2),
    (4, 3), (4, 4), (4, 5), (4, 6), (4, 7), (4, 8),
)
N = len(PARTS)
HEIGHT = 72


def reduce_kernel(table_a, table_b, keys, lives, means, count_out, table, *scratch):
    held, near, middle, second, last, third = (scratch[i * N : (i + 1) * N] for i in range(6))
    core_sems, near_sems, far_sems = scratch[6 * N :]
    z = lax.axis_index("section")
    row = lax.axis_index("rows")
    y, x, c = row // 8, (row // 2) % 4, row % 2
    place = (z, y, x)

    def position(axis, k):
        return lax.rem(place[axis] + k, 4)

    def device(axis, k):
        at = list(place)
        at[axis] = position(axis, k)
        return (at[0], at[1] * 8 + at[2] * 2 + c)

    other = (z, y * 8 + x * 2 + (1 - c))
    peers = [device(axis, k) for axis in range(3) for k in (1, 3)] + [other]
    barrier = pltpu.get_barrier_semaphore()
    for peer in peers:
        pl.semaphore_signal(barrier, inc=1, device_id=peer, device_id_type=MESH)

    def join(i, carry):
        at = (i // 16, (i // 4) % 4, i % 4)
        table[(*at, slice(None), slice(0, 64))] = table_a[at] + table_b[at]
        return carry

    lax.fori_loop(0, 64, join, 0)
    sub64 = lax.broadcasted_iota(i32, (64, 128), 0)
    sub128 = lax.broadcasted_iota(i32, (128, 128), 0)

    def tally(i, found):
        for u in range(4):
            key_row = keys[pl.ds(i * 4 + u, 1), :]
            alive = lives[pl.ds(i * 4 + u, 1), :].astype(f32)
            high = jnp.where((key_row >> 7) == sub64, alive, 0.0).astype(bf16)
            low = jnp.where((key_row & 127) == sub128, 1.0, 0.0).astype(bf16)
            found = found + lax.dot_general(high, low, (((1,), (1,)), ((), ())), preferred_element_type=f32)
        return found

    found = lax.fori_loop(0, 8, tally, jnp.zeros((64, 128), f32))
    for i in range(64):
        line = jnp.broadcast_to(found[i : i + 1], (8, 128))
        for core in range(2):
            table[i // 16, (i // 4) % 4, i % 4, core, 64:72, :] = line
    pl.semaphore_wait(barrier, len(peers))

    def send(src, dst, send_sem, recv_sem, to):
        pltpu.make_async_remote_copy(
            src_ref=src, dst_ref=dst, send_sem=send_sem, recv_sem=recv_sem, device_id=to, device_id_type=MESH
        ).start()

    def wait(ref, sem):
        pltpu.make_async_copy(ref, ref, sem).wait()

    def piece(ref, axes, axis, index, half=None):
        where = [slice(None)] * len(axes)
        where[axes.index(axis)] = index
        if half is not None:
            where[1 if axes[0] == axis else 0] = pl.ds(2 * half, 2)
        return ref.at[tuple(where)]

    def spread(n, stage, source, axes, target):
        axis = PARTS[n][2][stage]
        for k in (2, 1, 3):
            send(
                piece(source, axes, axis, position(axis, k)), target.at[k - 1],
                far_sems.at[n, stage - 1, 0], far_sems.at[n, stage - 1, 1], device(axis, k))

    def summed(n, stage, source, axes, target):
        axis = PARTS[n][2][stage]
        wait(target, far_sems.at[n, stage - 1, 1])
        return (piece(source, axes, axis, place[axis])[...] + target[0]) + (target[1] + target[2])

    every = [0, 1, 2]
    for n, (start, size, order) in enumerate(PARTS):
        send(table.at[:, :, :, 1 - c, pl.ds(start, size), :], held[n], core_sems.at[0, n], core_sems.at[1, n], other)
    values = []
    for turn, n in TURNS:
        start, size, order = PARTS[n]
        axis = order[0]

        def hop(slot, recv, index, half, k):
            send(
                piece(held[n], every, axis, index, half), near[n].at[slot],
                near_sems.at[n, 3], near_sems.at[n, recv], device(axis, k))

        axes = [i for i in every if i != axis]
        if turn == 0:
            wait(held[n], core_sems.at[1, n])
            for i in range(4):
                held[n][i] += table[i, :, :, c, start : start + size, :]
            hop(0, 0, position(axis, 2), 0, 1)
            hop(1, 1, position(axis, 2), 1, 3)
        elif turn == 5:
            hop(2, 2, position(axis, 1), 1, 1)
            hop(3, 2, position(axis, 3), 0, 3)
        elif turn == 1:
            for half, k in ((0, 1), (1, 3)):
                wait(near[n].at[half], near_sems.at[n, half])
                block = piece(held[n], every, axis, position(axis, k), half)
                block[...] += near[n][half]
                hop(4 + half, 2, position(axis, k), half, k)
        elif turn == 2:
            wait(near[n].at[2:6], near_sems.at[n, 2])
            middle[n][0:2] = (piece(held[n], every, axis, place[axis], 0)[...] + near[n][3]) + near[n][4]
            middle[n][2:4] = (piece(held[n], every, axis, place[axis], 1)[...] + near[n][2]) + near[n][5]
            spread(n, 1, middle[n], axes, second[n])
        elif turn == 3:
            last[n][...] = summed(n, 1, middle[n], axes, second[n])
            spread(n, 2, last[n], [order[2]], third[n])
        else:
            value = summed(n, 2, last[n], [order[2]], third[n])
            if start + size == HEIGHT:
                line = value[size - 8 : size - 7]
                wide = jnp.transpose(jnp.broadcast_to(line, (128, 128)))
                total = jnp.maximum(jnp.where(c == 0, wide[:64], wide[64:]), 1.0)
                count_out[...] = jnp.broadcast_to(jnp.where(c == 0, line, pltpu.roll(line, 64, 1)), (8, 128))
                size -= 8
            values.append((start, size, value))
    for start, size, value in values:
        if size:
            means[start : start + size, :] = value[:size] / total[start : start + size]
    for n in range(N):
        wait(held[n], core_sems.at[0, n])
        wait(near[n], near_sems.at[n, 3])
        wait(second[n], far_sems.at[n, 0, 0])
        wait(third[n], far_sems.at[n, 1, 0])


def reduce_to_owner(table_a, table_b, keys, lives):
    buffers = [pltpu.VMEM((4, 4, 4, 2, HEIGHT, D), f32)]
    for lead in ((4, 4, 4), (6, 2, 4), (4, 4), (3, 4), (4,), (3,)):
        buffers += [pltpu.VMEM((*lead, size, D), f32) for _, size, _ in PARTS]
    return pl.pallas_call(
        reduce_kernel,
        out_shape=(jax.ShapeDtypeStruct((64, D), f32), jax.ShapeDtypeStruct((8, D), f32)),
        in_specs=[spec(VM)] * 4,
        out_specs=(spec(VM), spec(VM)),
        scratch_shapes=buffers + [
            pltpu.SemaphoreType.DMA((2, N)),
            pltpu.SemaphoreType.DMA((N, 4)),
            pltpu.SemaphoreType.DMA((N, 2, 2)),
        ],
        compiler_params=pltpu.CompilerParams(collective_id=1, has_side_effects=True, vmem_limit_bytes=20 << 20),
    )(table_a.reshape(4, 4, 4, 2, 64, D), table_b.reshape(4, 4, 4, 2, 64, D), keys, lives)


def shards(rows_data, row_keys, valid_counts, predicates, section_weight, section_bias):
    w, b, same, level, lives, clear_a, clear_b, key_rows = exchange(
        section_weight, section_bias.reshape(1, 1, D), predicates.reshape(4, MICRO, 32), row_keys, valid_counts.T)
    tables = sections(rows_data, key_rows, w, b, same, level, clear_a, clear_b, valid_counts.T)
    means, total = reduce_to_owner(*tables, key_rows, lives)
    return means, total[0, :64]


def solution(mesh):
    placed = (
        P("section", "rows", None),
        P("section", "rows"),
        P("section", "rows"),
        P("section", None, "rows"),
        P("section", None, None),
        P("section", None),
    )
    return jax.shard_map(
        shards,
        mesh=mesh,
        in_specs=placed,
        out_specs=(P(("section", "rows"), None), P(("section", "rows"))),
        check_vma=False,
    )
```

```python
import functools

import jax
import jax.numpy as jnp
from jax import lax
from jax.experimental import pallas as pl
from jax.experimental.pallas import tpu as pltpu
from jax.sharding import PartitionSpec as P

KEYS = 8192
SECTIONS = 4
D = 128
MICRO = 4
BLOCK = 1024
ROWS = MICRO * BLOCK
GROUP = 8
CHUNK = 256
f32, bf16, i32 = jnp.float32, jnp.bfloat16, jnp.int32
MESH = pl.DeviceIdType.MESH
VM, SM, HB = pltpu.VMEM, pltpu.SMEM, pltpu.HBM


def spec(space):
    return pl.BlockSpec(memory_space=space)


def pinned(x):
    return pltpu.with_memory_space_constraint(x, HB)


def high_low(x):
    high = x.astype(bf16)
    return high, (x - high.astype(f32)).astype(bf16)


def exchange_kernel(
    w_in, b_in, p_in, k_in, v_in,
    w_twice, b_all, same, lives, table_a, table_b, key_rows,
    w_all, keys, valid, flags, words_v, words, send, recv, pair_send, pair_recv, local,
):
    me = lax.axis_index("section")
    row = lax.axis_index("rows")
    c = row % 2
    other = (me, row + 1 - 2 * c)
    own = [
        pltpu.make_async_copy(src, dst, local.at[n])
        for n, (src, dst) in enumerate((
            (p_in, flags), (p_in.at[me], words_v.at[me]), (b_in.at[0], b_all.at[me]), (w_in.at[0], w_all.at[me]),
            (k_in, keys), (v_in, valid)))
    ]
    for copy in own:
        copy.start()
    barrier = pltpu.get_barrier_semaphore()
    for k in range(1, 4):
        pl.semaphore_signal(barrier, inc=1, device_id=(lax.rem(me + k, 4), row), device_id_type=MESH)
    pl.semaphore_signal(barrier, inc=1, device_id=other, device_id_type=MESH)

    def clear(i, carry):
        at = pl.ds(pl.multiple_of(i * 512, 512), 512)
        table_a[at, :] = jnp.zeros((512, D), f32)
        table_b[at, :] = jnp.zeros((512, D), f32)
        return carry

    lax.fori_loop(0, KEYS // 512, clear, 0)
    for copy in own[:4]:
        copy.wait()
    pl.semaphore_wait(barrier, 4)
    half = pl.ds(pl.multiple_of(c * 64, 64), 64)
    copies = []
    for n, k in enumerate((2, 1, 3)):
        to = lax.rem(me + k, 4)
        for a, (src, dst) in enumerate((
            (flags.at[to], words_v.at[me]), (w_all.at[me, half], w_all.at[me, half]), (b_all.at[me], b_all.at[me]),
        )):
            copies.append((a, pltpu.make_async_remote_copy(
                src_ref=src, dst_ref=dst, send_sem=send.at[n, a], recv_sem=recv.at[n, a],
                device_id=(to, row), device_id_type=MESH)))
    for a in range(3):
        for which, copy in copies:
            if which == a:
                copy.start()

    def prepare(origin):
        top = jnp.concatenate(high_low(w_all[origin]), axis=1)
        w_twice[origin] = jnp.concatenate([top, top], axis=0)

    prepare(me)
    own[4].wait()
    own[5].wait()
    group_i = (lax.broadcasted_iota(i32, (1, 128), 1) // GROUP) * KEYS

    for m in range(MICRO):
        for j in range(8):
            key_rows[m * 8 + j : m * 8 + j + 1, :] = keys[m : m + 1, j * 128 : (j + 1) * 128]

    def key_row_at(m, j):
        return key_rows[pl.ds(m * 8 + j, 1), :]

    def sameness(i, carry):
        for u in range(4):
            key_row = key_row_at(i // 2, (i % 2) * 4 + u) + group_i
            key_col = jnp.transpose(jnp.broadcast_to(key_row, (128, 128)))
            same[i * 4 + u] = jnp.where(key_col == key_row, 1.0, 0.0).astype(bf16)
        return carry

    lax.fori_loop(0, 8, sameness, 0)
    for which, copy in copies:
        if which == 0:
            copy.wait()
    to_scalar = pltpu.make_async_copy(words_v, words, local.at[6])
    to_scalar.start()
    passed = []
    for n, k in enumerate((2, 1, 3)):
        origin = lax.rem(me + 4 - k, 4)
        copies[3 * n + 1][1].wait()
        block = w_all.at[origin, half]
        copy = pltpu.make_async_remote_copy(
            src_ref=block, dst_ref=block, send_sem=pair_send.at[n], recv_sem=pair_recv.at[n],
            device_id=other, device_id_type=MESH)
        copy.start()
        passed.append(copy)
    to_scalar.wait()
    lane = lax.broadcasted_iota(i32, (8, 128), 1)

    def tally(i, carry):
        m = i // 2
        nv = valid[0, m]
        for u in range(4):
            j = (i % 2) * 4 + u
            total = jnp.zeros((8, 128), i32)
            alive = []
            for w in range(4):
                n = nv - (j * 4 + w) * 32
                alive.append(jnp.where(n >= 32, jnp.int32(-1), (jnp.int32(1) << jnp.clip(n, 0, 31)) - 1))
            for s in range(SECTIONS):
                alive = [a & words[s, m, j * 4 + w] for w, a in enumerate(alive)]
                v = jnp.where(
                    lane < 64,
                    jnp.where(lane < 32, alive[0], alive[1]),
                    jnp.where(lane < 96, alive[2], alive[3]))
                total = total + ((v >> (lane & 31)) & 1)
            lives[pl.ds(i * 4 + u, 1), :] = total[:1]
        return carry

    lax.fori_loop(0, 8, tally, 0)
    for which, copy in copies:
        if which == 2:
            copy.wait()
    for n, k in enumerate((2, 1, 3)):
        passed[n].wait()
        prepare(lax.rem(me + 4 - k, 4))


def exchange(weight, bias, predicates, keys, valid):
    return pl.pallas_call(
        exchange_kernel,
        out_shape=(
            jax.ShapeDtypeStruct((4, 256, 256), bf16),
            jax.ShapeDtypeStruct((4, 1, D), f32),
            jax.ShapeDtypeStruct((32, 128, 128), bf16),
            jax.ShapeDtypeStruct((32, 128), i32),
            jax.ShapeDtypeStruct((KEYS, D), f32),
            jax.ShapeDtypeStruct((KEYS, D), f32),
            jax.ShapeDtypeStruct((32, 128), i32),
        ),
        in_specs=[spec(HB)] * 5,
        out_specs=(spec(VM),) * 7,
        scratch_shapes=[
            pltpu.VMEM((4, D, D), f32),
            pltpu.VMEM((MICRO, BLOCK), i32),
            pltpu.SMEM((1, MICRO), i32),
            pltpu.VMEM((4, 4, 32), i32),
            pltpu.VMEM((4, 4, 32), i32),
            pltpu.SMEM((4, 4, 32), i32),
            pltpu.SemaphoreType.DMA((3, 3)),
            pltpu.SemaphoreType.DMA((3, 3)),
            pltpu.SemaphoreType.DMA((3,)),
            pltpu.SemaphoreType.DMA((3,)),
            pltpu.SemaphoreType.DMA((7,)),
        ],
        compiler_params=pltpu.CompilerParams(collective_id=0, has_side_effects=True, vmem_limit_bytes=8 << 20),
        cost_estimate=pl.CostEstimate(flops=40_000_000_000, bytes_accessed=1 << 20, transcendentals=0),
    )(pinned(weight), pinned(bias), pinned(predicates), pinned(keys), pinned(valid))


def sections_kernel(
    rows, keys_in, w2, b, same, lives, clear_a, clear_b, v_in, table_a, table_b, ready, keys, valid, sems
):
    fetch = [pltpu.make_async_copy(keys_in, keys, sems.at[0]), pltpu.make_async_copy(v_in, valid, sems.at[1])]
    for copy in fetch:
        copy.start()

    def batch(m, carry):
        h = rows[m]
        columns = jnp.transpose(jnp.concatenate([lives[pl.ds(pl.multiple_of(m * 8, 8), 8), :]] * 16, axis=0))
        alive = jnp.concatenate([jnp.broadcast_to(columns[:, j : j + 1], (128, 128)) for j in range(8)], axis=0)
        total = jnp.zeros((BLOCK, D), f32)
        for s in range(SECTIONS):
            p = jnp.dot(jnp.concatenate(high_low(h), axis=1), w2[s], preferred_element_type=f32)
            h = h + jnp.tanh(p[:, :D] + (p[:, D:] + b[s]))
            total = total + jnp.where(alive > s, h, 0.0)
        both = jnp.concatenate(high_low(total), axis=1)
        for j in range(8):
            p = jnp.dot(same[m * 8 + j], both[j * 128 : (j + 1) * 128], preferred_element_type=f32)
            ready[pl.ds(pl.multiple_of(m * BLOCK + j * 128, 128), 128), :] = p[:, :D] + p[:, D:]
        return carry

    lax.fori_loop(0, MICRO, batch, 0)
    for copy in fetch:
        copy.wait()
    tables = (table_a, table_b)
    groups = CHUNK // GROUP

    def scatter(first, i, carry):
        u = first + i
        def load(g):
            at = [keys[u * (CHUNK // 128) + (g * GROUP + i) // 128, (g * GROUP + i) % 128] for i in range(GROUP)]
            return at, [tables[g % 2][pl.ds(k, 1), :] for k in at]

        def store(g, at, held):
            for i, k in enumerate(at):
                tables[g % 2][pl.ds(k, 1), :] = held[i] + ready[pl.ds(u * CHUNK + g * GROUP + i, 1), :]

        flying = {g: load(g) for g in range(2)}
        for g in range(groups):
            store(g, *flying.pop(g))
            if g + 2 < groups:
                flying[g + 2] = load(g + 2)
        return carry

    for m in range(MICRO):
        chunks = (valid[0, m] + CHUNK - 1) // CHUNK
        lax.fori_loop(0, chunks, functools.partial(scatter, m * (BLOCK // CHUNK)), 0)


def sections(rows, keys, w, b, same, lives, clear_a, clear_b, valid):
    return pl.pallas_call(
        sections_kernel,
        out_shape=(jax.ShapeDtypeStruct((KEYS, D), f32),) * 2,
        in_specs=[spec(VM)] * 8 + [spec(HB)],
        out_specs=(spec(VM),) * 2,
        scratch_shapes=[
            pltpu.VMEM((ROWS, D), f32),
            pltpu.SMEM((32, 128), i32),
            pltpu.SMEM((1, MICRO), i32),
            pltpu.SemaphoreType.DMA((2,)),
        ],
        input_output_aliases={6: 0, 7: 1},
        compiler_params=pltpu.CompilerParams(vmem_limit_bytes=12 << 20),
    )(rows, keys, w, b, same, lives, clear_a, clear_b, pinned(valid))


PARTS = (
    (0, 8, (0, 1, 2)),
    (24, 8, (1, 2, 0)),
    (48, 8, (2, 0, 1)),
    (8, 8, (0, 1, 2)),
    (32, 8, (1, 2, 0)),
    (56, 8, (2, 0, 1)),
    (16, 8, (0, 1, 2)),
    (40, 8, (1, 2, 0)),
    (64, 8, (2, 0, 1)),
)
TURNS = (
    (0, 0), (5, 0), (0, 1), (5, 1), (0, 2), (5, 2), (0, 3), (5, 3), (0, 4), (5, 4), (0, 5), (5, 5),
    (0, 6), (5, 6), (0, 7), (5, 7), (0, 8), (5, 8), (1, 0), (1, 1), (1, 2), (1, 3), (1, 4), (1, 5),
    (1, 6), (1, 7), (1, 8), (2, 0), (2, 1), (2, 2), (2, 3), (2, 4), (2, 5), (2, 6), (2, 7), (2, 8),
    (3, 0), (3, 1), (3, 2), (3, 3), (3, 4), (3, 5), (3, 6), (3, 7), (3, 8), (4, 0), (4, 1), (4, 2),
    (4, 3), (4, 4), (4, 5), (4, 6), (4, 7), (4, 8),
)
N = len(PARTS)
HEIGHT = 72


def reduce_kernel(table_a, table_b, keys, lives, sums, pair, *scratch):
    held, near, middle, second, last, third = (scratch[i * N : (i + 1) * N] for i in range(6))
    core_sems, near_sems, far_sems = scratch[6 * N :]
    z = lax.axis_index("section")
    row = lax.axis_index("rows")
    y, x, c = row // 8, (row // 2) % 4, row % 2
    place = (z, y, x)

    def position(axis, k):
        return lax.rem(place[axis] + k, 4)

    def device(axis, k):
        at = list(place)
        at[axis] = position(axis, k)
        return (at[0], at[1] * 8 + at[2] * 2 + c)

    other = (z, y * 8 + x * 2 + (1 - c))
    peers = [device(axis, k) for axis in range(3) for k in (1, 3)] + [other]
    barrier = pltpu.get_barrier_semaphore()
    for peer in peers:
        pl.semaphore_signal(barrier, inc=1, device_id=peer, device_id_type=MESH)

    def join(i, carry):
        at = (i // 16, (i // 4) % 4, i % 4)
        pair[(*at, slice(0, 64))] = table_a[(*at, 1 - c)] + table_b[(*at, 1 - c)]
        return carry

    lax.fori_loop(0, 64, join, 0)
    pl.semaphore_wait(barrier, len(peers))

    def send(src, dst, send_sem, recv_sem, to):
        pltpu.make_async_remote_copy(
            src_ref=src, dst_ref=dst, send_sem=send_sem, recv_sem=recv_sem, device_id=to, device_id_type=MESH
        ).start()

    def wait(ref, sem):
        pltpu.make_async_copy(ref, ref, sem).wait()

    def piece(ref, axes, axis, index, half=None):
        where = [slice(None)] * len(axes)
        where[axes.index(axis)] = index
        if half is not None:
            where[1 if axes[0] == axis else 0] = pl.ds(2 * half, 2)
        return ref.at[tuple(where)]

    def spread(n, stage, source, axes, target):
        axis = PARTS[n][2][stage]
        for k in (2, 1, 3):
            send(
                piece(source, axes, axis, position(axis, k)), target.at[k - 1],
                far_sems.at[n, stage - 1, 0], far_sems.at[n, stage - 1, 1], device(axis, k))

    def summed(n, stage, source, axes, target):
        axis = PARTS[n][2][stage]
        wait(target, far_sems.at[n, stage - 1, 1])
        return (piece(source, axes, axis, place[axis])[...] + target[0]) + (target[1] + target[2])

    every = [0, 1, 2]

    def swap(n):
        start, size, order = PARTS[n]
        send(pair.at[:, :, :, pl.ds(start, size), :], held[n], core_sems.at[0, n], core_sems.at[1, n], other)

    for n in range(N - 1):
        swap(n)
    sub64 = lax.broadcasted_iota(i32, (64, 128), 0)
    sub128 = lax.broadcasted_iota(i32, (128, 128), 0)

    def tally(i, found):
        for u in range(4):
            key_row = keys[pl.ds(i * 4 + u, 1), :]
            alive = lives[pl.ds(i * 4 + u, 1), :].astype(f32)
            high = jnp.where((key_row >> 7) == sub64, alive, 0.0).astype(bf16)
            low = jnp.where((key_row & 127) == sub128, 1.0, 0.0).astype(bf16)
            found = found + lax.dot_general(high, low, (((1,), (1,)), ((), ())), preferred_element_type=f32)
        return found

    found = lax.fori_loop(0, 8, tally, jnp.zeros((64, 128), f32))
    for i in range(64):
        pair[i // 16, (i // 4) % 4, i % 4, 64:72, :] = jnp.broadcast_to(found[i : i + 1], (8, 128))
    swap(N - 1)
    for turn, n in TURNS:
        start, size, order = PARTS[n]
        axis = order[0]

        def hop(slot, recv, index, half, k):
            send(
                piece(held[n], every, axis, index, half), near[n].at[slot],
                near_sems.at[n, 3], near_sems.at[n, recv], device(axis, k))

        axes = [i for i in every if i != axis]
        if turn == 0:
            wait(held[n], core_sems.at[1, n])
            for i in range(4):
                if n == N - 1:
                    mine = pair[i, :, :, 64:72, :]
                else:
                    at = (i, slice(None), slice(None), c, slice(start, start + size))
                    mine = table_a[at] + table_b[at]
                held[n][i] += mine
            hop(0, 0, position(axis, 2), 0, 1)
            hop(1, 1, position(axis, 2), 1, 3)
        elif turn == 5:
            hop(2, 2, position(axis, 1), 1, 1)
            hop(3, 2, position(axis, 3), 0, 3)
        elif turn == 1:
            for half, k in ((0, 1), (1, 3)):
                wait(near[n].at[half], near_sems.at[n, half])
                block = piece(held[n], every, axis, position(axis, k), half)
                block[...] += near[n][half]
                hop(4 + half, 2, position(axis, k), half, k)
        elif turn == 2:
            wait(near[n].at[2:6], near_sems.at[n, 2])
            middle[n][0:2] = (piece(held[n], every, axis, place[axis], 0)[...] + near[n][3]) + near[n][4]
            middle[n][2:4] = (piece(held[n], every, axis, place[axis], 1)[...] + near[n][2]) + near[n][5]
            spread(n, 1, middle[n], axes, second[n])
        elif turn == 3:
            last[n][...] = summed(n, 1, middle[n], axes, second[n])
            spread(n, 2, last[n], [order[2]], third[n])
        else:
            sums[start : start + size, :] = summed(n, 2, last[n], [order[2]], third[n])
    for n in range(N):
        wait(held[n], core_sems.at[0, n])
        wait(near[n], near_sems.at[n, 3])
        wait(second[n], far_sems.at[n, 0, 0])
        wait(third[n], far_sems.at[n, 1, 0])


def reduce_to_owner(table_a, table_b, keys, lives):
    buffers = [pltpu.VMEM((4, 4, 4, HEIGHT, D), f32)]
    for lead in ((4, 4, 4), (6, 2, 4), (4, 4), (3, 4), (4,), (3,)):
        buffers += [pltpu.VMEM((*lead, size, D), f32) for _, size, _ in PARTS]
    return pl.pallas_call(
        reduce_kernel,
        out_shape=jax.ShapeDtypeStruct((HEIGHT, D), f32),
        in_specs=[spec(VM)] * 4,
        out_specs=spec(VM),
        scratch_shapes=buffers + [
            pltpu.SemaphoreType.DMA((2, N)),
            pltpu.SemaphoreType.DMA((N, 4)),
            pltpu.SemaphoreType.DMA((N, 2, 2)),
        ],
        compiler_params=pltpu.CompilerParams(collective_id=1, has_side_effects=True, vmem_limit_bytes=20 << 20),
    )(table_a.reshape(4, 4, 4, 2, 64, D), table_b.reshape(4, 4, 4, 2, 64, D), keys, lives)


def means_kernel(sums, means, counts):
    c = lax.axis_index("rows") % 2
    line = sums[64:65, :]
    wide = jnp.transpose(jnp.broadcast_to(line, (128, 128)))
    means[...] = sums[:64] / jnp.maximum(jnp.where(c == 0, wide[:64], wide[64:]), 1.0)
    counts[...] = jnp.where(c == 0, line, pltpu.roll(line, 64, 1))[:, :64]


def means_of(sums):
    return pl.pallas_call(
        means_kernel,
        out_shape=(jax.ShapeDtypeStruct((64, D), f32), jax.ShapeDtypeStruct((1, 64), f32)),
        in_specs=[spec(VM)],
        out_specs=(spec(VM), spec(VM)),
        compiler_params=pltpu.CompilerParams(vmem_limit_bytes=1 << 20),
    )(sums)


def shards(rows_data, row_keys, valid_counts, predicates, section_weight, section_bias):
    w, b, same, lives, clear_a, clear_b, key_rows = exchange(
        section_weight, section_bias.reshape(1, 1, D), predicates.reshape(4, MICRO, 32), row_keys, valid_counts.T)
    tables = sections(rows_data, key_rows, w, b, same, lives, clear_a, clear_b, valid_counts.T)
    means, counts = means_of(reduce_to_owner(*tables, key_rows, lives))
    return means, counts.reshape(64)


def solution(mesh):
    placed = (
        P("section", "rows", None),
        P("section", "rows"),
        P("section", "rows"),
        P("section", None, "rows"),
        P("section", None, None),
        P("section", None),
    )
    return jax.shard_map(
        shards,
        mesh=mesh,
        in_specs=placed,
        out_specs=(P(("section", "rows"), None), P(("section", "rows"))),
        check_vma=False,
    )
```

```python
import functools

import jax
import jax.numpy as jnp
from jax import lax
from jax.experimental import pallas as pl
from jax.experimental.pallas import tpu as pltpu
from jax.sharding import PartitionSpec as P

KEYS = 8192
SECTIONS = 4
D = 128
MICRO = 4
BLOCK = 1024
ROWS = MICRO * BLOCK
GROUP = 8
CHUNK = 256
f32, bf16, i32 = jnp.float32, jnp.bfloat16, jnp.int32
MESH = pl.DeviceIdType.MESH
VM, SM, HB = pltpu.VMEM, pltpu.SMEM, pltpu.HBM


def spec(space):
    return pl.BlockSpec(memory_space=space)


def pinned(x):
    return pltpu.with_memory_space_constraint(x, HB)


def high_low(x):
    high = x.astype(bf16)
    return high, (x - high.astype(f32)).astype(bf16)


def exchange_kernel(
    w_in, b_in, p_in, k_in, v_in,
    w_twice, b_all, same, lives, table_a, table_b, key_rows,
    w_all, keys, valid, flags, words_v, words, send, recv, pair_send, pair_recv, local,
):
    me = lax.axis_index("section")
    row = lax.axis_index("rows")
    c = row % 2
    other = (me, row + 1 - 2 * c)
    own = [
        pltpu.make_async_copy(src, dst, local.at[n])
        for n, (src, dst) in enumerate((
            (p_in, flags), (p_in.at[me], words_v.at[me]), (b_in.at[0], b_all.at[me]), (w_in.at[0], w_all.at[me]),
            (k_in, keys), (v_in, valid)))
    ]
    for copy in own:
        copy.start()
    barrier = pltpu.get_barrier_semaphore()
    for k in range(1, 4):
        pl.semaphore_signal(barrier, inc=1, device_id=(lax.rem(me + k, 4), row), device_id_type=MESH)
    pl.semaphore_signal(barrier, inc=1, device_id=other, device_id_type=MESH)

    def clear(i, carry):
        at = pl.ds(pl.multiple_of(i * 512, 512), 512)
        table_a[at, :] = jnp.zeros((512, D), f32)
        table_b[at, :] = jnp.zeros((512, D), f32)
        return carry

    lax.fori_loop(0, KEYS // 512, clear, 0)
    for copy in own[:4]:
        copy.wait()
    pl.semaphore_wait(barrier, 4)
    half = pl.ds(pl.multiple_of(c * 64, 64), 64)
    copies = []
    for n, k in enumerate((2, 1, 3)):
        to = lax.rem(me + k, 4)
        for a, (src, dst) in enumerate((
            (flags.at[to], words_v.at[me]), (w_all.at[me, half], w_all.at[me, half]), (b_all.at[me], b_all.at[me]),
        )):
            copies.append((a, pltpu.make_async_remote_copy(
                src_ref=src, dst_ref=dst, send_sem=send.at[n, a], recv_sem=recv.at[n, a],
                device_id=(to, row), device_id_type=MESH)))
    for a in range(3):
        for which, copy in copies:
            if which == a:
                copy.start()

    def prepare(origin):
        top = jnp.concatenate(high_low(w_all[origin]), axis=1)
        w_twice[origin] = jnp.concatenate([top, top], axis=0)

    prepare(me)
    own[4].wait()
    own[5].wait()
    group_i = (lax.broadcasted_iota(i32, (1, 128), 1) // GROUP) * KEYS

    for m in range(MICRO):
        for j in range(8):
            key_rows[m * 8 + j : m * 8 + j + 1, :] = keys[m : m + 1, j * 128 : (j + 1) * 128]

    def key_row_at(m, j):
        return key_rows[pl.ds(m * 8 + j, 1), :]

    def sameness(i, carry):
        for u in range(4):
            key_row = key_row_at(i // 2, (i % 2) * 4 + u) + group_i
            key_col = jnp.transpose(jnp.broadcast_to(key_row, (128, 128)))
            same[i * 4 + u] = jnp.where(key_col == key_row, 1.0, 0.0).astype(bf16)
        return carry

    lax.fori_loop(0, 8, sameness, 0)
    for which, copy in copies:
        if which == 0:
            copy.wait()
    to_scalar = pltpu.make_async_copy(words_v, words, local.at[6])
    to_scalar.start()
    passed = []
    for n, k in enumerate((2, 1, 3)):
        origin = lax.rem(me + 4 - k, 4)
        copies[3 * n + 1][1].wait()
        block = w_all.at[origin, half]
        copy = pltpu.make_async_remote_copy(
            src_ref=block, dst_ref=block, send_sem=pair_send.at[n], recv_sem=pair_recv.at[n],
            device_id=other, device_id_type=MESH)
        copy.start()
        passed.append(copy)
    to_scalar.wait()
    lane = lax.broadcasted_iota(i32, (8, 128), 1)

    def tally(i, carry):
        m = i // 2
        nv = valid[0, m]
        for u in range(4):
            j = (i % 2) * 4 + u
            total = jnp.zeros((8, 128), i32)
            alive = []
            for w in range(4):
                n = nv - (j * 4 + w) * 32
                alive.append(jnp.where(n >= 32, jnp.int32(-1), (jnp.int32(1) << jnp.clip(n, 0, 31)) - 1))
            for s in range(SECTIONS):
                alive = [a & words[s, m, j * 4 + w] for w, a in enumerate(alive)]
                v = jnp.where(
                    lane < 64,
                    jnp.where(lane < 32, alive[0], alive[1]),
                    jnp.where(lane < 96, alive[2], alive[3]))
                total = total + ((v >> (lane & 31)) & 1)
            lives[pl.ds(i * 4 + u, 1), :] = total[:1]
        return carry

    lax.fori_loop(0, 8, tally, 0)
    for which, copy in copies:
        if which == 2:
            copy.wait()
    for n, k in enumerate((2, 1, 3)):
        passed[n].wait()
        prepare(lax.rem(me + 4 - k, 4))


def exchange(weight, bias, predicates, keys, valid):
    return pl.pallas_call(
        exchange_kernel,
        out_shape=(
            jax.ShapeDtypeStruct((4, 256, 256), bf16),
            jax.ShapeDtypeStruct((4, 1, D), f32),
            jax.ShapeDtypeStruct((32, 128, 128), bf16),
            jax.ShapeDtypeStruct((32, 128), i32),
            jax.ShapeDtypeStruct((KEYS, D), f32),
            jax.ShapeDtypeStruct((KEYS, D), f32),
            jax.ShapeDtypeStruct((32, 128), i32),
        ),
        in_specs=[spec(HB)] * 5,
        out_specs=(spec(VM),) * 7,
        scratch_shapes=[
            pltpu.VMEM((4, D, D), f32),
            pltpu.VMEM((MICRO, BLOCK), i32),
            pltpu.SMEM((1, MICRO), i32),
            pltpu.VMEM((4, 4, 32), i32),
            pltpu.VMEM((4, 4, 32), i32),
            pltpu.SMEM((4, 4, 32), i32),
            pltpu.SemaphoreType.DMA((3, 3)),
            pltpu.SemaphoreType.DMA((3, 3)),
            pltpu.SemaphoreType.DMA((3,)),
            pltpu.SemaphoreType.DMA((3,)),
            pltpu.SemaphoreType.DMA((7,)),
        ],
        compiler_params=pltpu.CompilerParams(collective_id=0, has_side_effects=True, vmem_limit_bytes=8 << 20),
        cost_estimate=pl.CostEstimate(flops=40_000_000_000, bytes_accessed=1 << 20, transcendentals=0),
    )(pinned(weight), pinned(bias), pinned(predicates), pinned(keys), pinned(valid))


def sections_kernel(
    rows, keys_in, w2, b, same, lives, clear_a, clear_b, v_in, table_a, table_b, ready, keys, valid, sems
):
    fetch = [pltpu.make_async_copy(keys_in, keys, sems.at[0]), pltpu.make_async_copy(v_in, valid, sems.at[1])]
    for copy in fetch:
        copy.start()

    def batch(m, carry):
        h = rows[m]
        columns = jnp.transpose(jnp.concatenate([lives[pl.ds(pl.multiple_of(m * 8, 8), 8), :]] * 16, axis=0))
        alive = jnp.concatenate([jnp.broadcast_to(columns[:, j : j + 1], (128, 128)) for j in range(8)], axis=0)
        total = jnp.zeros((BLOCK, D), f32)
        for s in range(SECTIONS):
            p = jnp.dot(jnp.concatenate(high_low(h), axis=1), w2[s], preferred_element_type=f32)
            h = h + jnp.tanh(p[:, :D] + (p[:, D:] + b[s]))
            total = total + jnp.where(alive > s, h, 0.0)
        both = jnp.concatenate(high_low(total), axis=1)
        for j in range(8):
            p = jnp.dot(same[m * 8 + j], both[j * 128 : (j + 1) * 128], preferred_element_type=f32)
            ready[pl.ds(pl.multiple_of(m * BLOCK + j * 128, 128), 128), :] = p[:, :D] + p[:, D:]
        return carry

    lax.fori_loop(0, MICRO, batch, 0)
    for copy in fetch:
        copy.wait()
    tables = (table_a, table_b)
    groups = CHUNK // GROUP

    def scatter(first, i, carry):
        u = first + i
        def load(g):
            at = [keys[u * (CHUNK // 128) + (g * GROUP + i) // 128, (g * GROUP + i) % 128] for i in range(GROUP)]
            return at, [tables[g % 2][pl.ds(k, 1), :] for k in at]

        def store(g, at, held):
            for i, k in enumerate(at):
                tables[g % 2][pl.ds(k, 1), :] = held[i] + ready[pl.ds(u * CHUNK + g * GROUP + i, 1), :]

        flying = {g: load(g) for g in range(2)}
        for g in range(groups):
            store(g, *flying.pop(g))
            if g + 2 < groups:
                flying[g + 2] = load(g + 2)
        return carry

    for m in range(MICRO):
        chunks = (valid[0, m] + CHUNK - 1) // CHUNK
        lax.fori_loop(0, chunks, functools.partial(scatter, m * (BLOCK // CHUNK)), 0)


def sections(rows, keys, w, b, same, lives, clear_a, clear_b, valid):
    return pl.pallas_call(
        sections_kernel,
        out_shape=(jax.ShapeDtypeStruct((KEYS, D), f32),) * 2,
        in_specs=[spec(VM)] * 8 + [spec(HB)],
        out_specs=(spec(VM),) * 2,
        scratch_shapes=[
            pltpu.VMEM((ROWS, D), f32),
            pltpu.SMEM((32, 128), i32),
            pltpu.SMEM((1, MICRO), i32),
            pltpu.SemaphoreType.DMA((2,)),
        ],
        input_output_aliases={6: 0, 7: 1},
        compiler_params=pltpu.CompilerParams(vmem_limit_bytes=12 << 20),
    )(rows, keys, w, b, same, lives, clear_a, clear_b, pinned(valid))


ORDERS = ((0, 1, 2), (1, 2, 0), (2, 0, 1))
BAND, PART, COUNTED = 24, 8, 8
N = 9
HEIGHT = 72


def reduce_kernel(table_a, table_b, keys, lives, sums, pair, *scratch):
    held = scratch[0:3]
    near, middle, second, last, third = (scratch[3 + i * N : 3 + (i + 1) * N] for i in range(5))
    core_recv, core_send, near_sems, far_sems = scratch[3 + 5 * N :]
    z = lax.axis_index("section")
    row = lax.axis_index("rows")
    y, x, c = row // 8, (row // 2) % 4, row % 2
    place = (z, y, x)

    def position(axis, k):
        return lax.rem(place[axis] + k, 4)

    def device(axis, k):
        at = list(place)
        at[axis] = position(axis, k)
        return (at[0], at[1] * 8 + at[2] * 2 + c)

    other = (z, y * 8 + x * 2 + (1 - c))
    peers = [device(axis, k) for axis in range(3) for k in (1, 3)] + [other]
    barrier = pltpu.get_barrier_semaphore()
    for peer in peers:
        pl.semaphore_signal(barrier, inc=1, device_id=peer, device_id_type=MESH)

    def join(i, carry):
        at = (i // 16, (i // 4) % 4, i % 4)
        pair[(*at, slice(0, 64))] = table_a[(*at, 1 - c)] + table_b[(*at, 1 - c)]
        return carry

    lax.fori_loop(0, 64, join, 0)
    pl.semaphore_wait(barrier, len(peers))

    def send(src, dst, send_sem, recv_sem, to):
        pltpu.make_async_remote_copy(
            src_ref=src, dst_ref=dst, send_sem=send_sem, recv_sem=recv_sem, device_id=to, device_id_type=MESH
        ).start()

    def wait(ref, sem):
        pltpu.make_async_copy(ref, ref, sem).wait()

    every = [0, 1, 2]

    def where_of(axes, axis, index, half=None):
        where = [slice(None)] * len(axes)
        where[axes.index(axis)] = index
        if half is not None:
            where[1 if axes[0] == axis else 0] = pl.ds(2 * half, 2)
        return tuple(where)

    def keyed(band):
        return BAND - COUNTED if band == 2 else BAND

    def swap(band, index, kind):
        at, size = where_of(every, ORDERS[band][0], index), keyed(band)
        send(
            pair.at[(*at, pl.ds(band * BAND, size))], held[band].at[(*at, pl.ds(0, size))],
            core_send.at[band], core_recv.at[band, kind], other)

    def swapped(band, kind, blocks):
        size = keyed(band)
        wait(held[band].at[0:blocks, :, :, pl.ds(0, size)], core_recv.at[band, kind])
        for k in {0: (2,), 1: (1, 3), 2: (0,)}[kind]:
            at = where_of(every, ORDERS[band][0], position(ORDERS[band][0], k))
            rows = (c, slice(band * BAND, band * BAND + size))
            held[band][(*at, slice(0, size))] += table_a[(*at, *rows)] + table_b[(*at, *rows)]

    for kind, steps in enumerate(((2,), (1, 3), (0,))):
        for band in range(3):
            for k in steps:
                swap(band, position(ORDERS[band][0], k), kind)
    sub64 = lax.broadcasted_iota(i32, (64, 128), 0)
    sub128 = lax.broadcasted_iota(i32, (128, 128), 0)

    def tally(i, found):
        for u in range(4):
            key_row = keys[pl.ds(i * 4 + u, 1), :]
            alive = lives[pl.ds(i * 4 + u, 1), :].astype(f32)
            high = jnp.where((key_row >> 7) == sub64, alive, 0.0).astype(bf16)
            low = jnp.where((key_row & 127) == sub128, 1.0, 0.0).astype(bf16)
            found = found + lax.dot_general(high, low, (((1,), (1,)), ((), ())), preferred_element_type=f32)
        return found

    found = lax.fori_loop(0, 8, tally, jnp.zeros((64, 128), f32))
    for i in range(64):
        pair[i // 16, (i // 4) % 4, i % 4, 64:72, :] = jnp.broadcast_to(found[i : i + 1], (8, 128))
    counted = held[2].at[:, :, :, pl.ds(BAND - COUNTED, COUNTED)]
    send(pair.at[:, :, :, pl.ds(64, COUNTED)], counted, core_send.at[2], core_recv.at[3, 0], other)

    def block_of(n, k, half):
        band, step = n % 3, n // 3
        axis = ORDERS[band][0]
        return held[band].at[(*where_of(every, axis, position(axis, k), half), pl.ds(step * PART, PART))]

    def hop(n, slot, recv, block, k):
        send(block, near[n].at[slot], near_sems.at[n, 3], near_sems.at[n, recv], device(ORDERS[n % 3][0], k))

    def relay(n):
        hop(n, 0, 0, block_of(n, 2, 0), 1)
        hop(n, 1, 1, block_of(n, 2, 1), 3)

    def direct(n):
        hop(n, 2, 2, block_of(n, 1, 1), 1)
        hop(n, 3, 2, block_of(n, 3, 0), 3)

    for band in range(3):
        swapped(band, 0, 1)
        for n in range(band, N - 1 if band == 2 else N, 3):
            relay(n)
    for band in range(3):
        swapped(band, 1, 2)
        for n in range(band, N - 1 if band == 2 else N, 3):
            direct(n)
    wait(counted, core_recv.at[3, 0])
    for i in range(4):
        held[2][i, :, :, BAND - COUNTED :] += pair[i, :, :, 64:72]
    relay(N - 1)
    direct(N - 1)

    def spread(n, stage, source, axes, target):
        axis = ORDERS[n % 3][stage]
        for k in (2, 1, 3):
            send(
                source.at[where_of(axes, axis, position(axis, k))], target.at[k - 1],
                far_sems.at[n, stage - 1, 0], far_sems.at[n, stage - 1, 1], device(axis, k))

    def summed(n, stage, source, axes, target):
        axis = ORDERS[n % 3][stage]
        wait(target, far_sems.at[n, stage - 1, 1])
        return (source[where_of(axes, axis, place[axis])] + target[0]) + (target[1] + target[2])

    for n in range(N):
        for half, k in ((0, 1), (1, 3)):
            wait(near[n].at[half], near_sems.at[n, half])
            block = block_of(n, k, half)
            block[...] += near[n][half]
            hop(n, 4 + half, 2, block, k)
    for band in range(3):
        swapped(band, 2, 1)
    for n in range(N):
        axis = ORDERS[n % 3][0]
        wait(near[n].at[2:6], near_sems.at[n, 2])
        middle[n][0:2] = (block_of(n, 0, 0)[...] + near[n][3]) + near[n][4]
        middle[n][2:4] = (block_of(n, 0, 1)[...] + near[n][2]) + near[n][5]
        spread(n, 1, middle[n], [i for i in every if i != axis], second[n])
    for n in range(N):
        axis = ORDERS[n % 3][0]
        last[n][...] = summed(n, 1, middle[n], [i for i in every if i != axis], second[n])
        spread(n, 2, last[n], [ORDERS[n % 3][2]], third[n])
    for n in range(N):
        start = (n % 3) * BAND + (n // 3) * PART
        sums[start : start + PART, :] = summed(n, 2, last[n], [ORDERS[n % 3][2]], third[n])
    for band in range(3):
        wait(held[band], core_send.at[band])
    for n in range(N):
        wait(near[n], near_sems.at[n, 3])
        wait(second[n], far_sems.at[n, 0, 0])
        wait(third[n], far_sems.at[n, 1, 0])


def reduce_to_owner(table_a, table_b, keys, lives):
    buffers = [pltpu.VMEM((4, 4, 4, HEIGHT, D), f32)] + [pltpu.VMEM((4, 4, 4, BAND, D), f32)] * 3
    for lead in ((6, 2, 4), (4, 4), (3, 4), (4,), (3,)):
        buffers += [pltpu.VMEM((*lead, PART, D), f32)] * N
    return pl.pallas_call(
        reduce_kernel,
        out_shape=jax.ShapeDtypeStruct((HEIGHT, D), f32),
        in_specs=[spec(VM)] * 4,
        out_specs=spec(VM),
        scratch_shapes=buffers + [
            pltpu.SemaphoreType.DMA((4, 3)),
            pltpu.SemaphoreType.DMA((3,)),
            pltpu.SemaphoreType.DMA((N, 4)),
            pltpu.SemaphoreType.DMA((N, 2, 2)),
        ],
        compiler_params=pltpu.CompilerParams(collective_id=1, has_side_effects=True, vmem_limit_bytes=20 << 20),
    )(table_a.reshape(4, 4, 4, 2, 64, D), table_b.reshape(4, 4, 4, 2, 64, D), keys, lives)


def means_kernel(sums, means, counts):
    c = lax.axis_index("rows") % 2
    line = sums[64:65, :]
    wide = jnp.transpose(jnp.broadcast_to(line, (128, 128)))
    means[...] = sums[:64] / jnp.maximum(jnp.where(c == 0, wide[:64], wide[64:]), 1.0)
    counts[...] = jnp.where(c == 0, line, pltpu.roll(line, 64, 1))[:, :64]


def means_of(sums):
    return pl.pallas_call(
        means_kernel,
        out_shape=(jax.ShapeDtypeStruct((64, D), f32), jax.ShapeDtypeStruct((1, 64), f32)),
        in_specs=[spec(VM)],
        out_specs=(spec(VM), spec(VM)),
        compiler_params=pltpu.CompilerParams(vmem_limit_bytes=1 << 20),
    )(sums)


def shards(rows_data, row_keys, valid_counts, predicates, section_weight, section_bias):
    w, b, same, lives, clear_a, clear_b, key_rows = exchange(
        section_weight, section_bias.reshape(1, 1, D), predicates.reshape(4, MICRO, 32), row_keys, valid_counts.T)
    tables = sections(rows_data, key_rows, w, b, same, lives, clear_a, clear_b, valid_counts.T)
    means, counts = means_of(reduce_to_owner(*tables, key_rows, lives))
    return means, counts.reshape(64)


def solution(mesh):
    placed = (
        P("section", "rows", None),
        P("section", "rows"),
        P("section", "rows"),
        P("section", None, "rows"),
        P("section", None, None),
        P("section", None),
    )
    return jax.shard_map(
        shards,
        mesh=mesh,
        in_specs=placed,
        out_specs=(P(("section", "rows"), None), P(("section", "rows"))),
        check_vma=False,
    )
```

```python
import functools

import jax
import jax.numpy as jnp
from jax import lax
from jax.experimental import pallas as pl
from jax.experimental.pallas import tpu as pltpu
from jax.sharding import PartitionSpec as P

KEYS = 8192
SECTIONS = 4
D = 128
MICRO = 4
BLOCK = 1024
ROWS = MICRO * BLOCK
GROUP = 8
CHUNK = 256
f32, bf16, i32 = jnp.float32, jnp.bfloat16, jnp.int32
MESH = pl.DeviceIdType.MESH
VM, SM, HB = pltpu.VMEM, pltpu.SMEM, pltpu.HBM


def spec(space):
    return pl.BlockSpec(memory_space=space)


def pinned(x):
    return pltpu.with_memory_space_constraint(x, HB)


def high_low(x):
    high = x.astype(bf16)
    return high, (x - high.astype(f32)).astype(bf16)


def exchange_kernel(
    w_in, b_in, p_in, k_in, v_in,
    w_twice, b_all, same, words, valid, table_a, table_b, key_rows,
    w_all, keys, flags, send, recv, local,
):
    me = lax.axis_index("section")
    row = lax.axis_index("rows")
    own = [
        pltpu.make_async_copy(src, dst, local.at[n])
        for n, (src, dst) in enumerate((
            (p_in, flags), (p_in.at[me], words.at[me]), (b_in.at[0], b_all.at[me]), (w_in.at[0], w_all.at[me]),
            (k_in, keys), (v_in, valid)))
    ]
    for copy in own:
        copy.start()
    barrier = pltpu.get_barrier_semaphore()
    for k in range(1, 4):
        pl.semaphore_signal(barrier, inc=1, device_id=(lax.rem(me + k, 4), row), device_id_type=MESH)

    def clear(i, carry):
        at = pl.ds(pl.multiple_of(i * 512, 512), 512)
        table_a[at, :] = jnp.zeros((512, D), f32)
        table_b[at, :] = jnp.zeros((512, D), f32)
        return carry

    lax.fori_loop(0, KEYS // 512, clear, 0)
    for copy in own[:4]:
        copy.wait()
    pl.semaphore_wait(barrier, 3)
    copies = []
    for n, k in enumerate((2, 1, 3)):
        to = lax.rem(me + k, 4)
        for a, (src, dst) in enumerate((
            (flags.at[to], words.at[me]), (w_all.at[me], w_all.at[me]), (b_all.at[me], b_all.at[me]),
        )):
            copies.append((a, pltpu.make_async_remote_copy(
                src_ref=src, dst_ref=dst, send_sem=send.at[n, a], recv_sem=recv.at[n, a],
                device_id=(to, row), device_id_type=MESH)))
    for a in range(3):
        for which, copy in copies:
            if which == a:
                copy.start()

    def prepare(origin):
        top = jnp.concatenate(high_low(w_all[origin]), axis=1)
        w_twice[origin] = jnp.concatenate([top, top], axis=0)

    prepare(me)
    own[4].wait()
    own[5].wait()
    group_i = (lax.broadcasted_iota(i32, (1, 128), 1) // GROUP) * KEYS

    for m in range(MICRO):
        for j in range(8):
            key_rows[m * 8 + j : m * 8 + j + 1, :] = keys[m : m + 1, j * 128 : (j + 1) * 128]

    def key_row_at(m, j):
        return key_rows[pl.ds(m * 8 + j, 1), :]

    def sameness(i, carry):
        for u in range(4):
            key_row = key_row_at(i // 2, (i % 2) * 4 + u) + group_i
            key_col = jnp.transpose(jnp.broadcast_to(key_row, (128, 128)))
            same[i * 4 + u] = jnp.where(key_col == key_row, 1.0, 0.0).astype(bf16)
        return carry

    lax.fori_loop(0, 8, sameness, 0)
    for which, copy in copies:
        if which == 0:
            copy.wait()
    for which, copy in copies:
        if which == 2:
            copy.wait()
    for n, k in enumerate((2, 1, 3)):
        copies[3 * n + 1][1].wait()
        prepare(lax.rem(me + 4 - k, 4))


def exchange(weight, bias, predicates, keys, valid):
    return pl.pallas_call(
        exchange_kernel,
        out_shape=(
            jax.ShapeDtypeStruct((4, 256, 256), bf16),
            jax.ShapeDtypeStruct((4, 1, D), f32),
            jax.ShapeDtypeStruct((32, 128, 128), bf16),
            jax.ShapeDtypeStruct((SECTIONS, MICRO, 32), i32),
            jax.ShapeDtypeStruct((1, MICRO), i32),
            jax.ShapeDtypeStruct((KEYS, D), f32),
            jax.ShapeDtypeStruct((KEYS, D), f32),
            jax.ShapeDtypeStruct((32, 128), i32),
        ),
        in_specs=[spec(HB)] * 5,
        out_specs=(spec(VM),) * 8,
        scratch_shapes=[
            pltpu.VMEM((4, D, D), f32),
            pltpu.VMEM((MICRO, BLOCK), i32),
            pltpu.VMEM((4, 4, 32), i32),
            pltpu.SemaphoreType.DMA((3, 3)),
            pltpu.SemaphoreType.DMA((3, 3)),
            pltpu.SemaphoreType.DMA((6,)),
        ],
        compiler_params=pltpu.CompilerParams(collective_id=0, has_side_effects=True, vmem_limit_bytes=8 << 20),
        cost_estimate=pl.CostEstimate(flops=40_000_000_000, bytes_accessed=1 << 20, transcendentals=0),
    )(pinned(weight), pinned(bias), pinned(predicates), pinned(keys), pinned(valid))


def sections_kernel(
    rows, keys_in, w2, b, same, words, limits, clear_a, clear_b, v_in, table_a, table_b, lives, ready, keys, valid, sems
):
    fetch = [pltpu.make_async_copy(keys_in, keys, sems.at[0]), pltpu.make_async_copy(v_in, valid, sems.at[1])]
    for copy in fetch:
        copy.start()

    sub = lax.broadcasted_iota(i32, (8, 128), 0)
    lane = lax.broadcasted_iota(i32, (8, 128), 1)
    for m in range(MICRO):
        alive = jnp.where(sub * 128 + lane < limits[0:1, m : m + 1], 1, 0)
        found = jnp.zeros((8, 128), i32)
        for s in range(SECTIONS):
            line = jnp.concatenate([words[s, m : m + 1, :]] * 4, axis=1)
            word = jnp.take_along_axis(
                jnp.broadcast_to(line, (8, 128)), sub * 4 + (lane >> 5), axis=1, mode="promise_in_bounds")
            alive = alive & (word >> (lane & 31))
            found = found + alive
        lives[m * 8 : (m + 1) * 8, :] = found

    def batch(m, carry):
        h = rows[m]
        columns = jnp.transpose(jnp.concatenate([lives[pl.ds(pl.multiple_of(m * 8, 8), 8), :]] * 16, axis=0))
        alive = jnp.concatenate([jnp.broadcast_to(columns[:, j : j + 1], (128, 128)) for j in range(8)], axis=0)
        total = jnp.zeros((BLOCK, D), f32)
        for s in range(SECTIONS):
            p = jnp.dot(jnp.concatenate(high_low(h), axis=1), w2[s], preferred_element_type=f32)
            h = h + jnp.tanh(p[:, :D] + (p[:, D:] + b[s]))
            total = total + jnp.where(alive > s, h, 0.0)
        both = jnp.concatenate(high_low(total), axis=1)
        for j in range(8):
            p = jnp.dot(same[m * 8 + j], both[j * 128 : (j + 1) * 128], preferred_element_type=f32)
            ready[pl.ds(pl.multiple_of(m * BLOCK + j * 128, 128), 128), :] = p[:, :D] + p[:, D:]
        return carry

    lax.fori_loop(0, MICRO, batch, 0)
    for copy in fetch:
        copy.wait()
    tables = (table_a, table_b)
    groups = CHUNK // GROUP

    def scatter(first, i, carry):
        u = first + i
        def load(g):
            at = [keys[u * (CHUNK // 128) + (g * GROUP + i) // 128, (g * GROUP + i) % 128] for i in range(GROUP)]
            return at, [tables[g % 2][pl.ds(k, 1), :] for k in at]

        def store(g, at, held):
            for i, k in enumerate(at):
                tables[g % 2][pl.ds(k, 1), :] = held[i] + ready[pl.ds(u * CHUNK + g * GROUP + i, 1), :]

        flying = {g: load(g) for g in range(2)}
        for g in range(groups):
            store(g, *flying.pop(g))
            if g + 2 < groups:
                flying[g + 2] = load(g + 2)
        return carry

    for m in range(MICRO):
        chunks = (valid[0, m] + CHUNK - 1) // CHUNK
        lax.fori_loop(0, chunks, functools.partial(scatter, m * (BLOCK // CHUNK)), 0)


def sections(rows, keys, w, b, same, words, limits, clear_a, clear_b, valid):
    return pl.pallas_call(
        sections_kernel,
        out_shape=(jax.ShapeDtypeStruct((KEYS, D), f32),) * 2 + (jax.ShapeDtypeStruct((32, 128), i32),),
        in_specs=[spec(VM)] * 9 + [spec(HB)],
        out_specs=(spec(VM),) * 3,
        scratch_shapes=[
            pltpu.VMEM((ROWS, D), f32),
            pltpu.SMEM((32, 128), i32),
            pltpu.SMEM((1, MICRO), i32),
            pltpu.SemaphoreType.DMA((2,)),
        ],
        input_output_aliases={7: 0, 8: 1},
        compiler_params=pltpu.CompilerParams(vmem_limit_bytes=12 << 20),
    )(rows, keys, w, b, same, words, limits, clear_a, clear_b, pinned(valid))


ORDERS = ((0, 1, 2), (1, 2, 0), (2, 0, 1))
BAND, PART, COUNTED = 24, 8, 8
N = 9
HEIGHT = 72


def reduce_kernel(table_a, table_b, keys, lives, sums, pair, *scratch):
    held = scratch[0:3]
    near, middle, second, last, third = (scratch[3 + i * N : 3 + (i + 1) * N] for i in range(5))
    core_recv, core_send, near_sems, far_sems = scratch[3 + 5 * N :]
    z = lax.axis_index("section")
    row = lax.axis_index("rows")
    y, x, c = row // 8, (row // 2) % 4, row % 2
    place = (z, y, x)

    def position(axis, k):
        return lax.rem(place[axis] + k, 4)

    def device(axis, k):
        at = list(place)
        at[axis] = position(axis, k)
        return (at[0], at[1] * 8 + at[2] * 2 + c)

    other = (z, y * 8 + x * 2 + (1 - c))
    peers = [device(axis, k) for axis in range(3) for k in (1, 3)] + [other]
    barrier = pltpu.get_barrier_semaphore()
    for peer in peers:
        pl.semaphore_signal(barrier, inc=1, device_id=peer, device_id_type=MESH)

    def join(i, carry):
        at = (i // 16, (i // 4) % 4, i % 4)
        pair[(*at, slice(0, 64))] = table_a[(*at, 1 - c)] + table_b[(*at, 1 - c)]
        return carry

    lax.fori_loop(0, 64, join, 0)
    pl.semaphore_wait(barrier, len(peers))

    def send(src, dst, send_sem, recv_sem, to):
        pltpu.make_async_remote_copy(
            src_ref=src, dst_ref=dst, send_sem=send_sem, recv_sem=recv_sem, device_id=to, device_id_type=MESH
        ).start()

    def wait(ref, sem):
        pltpu.make_async_copy(ref, ref, sem).wait()

    every = [0, 1, 2]

    def where_of(axes, axis, index, half=None):
        where = [slice(None)] * len(axes)
        where[axes.index(axis)] = index
        if half is not None:
            where[1 if axes[0] == axis else 0] = pl.ds(2 * half, 2)
        return tuple(where)

    def keyed(band):
        return BAND - COUNTED if band == 2 else BAND

    def swap(band, index, kind):
        at, size = where_of(every, ORDERS[band][0], index), keyed(band)
        send(
            pair.at[(*at, pl.ds(band * BAND, size))], held[band].at[(*at, pl.ds(0, size))],
            core_send.at[band], core_recv.at[band, kind], other)

    def swapped(band, kind, blocks):
        size = keyed(band)
        wait(held[band].at[0:blocks, :, :, pl.ds(0, size)], core_recv.at[band, kind])
        for k in {0: (2,), 1: (1, 3), 2: (0,)}[kind]:
            at = where_of(every, ORDERS[band][0], position(ORDERS[band][0], k))
            rows = (c, slice(band * BAND, band * BAND + size))
            held[band][(*at, slice(0, size))] += table_a[(*at, *rows)] + table_b[(*at, *rows)]

    for kind, steps in enumerate(((2,), (1, 3), (0,))):
        for band in range(3):
            for k in steps:
                swap(band, position(ORDERS[band][0], k), kind)
    sub64 = lax.broadcasted_iota(i32, (64, 128), 0)
    sub128 = lax.broadcasted_iota(i32, (128, 128), 0)

    def tally(i, found):
        for u in range(4):
            key_row = keys[pl.ds(i * 4 + u, 1), :]
            alive = lives[pl.ds(i * 4 + u, 1), :].astype(f32)
            high = jnp.where((key_row >> 7) == sub64, alive, 0.0).astype(bf16)
            low = jnp.where((key_row & 127) == sub128, 1.0, 0.0).astype(bf16)
            found = found + lax.dot_general(high, low, (((1,), (1,)), ((), ())), preferred_element_type=f32)
        return found

    found = lax.fori_loop(0, 8, tally, jnp.zeros((64, 128), f32))
    for i in range(64):
        pair[i // 16, (i // 4) % 4, i % 4, 64:72, :] = jnp.broadcast_to(found[i : i + 1], (8, 128))
    counted = held[2].at[:, :, :, pl.ds(BAND - COUNTED, COUNTED)]
    send(pair.at[:, :, :, pl.ds(64, COUNTED)], counted, core_send.at[2], core_recv.at[3, 0], other)

    def block_of(n, k, half):
        band, step = n % 3, n // 3
        axis = ORDERS[band][0]
        return held[band].at[(*where_of(every, axis, position(axis, k), half), pl.ds(step * PART, PART))]

    def hop(n, slot, recv, block, k):
        send(block, near[n].at[slot], near_sems.at[n, 3], near_sems.at[n, recv], device(ORDERS[n % 3][0], k))

    def relay(n):
        hop(n, 0, 0, block_of(n, 2, 0), 1)
        hop(n, 1, 1, block_of(n, 2, 1), 3)

    def direct(n):
        hop(n, 2, 2, block_of(n, 1, 1), 1)
        hop(n, 3, 2, block_of(n, 3, 0), 3)

    for band in range(3):
        swapped(band, 0, 1)
        for n in range(band, N - 1 if band == 2 else N, 3):
            relay(n)
    for band in range(3):
        swapped(band, 1, 2)
        for n in range(band, N - 1 if band == 2 else N, 3):
            direct(n)
    wait(counted, core_recv.at[3, 0])
    for i in range(4):
        held[2][i, :, :, BAND - COUNTED :] += pair[i, :, :, 64:72]
    relay(N - 1)
    direct(N - 1)

    def spread(n, stage, source, axes, target):
        axis = ORDERS[n % 3][stage]
        for k in (2, 1, 3):
            send(
                source.at[where_of(axes, axis, position(axis, k))], target.at[k - 1],
                far_sems.at[n, stage - 1, 0], far_sems.at[n, stage - 1, 1], device(axis, k))

    def summed(n, stage, source, axes, target):
        axis = ORDERS[n % 3][stage]
        wait(target, far_sems.at[n, stage - 1, 1])
        return (source[where_of(axes, axis, place[axis])] + target[0]) + (target[1] + target[2])

    for n in range(N):
        for half, k in ((0, 1), (1, 3)):
            wait(near[n].at[half], near_sems.at[n, half])
            block = block_of(n, k, half)
            block[...] += near[n][half]
            hop(n, 4 + half, 2, block, k)
    for band in range(3):
        swapped(band, 2, 1)
    for n in range(N):
        axis = ORDERS[n % 3][0]
        wait(near[n].at[2:6], near_sems.at[n, 2])
        middle[n][0:2] = (block_of(n, 0, 0)[...] + near[n][3]) + near[n][4]
        middle[n][2:4] = (block_of(n, 0, 1)[...] + near[n][2]) + near[n][5]
        spread(n, 1, middle[n], [i for i in every if i != axis], second[n])
    for n in range(N):
        axis = ORDERS[n % 3][0]
        last[n][...] = summed(n, 1, middle[n], [i for i in every if i != axis], second[n])
        spread(n, 2, last[n], [ORDERS[n % 3][2]], third[n])
    for n in range(N):
        start = (n % 3) * BAND + (n // 3) * PART
        sums[start : start + PART, :] = summed(n, 2, last[n], [ORDERS[n % 3][2]], third[n])
    for band in range(3):
        wait(held[band], core_send.at[band])
    for n in range(N):
        wait(near[n], near_sems.at[n, 3])
        wait(second[n], far_sems.at[n, 0, 0])
        wait(third[n], far_sems.at[n, 1, 0])


def reduce_to_owner(table_a, table_b, keys, lives):
    buffers = [pltpu.VMEM((4, 4, 4, HEIGHT, D), f32)] + [pltpu.VMEM((4, 4, 4, BAND, D), f32)] * 3
    for lead in ((6, 2, 4), (4, 4), (3, 4), (4,), (3,)):
        buffers += [pltpu.VMEM((*lead, PART, D), f32)] * N
    return pl.pallas_call(
        reduce_kernel,
        out_shape=jax.ShapeDtypeStruct((HEIGHT, D), f32),
        in_specs=[spec(VM)] * 4,
        out_specs=spec(VM),
        scratch_shapes=buffers + [
            pltpu.SemaphoreType.DMA((4, 3)),
            pltpu.SemaphoreType.DMA((3,)),
            pltpu.SemaphoreType.DMA((N, 4)),
            pltpu.SemaphoreType.DMA((N, 2, 2)),
        ],
        compiler_params=pltpu.CompilerParams(collective_id=1, has_side_effects=True, vmem_limit_bytes=20 << 20),
    )(table_a.reshape(4, 4, 4, 2, 64, D), table_b.reshape(4, 4, 4, 2, 64, D), keys, lives)


def means_kernel(sums, means, counts):
    c = lax.axis_index("rows") % 2
    line = sums[64:65, :]
    wide = jnp.transpose(jnp.broadcast_to(line, (128, 128)))
    means[...] = sums[:64] / jnp.maximum(jnp.where(c == 0, wide[:64], wide[64:]), 1.0)
    counts[...] = jnp.where(c == 0, line, pltpu.roll(line, 64, 1))[:, :64]


def means_of(sums):
    return pl.pallas_call(
        means_kernel,
        out_shape=(jax.ShapeDtypeStruct((64, D), f32), jax.ShapeDtypeStruct((1, 64), f32)),
        in_specs=[spec(VM)],
        out_specs=(spec(VM), spec(VM)),
        compiler_params=pltpu.CompilerParams(vmem_limit_bytes=1 << 20),
    )(sums)


def shards(rows_data, row_keys, valid_counts, predicates, section_weight, section_bias):
    w, b, same, words, limits, clear_a, clear_b, key_rows = exchange(
        section_weight, section_bias.reshape(1, 1, D), predicates.reshape(4, MICRO, 32), row_keys, valid_counts.T)
    table_a, table_b, lives = sections(
        rows_data, key_rows, w, b, same, words, limits, clear_a, clear_b, valid_counts.T)
    means, counts = means_of(reduce_to_owner(table_a, table_b, key_rows, lives))
    return means, counts.reshape(64)


def solution(mesh):
    placed = (
        P("section", "rows", None),
        P("section", "rows"),
        P("section", "rows"),
        P("section", None, "rows"),
        P("section", None, None),
        P("section", None),
    )
    return jax.shard_map(
        shards,
        mesh=mesh,
        in_specs=placed,
        out_specs=(P(("section", "rows"), None), P(("section", "rows"))),
        check_vma=False,
    )
```

```python
import functools

import jax
import jax.numpy as jnp
from jax import lax
from jax.experimental import pallas as pl
from jax.experimental.pallas import tpu as pltpu
from jax.sharding import PartitionSpec as P

KEYS = 8192
SECTIONS = 4
D = 128
MICRO = 4
BLOCK = 1024
ROWS = MICRO * BLOCK
GROUP = 8
TILE = 128
BATCH = 8
SURE = 256
f32, bf16, i32 = jnp.float32, jnp.bfloat16, jnp.int32
MESH = pl.DeviceIdType.MESH
VM, SM, HB = pltpu.VMEM, pltpu.SMEM, pltpu.HBM


def spec(space):
    return pl.BlockSpec(memory_space=space)


def pinned(x):
    return pltpu.with_memory_space_constraint(x, HB)


def high_low(x):
    high = x.astype(bf16)
    return high, (x - high.astype(f32)).astype(bf16)


def exchange_kernel(
    w_in, b_in, p_in, k_in, v_in,
    w_twice, b_all, same, words, valid, table_a, table_b, key_rows,
    w_all, keys, flags, send, recv, local,
):
    me = lax.axis_index("section")
    row = lax.axis_index("rows")
    own = [
        pltpu.make_async_copy(src, dst, local.at[n])
        for n, (src, dst) in enumerate((
            (p_in, flags), (p_in.at[me], words.at[me]), (b_in.at[0], b_all.at[me]), (w_in.at[0], w_all.at[me]),
            (k_in, keys), (v_in, valid)))
    ]
    for copy in own:
        copy.start()
    barrier = pltpu.get_barrier_semaphore()
    for k in range(1, 4):
        pl.semaphore_signal(barrier, inc=1, device_id=(lax.rem(me + k, 4), row), device_id_type=MESH)

    def clear(i, carry):
        at = pl.ds(pl.multiple_of(i * 512, 512), 512)
        table_a[at, :] = jnp.zeros((512, D), f32)
        table_b[at, :] = jnp.zeros((512, D), f32)
        return carry

    lax.fori_loop(0, KEYS // 512, clear, 0)
    for copy in own[:4]:
        copy.wait()
    pl.semaphore_wait(barrier, 3)
    copies = []
    for n, k in enumerate((2, 1, 3)):
        to = lax.rem(me + k, 4)
        for a, (src, dst) in enumerate((
            (flags.at[to], words.at[me]), (w_all.at[me], w_all.at[me]), (b_all.at[me], b_all.at[me]),
        )):
            copies.append((a, pltpu.make_async_remote_copy(
                src_ref=src, dst_ref=dst, send_sem=send.at[n, a], recv_sem=recv.at[n, a],
                device_id=(to, row), device_id_type=MESH)))
    for a in range(3):
        for which, copy in copies:
            if which == a:
                copy.start()

    def prepare(origin):
        top = jnp.concatenate(high_low(w_all[origin]), axis=1)
        w_twice[origin] = jnp.concatenate([top, top], axis=0)

    prepare(me)
    own[4].wait()
    own[5].wait()
    group_i = (lax.broadcasted_iota(i32, (1, 128), 1) // GROUP) * KEYS

    for m in range(MICRO):
        for j in range(8):
            key_rows[m * 8 + j : m * 8 + j + 1, :] = keys[m : m + 1, j * 128 : (j + 1) * 128]

    def key_row_at(m, j):
        return key_rows[pl.ds(m * 8 + j, 1), :]

    def sameness(i, carry):
        for u in range(4):
            key_row = key_row_at(i // 2, (i % 2) * 4 + u) + group_i
            key_col = jnp.transpose(jnp.broadcast_to(key_row, (128, 128)))
            same[i * 4 + u] = jnp.where(key_col == key_row, 1.0, 0.0).astype(bf16)
        return carry

    lax.fori_loop(0, 8, sameness, 0)
    for which, copy in copies:
        if which == 0:
            copy.wait()
    for which, copy in copies:
        if which == 2:
            copy.wait()
    for n, k in enumerate((2, 1, 3)):
        copies[3 * n + 1][1].wait()
        prepare(lax.rem(me + 4 - k, 4))


def exchange(weight, bias, predicates, keys, valid):
    return pl.pallas_call(
        exchange_kernel,
        out_shape=(
            jax.ShapeDtypeStruct((4, 256, 256), bf16),
            jax.ShapeDtypeStruct((4, 1, D), f32),
            jax.ShapeDtypeStruct((32, 128, 128), bf16),
            jax.ShapeDtypeStruct((SECTIONS, MICRO, 32), i32),
            jax.ShapeDtypeStruct((1, MICRO), i32),
            jax.ShapeDtypeStruct((KEYS, D), f32),
            jax.ShapeDtypeStruct((KEYS, D), f32),
            jax.ShapeDtypeStruct((32, 128), i32),
        ),
        in_specs=[spec(HB)] * 5,
        out_specs=(spec(VM),) * 8,
        scratch_shapes=[
            pltpu.VMEM((4, D, D), f32),
            pltpu.VMEM((MICRO, BLOCK), i32),
            pltpu.VMEM((4, 4, 32), i32),
            pltpu.SemaphoreType.DMA((3, 3)),
            pltpu.SemaphoreType.DMA((3, 3)),
            pltpu.SemaphoreType.DMA((6,)),
        ],
        compiler_params=pltpu.CompilerParams(collective_id=0, has_side_effects=True, vmem_limit_bytes=8 << 20),
        cost_estimate=pl.CostEstimate(flops=40_000_000_000, bytes_accessed=1 << 20, transcendentals=0),
    )(pinned(weight), pinned(bias), pinned(predicates), pinned(keys), pinned(valid))


def sections_kernel(
    rows, keys_in, w2, b, same, words, limits, clear_a, clear_b, v_in, table_a, table_b, lives, ready, keys, valid, sems
):
    fetch = [pltpu.make_async_copy(keys_in, keys, sems.at[0]), pltpu.make_async_copy(v_in, valid, sems.at[1])]
    for copy in fetch:
        copy.start()

    sub = lax.broadcasted_iota(i32, (8, 128), 0)
    lane = lax.broadcasted_iota(i32, (8, 128), 1)
    for m in range(MICRO):
        alive = jnp.where(sub * 128 + lane < limits[0:1, m : m + 1], 1, 0)
        found = jnp.zeros((8, 128), i32)
        for s in range(SECTIONS):
            line = jnp.concatenate([words[s, m : m + 1, :]] * 4, axis=1)
            word = jnp.take_along_axis(
                jnp.broadcast_to(line, (8, 128)), sub * 4 + (lane >> 5), axis=1, mode="promise_in_bounds")
            alive = alive & (word >> (lane & 31))
            found = found + alive
        lives[m * 8 : (m + 1) * 8, :] = found

    def compute(slot, tiles):
        h = jnp.concatenate([rows[t // 8, pl.ds(pl.multiple_of((t % 8) * TILE, TILE), TILE), :] for t in tiles], axis=0)
        levels = jnp.concatenate([lives[pl.ds(t, 1), :] for t in tiles], axis=0)
        columns = jnp.transpose(jnp.concatenate([levels] * 16, axis=0))
        alive = jnp.concatenate([jnp.broadcast_to(columns[:, j : j + 1], (128, 128)) for j in range(8)], axis=0)
        total = jnp.zeros((BATCH * TILE, D), f32)
        for s in range(SECTIONS):
            p = jnp.dot(jnp.concatenate(high_low(h), axis=1), w2[s], preferred_element_type=f32)
            h = h + jnp.tanh(p[:, :D] + (p[:, D:] + b[s]))
            total = total + jnp.where(alive > s, h, 0.0)
        both = jnp.concatenate(high_low(total), axis=1)
        for j, t in enumerate(tiles):
            p = jnp.dot(same[t], both[j * TILE : (j + 1) * TILE], preferred_element_type=f32)
            ready[pl.ds(pl.multiple_of((slot + j) * TILE, TILE), TILE), :] = p[:, :D] + p[:, D:]

    compute(0, [m * 8 + j for m in range(MICRO) for j in range(SURE // TILE)])
    for copy in fetch:
        copy.wait()
    ends = [0]
    for m in range(MICRO):
        ends.append(ends[-1] + (valid[0, m] - SURE + TILE - 1) // TILE)

    def tile_at(i):
        tile = SURE // TILE + i
        for m in range(1, MICRO):
            tile = jnp.where(i >= ends[m], m * 8 + SURE // TILE + i - ends[m], tile)
        return jnp.minimum(tile, 31)

    def batch(n, carry):
        compute(BATCH + n * BATCH, [tile_at(n * BATCH + j) for j in range(BATCH)])
        return carry

    lax.fori_loop(0, (ends[MICRO] + BATCH - 1) // BATCH, batch, 0)
    tables = (table_a, table_b)
    groups = TILE // GROUP

    def scatter(slot, tile):
        def load(g):
            at = [keys[tile, g * GROUP + i] for i in range(GROUP)]
            return at, [tables[g % 2][pl.ds(k, 1), :] for k in at]

        def store(g, at, held):
            for i, k in enumerate(at):
                tables[g % 2][pl.ds(k, 1), :] = held[i] + ready[pl.ds(slot * TILE + g * GROUP + i, 1), :]

        flying = {g: load(g) for g in range(2)}
        for g in range(groups):
            store(g, *flying.pop(g))
            if g + 2 < groups:
                flying[g + 2] = load(g + 2)

    def sure(i, carry):
        scatter(i, (i // 2) * 8 + i % 2)
        return carry

    def rest(i, carry):
        scatter(BATCH + i, tile_at(i))
        return carry

    lax.fori_loop(0, BATCH, sure, 0)
    lax.fori_loop(0, ends[MICRO], rest, 0)


def sections(rows, keys, w, b, same, words, limits, clear_a, clear_b, valid):
    return pl.pallas_call(
        sections_kernel,
        out_shape=(jax.ShapeDtypeStruct((KEYS, D), f32),) * 2 + (jax.ShapeDtypeStruct((32, 128), i32),),
        in_specs=[spec(VM)] * 9 + [spec(HB)],
        out_specs=(spec(VM),) * 3,
        scratch_shapes=[
            pltpu.VMEM((ROWS, D), f32),
            pltpu.SMEM((32, 128), i32),
            pltpu.SMEM((1, MICRO), i32),
            pltpu.SemaphoreType.DMA((2,)),
        ],
        input_output_aliases={7: 0, 8: 1},
        compiler_params=pltpu.CompilerParams(vmem_limit_bytes=12 << 20),
    )(rows, keys, w, b, same, words, limits, clear_a, clear_b, pinned(valid))


ORDERS = ((0, 1, 2), (1, 2, 0), (2, 0, 1))
BAND, PART, COUNTED = 24, 8, 8
N = 9
HEIGHT = 72


def reduce_kernel(table_a, table_b, keys, lives, sums, pair, *scratch):
    held = scratch[0:3]
    near, middle, second, last, third = (scratch[3 + i * N : 3 + (i + 1) * N] for i in range(5))
    core_recv, core_send, near_sems, far_sems = scratch[3 + 5 * N :]
    z = lax.axis_index("section")
    row = lax.axis_index("rows")
    y, x, c = row // 8, (row // 2) % 4, row % 2
    place = (z, y, x)

    def position(axis, k):
        return lax.rem(place[axis] + k, 4)

    def device(axis, k):
        at = list(place)
        at[axis] = position(axis, k)
        return (at[0], at[1] * 8 + at[2] * 2 + c)

    other = (z, y * 8 + x * 2 + (1 - c))
    peers = [device(axis, k) for axis in range(3) for k in (1, 3)] + [other]
    barrier = pltpu.get_barrier_semaphore()
    for peer in peers:
        pl.semaphore_signal(barrier, inc=1, device_id=peer, device_id_type=MESH)

    def join(i, carry):
        at = (i // 16, (i // 4) % 4, i % 4)
        pair[(*at, slice(0, 64))] = table_a[(*at, 1 - c)] + table_b[(*at, 1 - c)]
        return carry

    lax.fori_loop(0, 64, join, 0)
    pl.semaphore_wait(barrier, len(peers))

    def send(src, dst, send_sem, recv_sem, to):
        pltpu.make_async_remote_copy(
            src_ref=src, dst_ref=dst, send_sem=send_sem, recv_sem=recv_sem, device_id=to, device_id_type=MESH
        ).start()

    def wait(ref, sem):
        pltpu.make_async_copy(ref, ref, sem).wait()

    every = [0, 1, 2]

    def where_of(axes, axis, index, half=None):
        where = [slice(None)] * len(axes)
        where[axes.index(axis)] = index
        if half is not None:
            where[1 if axes[0] == axis else 0] = pl.ds(2 * half, 2)
        return tuple(where)

    def keyed(band):
        return BAND - COUNTED if band == 2 else BAND

    def swap(band, index, kind):
        at, size = where_of(every, ORDERS[band][0], index), keyed(band)
        send(
            pair.at[(*at, pl.ds(band * BAND, size))], held[band].at[(*at, pl.ds(0, size))],
            core_send.at[band], core_recv.at[band, kind], other)

    def swapped(band, kind, blocks):
        size = keyed(band)
        wait(held[band].at[0:blocks, :, :, pl.ds(0, size)], core_recv.at[band, kind])
        for k in {0: (2,), 1: (1, 3), 2: (0,)}[kind]:
            at = where_of(every, ORDERS[band][0], position(ORDERS[band][0], k))
            rows = (c, slice(band * BAND, band * BAND + size))
            held[band][(*at, slice(0, size))] += table_a[(*at, *rows)] + table_b[(*at, *rows)]

    for kind, steps in enumerate(((2,), (1, 3), (0,))):
        for band in range(3):
            for k in steps:
                swap(band, position(ORDERS[band][0], k), kind)
    sub64 = lax.broadcasted_iota(i32, (64, 128), 0)
    sub128 = lax.broadcasted_iota(i32, (128, 128), 0)

    def tally(i, found):
        for u in range(4):
            key_row = keys[pl.ds(i * 4 + u, 1), :]
            alive = lives[pl.ds(i * 4 + u, 1), :].astype(f32)
            high = jnp.where((key_row >> 7) == sub64, alive, 0.0).astype(bf16)
            low = jnp.where((key_row & 127) == sub128, 1.0, 0.0).astype(bf16)
            found = found + lax.dot_general(high, low, (((1,), (1,)), ((), ())), preferred_element_type=f32)
        return found

    found = lax.fori_loop(0, 8, tally, jnp.zeros((64, 128), f32))
    for i in range(64):
        pair[i // 16, (i // 4) % 4, i % 4, 64:72, :] = jnp.broadcast_to(found[i : i + 1], (8, 128))
    counted = held[2].at[:, :, :, pl.ds(BAND - COUNTED, COUNTED)]
    send(pair.at[:, :, :, pl.ds(64, COUNTED)], counted, core_send.at[2], core_recv.at[3, 0], other)

    def block_of(n, k, half):
        band, step = n % 3, n // 3
        axis = ORDERS[band][0]
        return held[band].at[(*where_of(every, axis, position(axis, k), half), pl.ds(step * PART, PART))]

    def hop(n, slot, recv, block, k):
        send(block, near[n].at[slot], near_sems.at[n, 3], near_sems.at[n, recv], device(ORDERS[n % 3][0], k))

    def relay(n):
        hop(n, 0, 0, block_of(n, 2, 0), 1)
        hop(n, 1, 1, block_of(n, 2, 1), 3)

    def direct(n):
        hop(n, 2, 2, block_of(n, 1, 1), 1)
        hop(n, 3, 2, block_of(n, 3, 0), 3)

    for band in range(3):
        swapped(band, 0, 1)
        for n in range(band, N - 1 if band == 2 else N, 3):
            relay(n)
    for band in range(3):
        swapped(band, 1, 2)
        for n in range(band, N - 1 if band == 2 else N, 3):
            direct(n)
    wait(counted, core_recv.at[3, 0])
    for i in range(4):
        held[2][i, :, :, BAND - COUNTED :] += pair[i, :, :, 64:72]
    relay(N - 1)
    direct(N - 1)

    def spread(n, stage, source, axes, target):
        axis = ORDERS[n % 3][stage]
        for k in (2, 1, 3):
            send(
                source.at[where_of(axes, axis, position(axis, k))], target.at[k - 1],
                far_sems.at[n, stage - 1, 0], far_sems.at[n, stage - 1, 1], device(axis, k))

    def summed(n, stage, source, axes, target):
        axis = ORDERS[n % 3][stage]
        wait(target, far_sems.at[n, stage - 1, 1])
        return (source[where_of(axes, axis, place[axis])] + target[0]) + (target[1] + target[2])

    for n in range(N):
        for half, k in ((0, 1), (1, 3)):
            wait(near[n].at[half], near_sems.at[n, half])
            block = block_of(n, k, half)
            block[...] += near[n][half]
            hop(n, 4 + half, 2, block, k)
    for band in range(3):
        swapped(band, 2, 1)
    for n in range(N):
        axis = ORDERS[n % 3][0]
        wait(near[n].at[2:6], near_sems.at[n, 2])
        middle[n][0:2] = (block_of(n, 0, 0)[...] + near[n][3]) + near[n][4]
        middle[n][2:4] = (block_of(n, 0, 1)[...] + near[n][2]) + near[n][5]
        spread(n, 1, middle[n], [i for i in every if i != axis], second[n])
    for n in range(N):
        axis = ORDERS[n % 3][0]
        last[n][...] = summed(n, 1, middle[n], [i for i in every if i != axis], second[n])
        spread(n, 2, last[n], [ORDERS[n % 3][2]], third[n])
    for n in range(N):
        start = (n % 3) * BAND + (n // 3) * PART
        sums[start : start + PART, :] = summed(n, 2, last[n], [ORDERS[n % 3][2]], third[n])
    for band in range(3):
        wait(held[band], core_send.at[band])
    for n in range(N):
        wait(near[n], near_sems.at[n, 3])
        wait(second[n], far_sems.at[n, 0, 0])
        wait(third[n], far_sems.at[n, 1, 0])


def reduce_to_owner(table_a, table_b, keys, lives):
    buffers = [pltpu.VMEM((4, 4, 4, HEIGHT, D), f32)] + [pltpu.VMEM((4, 4, 4, BAND, D), f32)] * 3
    for lead in ((6, 2, 4), (4, 4), (3, 4), (4,), (3,)):
        buffers += [pltpu.VMEM((*lead, PART, D), f32)] * N
    return pl.pallas_call(
        reduce_kernel,
        out_shape=jax.ShapeDtypeStruct((HEIGHT, D), f32),
        in_specs=[spec(VM)] * 4,
        out_specs=spec(VM),
        scratch_shapes=buffers + [
            pltpu.SemaphoreType.DMA((4, 3)),
            pltpu.SemaphoreType.DMA((3,)),
            pltpu.SemaphoreType.DMA((N, 4)),
            pltpu.SemaphoreType.DMA((N, 2, 2)),
        ],
        compiler_params=pltpu.CompilerParams(collective_id=1, has_side_effects=True, vmem_limit_bytes=20 << 20),
    )(table_a.reshape(4, 4, 4, 2, 64, D), table_b.reshape(4, 4, 4, 2, 64, D), keys, lives)


def means_kernel(sums, means, counts):
    c = lax.axis_index("rows") % 2
    line = sums[64:65, :]
    wide = jnp.transpose(jnp.broadcast_to(line, (128, 128)))
    means[...] = sums[:64] / jnp.maximum(jnp.where(c == 0, wide[:64], wide[64:]), 1.0)
    counts[...] = jnp.where(c == 0, line, pltpu.roll(line, 64, 1))[:, :64]


def means_of(sums):
    return pl.pallas_call(
        means_kernel,
        out_shape=(jax.ShapeDtypeStruct((64, D), f32), jax.ShapeDtypeStruct((1, 64), f32)),
        in_specs=[spec(VM)],
        out_specs=(spec(VM), spec(VM)),
        compiler_params=pltpu.CompilerParams(vmem_limit_bytes=1 << 20),
    )(sums)


def shards(rows_data, row_keys, valid_counts, predicates, section_weight, section_bias):
    w, b, same, words, limits, clear_a, clear_b, key_rows = exchange(
        section_weight, section_bias.reshape(1, 1, D), predicates.reshape(4, MICRO, 32), row_keys, valid_counts.T)
    table_a, table_b, lives = sections(
        rows_data, key_rows, w, b, same, words, limits, clear_a, clear_b, valid_counts.T)
    means, counts = means_of(reduce_to_owner(table_a, table_b, key_rows, lives))
    return means, counts.reshape(64)


def solution(mesh):
    placed = (
        P("section", "rows", None),
        P("section", "rows"),
        P("section", "rows"),
        P("section", None, "rows"),
        P("section", None, None),
        P("section", None),
    )
    return jax.shard_map(
        shards,
        mesh=mesh,
        in_specs=placed,
        out_specs=(P(("section", "rows"), None), P(("section", "rows"))),
        check_vma=False,
    )
```

```python
import functools

import jax
import jax.numpy as jnp
from jax import lax
from jax.experimental import pallas as pl
from jax.experimental.pallas import tpu as pltpu
from jax.sharding import PartitionSpec as P

KEYS = 8192
SECTIONS = 4
D = 128
MICRO = 4
BLOCK = 1024
ROWS = MICRO * BLOCK
GROUP = 8
TILE = 128
BATCH = 8
SURE = 256
f32, bf16, i32 = jnp.float32, jnp.bfloat16, jnp.int32
MESH = pl.DeviceIdType.MESH
VM, SM, HB = pltpu.VMEM, pltpu.SMEM, pltpu.HBM


def spec(space):
    return pl.BlockSpec(memory_space=space)


def pinned(x):
    return pltpu.with_memory_space_constraint(x, HB)


def high_low(x):
    high = x.astype(bf16)
    return high, (x - high.astype(f32)).astype(bf16)


def exchange_kernel(
    w_in, b_in, p_in, k_in, v_in,
    w_twice, b_all, same, words, valid, table_a, table_b, key_rows,
    w_all, keys, flags, send, recv, local,
):
    me = lax.axis_index("section")
    row = lax.axis_index("rows")
    own = [
        pltpu.make_async_copy(src, dst, local.at[n])
        for n, (src, dst) in enumerate((
            (p_in, flags), (p_in.at[me], words.at[me]), (b_in.at[0], b_all.at[me]), (w_in.at[0], w_all.at[me]),
            (k_in, keys), (v_in, valid)))
    ]
    for copy in own:
        copy.start()
    barrier = pltpu.get_barrier_semaphore()
    for k in range(1, 4):
        pl.semaphore_signal(barrier, inc=1, device_id=(lax.rem(me + k, 4), row), device_id_type=MESH)

    def clear(i, carry):
        at = pl.ds(pl.multiple_of(i * 512, 512), 512)
        table_a[at, :] = jnp.zeros((512, D), f32)
        table_b[at, :] = jnp.zeros((512, D), f32)
        return carry

    lax.fori_loop(0, KEYS // 512, clear, 0)
    for copy in own[:4]:
        copy.wait()
    pl.semaphore_wait(barrier, 3)
    copies = []
    for n, k in enumerate((2, 1, 3)):
        to = lax.rem(me + k, 4)
        for a, (src, dst) in enumerate((
            (flags.at[to], words.at[me]), (w_all.at[me], w_all.at[me]), (b_all.at[me], b_all.at[me]),
        )):
            copies.append((a, pltpu.make_async_remote_copy(
                src_ref=src, dst_ref=dst, send_sem=send.at[n, a], recv_sem=recv.at[n, a],
                device_id=(to, row), device_id_type=MESH)))
    for a in range(3):
        for which, copy in copies:
            if which == a:
                copy.start()

    def prepare(origin):
        top = jnp.concatenate(high_low(w_all[origin]), axis=1)
        w_twice[origin] = jnp.concatenate([top, top], axis=0)

    prepare(me)
    own[4].wait()
    own[5].wait()
    group_i = (lax.broadcasted_iota(i32, (1, 128), 1) // GROUP) * KEYS

    for m in range(MICRO):
        for j in range(8):
            key_rows[m * 8 + j : m * 8 + j + 1, :] = keys[m : m + 1, j * 128 : (j + 1) * 128]

    def key_row_at(m, j):
        return key_rows[pl.ds(m * 8 + j, 1), :]

    def sameness(i, carry):
        for u in range(4):
            key_row = key_row_at(i // 2, (i % 2) * 4 + u) + group_i
            key_col = jnp.transpose(jnp.broadcast_to(key_row, (128, 128)))
            same[i * 4 + u] = jnp.where(key_col == key_row, 1.0, 0.0).astype(bf16)
        return carry

    lax.fori_loop(0, 8, sameness, 0)
    for which, copy in copies:
        if which == 0:
            copy.wait()
    for which, copy in copies:
        if which == 2:
            copy.wait()
    for n, k in ((1, 1), (2, 3), (0, 2)):
        copies[3 * n + 1][1].wait()
        prepare(lax.rem(me + 4 - k, 4))


def exchange(weight, bias, predicates, keys, valid):
    return pl.pallas_call(
        exchange_kernel,
        out_shape=(
            jax.ShapeDtypeStruct((4, 256, 256), bf16),
            jax.ShapeDtypeStruct((4, 1, D), f32),
            jax.ShapeDtypeStruct((32, 128, 128), bf16),
            jax.ShapeDtypeStruct((SECTIONS, MICRO, 32), i32),
            jax.ShapeDtypeStruct((1, MICRO), i32),
            jax.ShapeDtypeStruct((KEYS, D), f32),
            jax.ShapeDtypeStruct((KEYS, D), f32),
            jax.ShapeDtypeStruct((32, 128), i32),
        ),
        in_specs=[spec(HB)] * 5,
        out_specs=(spec(VM),) * 8,
        scratch_shapes=[
            pltpu.VMEM((4, D, D), f32),
            pltpu.VMEM((MICRO, BLOCK), i32),
            pltpu.VMEM((4, 4, 32), i32),
            pltpu.SemaphoreType.DMA((3, 3)),
            pltpu.SemaphoreType.DMA((3, 3)),
            pltpu.SemaphoreType.DMA((6,)),
        ],
        compiler_params=pltpu.CompilerParams(collective_id=0, has_side_effects=True, vmem_limit_bytes=8 << 20),
        cost_estimate=pl.CostEstimate(flops=40_000_000_000, bytes_accessed=1 << 20, transcendentals=0),
    )(pinned(weight), pinned(bias), pinned(predicates), pinned(keys), pinned(valid))


def sections_kernel(
    rows, keys_in, w2, b, same, words, limits, clear_a, clear_b, v_in, table_a, table_b, lives, ready, keys, valid, sems
):
    fetch = [pltpu.make_async_copy(keys_in, keys, sems.at[0]), pltpu.make_async_copy(v_in, valid, sems.at[1])]
    for copy in fetch:
        copy.start()

    sub = lax.broadcasted_iota(i32, (8, 128), 0)
    lane = lax.broadcasted_iota(i32, (8, 128), 1)
    for m in range(MICRO):
        alive = jnp.where(sub * 128 + lane < limits[0:1, m : m + 1], 1, 0)
        found = jnp.zeros((8, 128), i32)
        for s in range(SECTIONS):
            line = jnp.concatenate([words[s, m : m + 1, :]] * 4, axis=1)
            word = jnp.take_along_axis(
                jnp.broadcast_to(line, (8, 128)), sub * 4 + (lane >> 5), axis=1, mode="promise_in_bounds")
            alive = alive & (word >> (lane & 31))
            found = found + alive
        lives[m * 8 : (m + 1) * 8, :] = found

    def compute(slot, tiles, used=BATCH):
        h = jnp.concatenate([rows[t // 8, pl.ds(pl.multiple_of((t % 8) * TILE, TILE), TILE), :] for t in tiles[:used]], axis=0)
        levels = jnp.concatenate([lives[pl.ds(t, 1), :] for t in tiles], axis=0)
        columns = jnp.transpose(jnp.concatenate([levels] * 16, axis=0))
        alive = jnp.concatenate([jnp.broadcast_to(columns[:, j : j + 1], (128, 128)) for j in range(used)], axis=0)
        total = jnp.zeros((used * TILE, D), f32)
        for s in range(SECTIONS):
            p = jnp.dot(jnp.concatenate(high_low(h), axis=1), w2[s], preferred_element_type=f32)
            h = h + jnp.tanh(p[:, :D] + (p[:, D:] + b[s]))
            total = total + jnp.where(alive > s, h, 0.0)
        both = jnp.concatenate(high_low(total), axis=1)
        for j, t in enumerate(tiles[:used]):
            p = jnp.dot(same[t], both[j * TILE : (j + 1) * TILE], preferred_element_type=f32)
            ready[pl.ds(pl.multiple_of((slot + j) * TILE, TILE), TILE), :] = p[:, :D] + p[:, D:]

    compute(0, [m * 8 + j for m in range(MICRO) for j in range(SURE // TILE)])
    for copy in fetch:
        copy.wait()
    ends = [0]
    for m in range(MICRO):
        ends.append(ends[-1] + (valid[0, m] - SURE + TILE - 1) // TILE)

    def tile_at(i):
        tile = SURE // TILE + i
        for m in range(1, MICRO):
            tile = jnp.where(i >= ends[m], m * 8 + SURE // TILE + i - ends[m], tile)
        return jnp.minimum(tile, 31)

    def batch(n, carry):
        compute(BATCH + n * BATCH, [tile_at(n * BATCH + j) for j in range(BATCH)])
        return carry

    whole = (ends[MICRO] + BATCH // 2 - 1) // BATCH
    lax.fori_loop(0, whole, batch, 0)

    @pl.when(ends[MICRO] > whole * BATCH)
    def _():
        compute(BATCH + whole * BATCH, [tile_at(whole * BATCH + j) for j in range(BATCH)], BATCH // 2)

    tables = (table_a, table_b)
    groups = TILE // GROUP

    def scatter(slot, tile):
        def load(g):
            at = [keys[tile, g * GROUP + i] for i in range(GROUP)]
            return at, [tables[g % 2][pl.ds(k, 1), :] for k in at]

        def store(g, at, held):
            for i, k in enumerate(at):
                tables[g % 2][pl.ds(k, 1), :] = held[i] + ready[pl.ds(slot * TILE + g * GROUP + i, 1), :]

        flying = {g: load(g) for g in range(2)}
        for g in range(groups):
            store(g, *flying.pop(g))
            if g + 2 < groups:
                flying[g + 2] = load(g + 2)

    def sure(i, carry):
        scatter(i, (i // 2) * 8 + i % 2)
        return carry

    def rest(i, carry):
        scatter(BATCH + i, tile_at(i))
        return carry

    lax.fori_loop(0, BATCH, sure, 0)
    lax.fori_loop(0, ends[MICRO], rest, 0)


def sections(rows, keys, w, b, same, words, limits, clear_a, clear_b, valid):
    return pl.pallas_call(
        sections_kernel,
        out_shape=(jax.ShapeDtypeStruct((KEYS, D), f32),) * 2 + (jax.ShapeDtypeStruct((32, 128), i32),),
        in_specs=[spec(VM)] * 9 + [spec(HB)],
        out_specs=(spec(VM),) * 3,
        scratch_shapes=[
            pltpu.VMEM((ROWS, D), f32),
            pltpu.SMEM((32, 128), i32),
            pltpu.SMEM((1, MICRO), i32),
            pltpu.SemaphoreType.DMA((2,)),
        ],
        input_output_aliases={7: 0, 8: 1},
        compiler_params=pltpu.CompilerParams(vmem_limit_bytes=12 << 20),
    )(rows, keys, w, b, same, words, limits, clear_a, clear_b, pinned(valid))


ORDERS = ((0, 1, 2), (1, 2, 0), (2, 0, 1))
BAND, PART, COUNTED = 24, 8, 8
N = 9
HEIGHT = 72


def reduce_kernel(table_a, table_b, keys, lives, sums, pair, *scratch):
    held = scratch[0:3]
    near, middle, second, last, third = (scratch[3 + i * N : 3 + (i + 1) * N] for i in range(5))
    core_recv, core_send, near_sems, far_sems = scratch[3 + 5 * N :]
    z = lax.axis_index("section")
    row = lax.axis_index("rows")
    y, x, c = row // 8, (row // 2) % 4, row % 2
    place = (z, y, x)

    def position(axis, k):
        return lax.rem(place[axis] + k, 4)

    def device(axis, k):
        at = list(place)
        at[axis] = position(axis, k)
        return (at[0], at[1] * 8 + at[2] * 2 + c)

    other = (z, y * 8 + x * 2 + (1 - c))
    peers = [device(axis, k) for axis in range(3) for k in (1, 3)] + [other]
    barrier = pltpu.get_barrier_semaphore()
    for peer in peers:
        pl.semaphore_signal(barrier, inc=1, device_id=peer, device_id_type=MESH)

    def join(i, carry):
        at = (i // 16, (i // 4) % 4, i % 4)
        pair[(*at, slice(0, 64))] = table_a[(*at, 1 - c)] + table_b[(*at, 1 - c)]
        return carry

    lax.fori_loop(0, 64, join, 0)
    pl.semaphore_wait(barrier, len(peers))

    def send(src, dst, send_sem, recv_sem, to):
        pltpu.make_async_remote_copy(
            src_ref=src, dst_ref=dst, send_sem=send_sem, recv_sem=recv_sem, device_id=to, device_id_type=MESH
        ).start()

    def wait(ref, sem):
        pltpu.make_async_copy(ref, ref, sem).wait()

    every = [0, 1, 2]

    def where_of(axes, axis, index, half=None):
        where = [slice(None)] * len(axes)
        where[axes.index(axis)] = index
        if half is not None:
            where[1 if axes[0] == axis else 0] = pl.ds(2 * half, 2)
        return tuple(where)

    def keyed(band):
        return BAND - COUNTED if band == 2 else BAND

    def swap(band, index, kind):
        at, size = where_of(every, ORDERS[band][0], index), keyed(band)
        send(
            pair.at[(*at, pl.ds(band * BAND, size))], held[band].at[(*at, pl.ds(0, size))],
            core_send.at[band], core_recv.at[band, kind], other)

    def swapped(band, kind, blocks):
        size = keyed(band)
        wait(held[band].at[0:blocks, :, :, pl.ds(0, size)], core_recv.at[band, kind])
        for k in {0: (2,), 1: (1, 3), 2: (0,)}[kind]:
            at = where_of(every, ORDERS[band][0], position(ORDERS[band][0], k))
            rows = (c, slice(band * BAND, band * BAND + size))
            held[band][(*at, slice(0, size))] += table_a[(*at, *rows)] + table_b[(*at, *rows)]

    for kind, steps in enumerate(((2,), (1, 3), (0,))):
        for band in range(3):
            for k in steps:
                swap(band, position(ORDERS[band][0], k), kind)
    sub64 = lax.broadcasted_iota(i32, (64, 128), 0)
    sub128 = lax.broadcasted_iota(i32, (128, 128), 0)

    def tally(i, found):
        for u in range(4):
            key_row = keys[pl.ds(i * 4 + u, 1), :]
            alive = lives[pl.ds(i * 4 + u, 1), :].astype(f32)
            high = jnp.where((key_row >> 7) == sub64, alive, 0.0).astype(bf16)
            low = jnp.where((key_row & 127) == sub128, 1.0, 0.0).astype(bf16)
            found = found + lax.dot_general(high, low, (((1,), (1,)), ((), ())), preferred_element_type=f32)
        return found

    found = lax.fori_loop(0, 8, tally, jnp.zeros((64, 128), f32))
    for i in range(64):
        pair[i // 16, (i // 4) % 4, i % 4, 64:72, :] = jnp.broadcast_to(found[i : i + 1], (8, 128))
    counted = held[2].at[:, :, :, pl.ds(BAND - COUNTED, COUNTED)]
    send(pair.at[:, :, :, pl.ds(64, COUNTED)], counted, core_send.at[2], core_recv.at[3, 0], other)

    def block_of(n, k, half):
        band, step = n % 3, n // 3
        axis = ORDERS[band][0]
        return held[band].at[(*where_of(every, axis, position(axis, k), half), pl.ds(step * PART, PART))]

    def hop(n, slot, recv, block, k):
        send(block, near[n].at[slot], near_sems.at[n, 3], near_sems.at[n, recv], device(ORDERS[n % 3][0], k))

    def relay(n):
        hop(n, 0, 0, block_of(n, 2, 0), 1)
        hop(n, 1, 1, block_of(n, 2, 1), 3)

    def direct(n):
        hop(n, 2, 2, block_of(n, 1, 1), 1)
        hop(n, 3, 2, block_of(n, 3, 0), 3)

    for band in range(3):
        swapped(band, 0, 1)
        for n in range(band, N - 1 if band == 2 else N, 3):
            relay(n)
    for band in range(3):
        swapped(band, 1, 2)
        for n in range(band, N - 1 if band == 2 else N, 3):
            direct(n)
    wait(counted, core_recv.at[3, 0])
    for i in range(4):
        held[2][i, :, :, BAND - COUNTED :] += pair[i, :, :, 64:72]
    relay(N - 1)
    direct(N - 1)

    def spread(n, stage, source, axes, target):
        axis = ORDERS[n % 3][stage]
        for k in (2, 1, 3):
            send(
                source.at[where_of(axes, axis, position(axis, k))], target.at[k - 1],
                far_sems.at[n, stage - 1, 0], far_sems.at[n, stage - 1, 1], device(axis, k))

    def summed(n, stage, source, axes, target):
        axis = ORDERS[n % 3][stage]
        wait(target, far_sems.at[n, stage - 1, 1])
        return (source[where_of(axes, axis, place[axis])] + target[0]) + (target[1] + target[2])

    for n in range(N):
        if n == 6:
            for band in range(3):
                swapped(band, 2, 1)
        for half, k in ((0, 1), (1, 3)):
            wait(near[n].at[half], near_sems.at[n, half])
            block = block_of(n, k, half)
            block[...] += near[n][half]
            hop(n, 4 + half, 2, block, k)
    for n in range(N):
        axis = ORDERS[n % 3][0]
        wait(near[n].at[2:6], near_sems.at[n, 2])
        middle[n][0:2] = (block_of(n, 0, 0)[...] + near[n][3]) + near[n][4]
        middle[n][2:4] = (block_of(n, 0, 1)[...] + near[n][2]) + near[n][5]
        spread(n, 1, middle[n], [i for i in every if i != axis], second[n])
    for n in range(N):
        axis = ORDERS[n % 3][0]
        last[n][...] = summed(n, 1, middle[n], [i for i in every if i != axis], second[n])
        spread(n, 2, last[n], [ORDERS[n % 3][2]], third[n])
    for n in range(N):
        start = (n % 3) * BAND + (n // 3) * PART
        sums[start : start + PART, :] = summed(n, 2, last[n], [ORDERS[n % 3][2]], third[n])
    for band in range(3):
        wait(held[band], core_send.at[band])
    for n in range(N):
        wait(near[n], near_sems.at[n, 3])
        wait(second[n], far_sems.at[n, 0, 0])
        wait(third[n], far_sems.at[n, 1, 0])


def reduce_to_owner(table_a, table_b, keys, lives):
    buffers = [pltpu.VMEM((4, 4, 4, HEIGHT, D), f32)] + [pltpu.VMEM((4, 4, 4, BAND, D), f32)] * 3
    for lead in ((6, 2, 4), (4, 4), (3, 4), (4,), (3,)):
        buffers += [pltpu.VMEM((*lead, PART, D), f32)] * N
    return pl.pallas_call(
        reduce_kernel,
        out_shape=jax.ShapeDtypeStruct((HEIGHT, D), f32),
        in_specs=[spec(VM)] * 4,
        out_specs=spec(VM),
        scratch_shapes=buffers + [
            pltpu.SemaphoreType.DMA((4, 3)),
            pltpu.SemaphoreType.DMA((3,)),
            pltpu.SemaphoreType.DMA((N, 4)),
            pltpu.SemaphoreType.DMA((N, 2, 2)),
        ],
        compiler_params=pltpu.CompilerParams(collective_id=1, has_side_effects=True, vmem_limit_bytes=20 << 20),
    )(table_a.reshape(4, 4, 4, 2, 64, D), table_b.reshape(4, 4, 4, 2, 64, D), keys, lives)


def means_kernel(sums, means, counts):
    c = lax.axis_index("rows") % 2
    line = sums[64:65, :]
    wide = jnp.transpose(jnp.broadcast_to(line, (128, 128)))
    means[...] = sums[:64] / jnp.maximum(jnp.where(c == 0, wide[:64], wide[64:]), 1.0)
    counts[...] = jnp.where(c == 0, line, pltpu.roll(line, 64, 1))[:, :64]


def means_of(sums):
    return pl.pallas_call(
        means_kernel,
        out_shape=(jax.ShapeDtypeStruct((64, D), f32), jax.ShapeDtypeStruct((1, 64), f32)),
        in_specs=[spec(VM)],
        out_specs=(spec(VM), spec(VM)),
        compiler_params=pltpu.CompilerParams(vmem_limit_bytes=1 << 20),
    )(sums)


def shards(rows_data, row_keys, valid_counts, predicates, section_weight, section_bias):
    w, b, same, words, limits, clear_a, clear_b, key_rows = exchange(
        section_weight, section_bias.reshape(1, 1, D), predicates.reshape(4, MICRO, 32), row_keys, valid_counts.T)
    table_a, table_b, lives = sections(
        rows_data, key_rows, w, b, same, words, limits, clear_a, clear_b, valid_counts.T)
    means, counts = means_of(reduce_to_owner(table_a, table_b, key_rows, lives))
    return means, counts.reshape(64)


def solution(mesh):
    placed = (
        P("section", "rows", None),
        P("section", "rows"),
        P("section", "rows"),
        P("section", None, "rows"),
        P("section", None, None),
        P("section", None),
    )
    return jax.shard_map(
        shards,
        mesh=mesh,
        in_specs=placed,
        out_specs=(P(("section", "rows"), None), P(("section", "rows"))),
        check_vma=False,
    )
```

```python
import functools

import jax
import jax.numpy as jnp
from jax import lax
from jax.experimental import pallas as pl
from jax.experimental.pallas import tpu as pltpu
from jax.sharding import PartitionSpec as P

KEYS = 8192
SECTIONS = 4
D = 128
MICRO = 4
BLOCK = 1024
ROWS = MICRO * BLOCK
GROUP = 8
TILE = 128
BATCH = 8
SURE = 256
f32, bf16, i32 = jnp.float32, jnp.bfloat16, jnp.int32
MESH = pl.DeviceIdType.MESH
VM, SM, HB = pltpu.VMEM, pltpu.SMEM, pltpu.HBM


def spec(space):
    return pl.BlockSpec(memory_space=space)


def pinned(x):
    return pltpu.with_memory_space_constraint(x, HB)


def high_low(x):
    high = x.astype(bf16)
    return high, (x - high.astype(f32)).astype(bf16)


def exchange_kernel(
    w_in, b_in, p_in, k_in, v_in,
    w_twice, b_all, same, words, valid, table_a, table_b, key_rows,
    w_all, keys, flags, send, recv, local,
):
    me = lax.axis_index("section")
    row = lax.axis_index("rows")
    own = [
        pltpu.make_async_copy(src, dst, local.at[n])
        for n, (src, dst) in enumerate((
            (p_in, flags), (p_in.at[me], words.at[me]), (b_in.at[0], b_all.at[me]), (w_in.at[0], w_all.at[me]),
            (k_in, keys), (v_in, valid)))
    ]
    for copy in own:
        copy.start()
    barrier = pltpu.get_barrier_semaphore()
    for k in range(1, 4):
        pl.semaphore_signal(barrier, inc=1, device_id=(lax.rem(me + k, 4), row), device_id_type=MESH)

    def clear(i, carry):
        at = pl.ds(pl.multiple_of(i * 512, 512), 512)
        table_a[at, :] = jnp.zeros((512, D), f32)
        table_b[at, :] = jnp.zeros((512, D), f32)
        return carry

    lax.fori_loop(0, KEYS // 512, clear, 0)
    for copy in own[:4]:
        copy.wait()
    pl.semaphore_wait(barrier, 3)
    copies = []
    for n, k in enumerate((2, 1, 3)):
        to = lax.rem(me + k, 4)
        for a, (src, dst) in enumerate((
            (flags.at[to], words.at[me]), (w_all.at[me], w_all.at[me]), (b_all.at[me], b_all.at[me]),
        )):
            copies.append((a, pltpu.make_async_remote_copy(
                src_ref=src, dst_ref=dst, send_sem=send.at[n, a], recv_sem=recv.at[n, a],
                device_id=(to, row), device_id_type=MESH)))
    for a in range(3):
        for which, copy in copies:
            if which == a:
                copy.start()

    def prepare(origin):
        top = jnp.concatenate(high_low(w_all[origin]), axis=1)
        w_twice[origin] = jnp.concatenate([top, top], axis=0)

    prepare(me)
    own[4].wait()
    own[5].wait()
    group_i = (lax.broadcasted_iota(i32, (1, 128), 1) // GROUP) * KEYS

    for m in range(MICRO):
        for j in range(8):
            key_rows[m * 8 + j : m * 8 + j + 1, :] = keys[m : m + 1, j * 128 : (j + 1) * 128]

    def key_row_at(m, j):
        return key_rows[pl.ds(m * 8 + j, 1), :]

    def sameness(i, carry):
        for u in range(4):
            key_row = key_row_at(i // 2, (i % 2) * 4 + u) + group_i
            key_col = jnp.transpose(jnp.broadcast_to(key_row, (128, 128)))
            same[i * 4 + u] = jnp.where(key_col == key_row, 1.0, 0.0).astype(bf16)
        return carry

    lax.fori_loop(0, 8, sameness, 0)
    for which, copy in copies:
        if which == 0:
            copy.wait()
    for which, copy in copies:
        if which == 2:
            copy.wait()
    for n, k in ((1, 1), (2, 3), (0, 2)):
        copies[3 * n + 1][1].wait()
        prepare(lax.rem(me + 4 - k, 4))


def exchange(weight, bias, predicates, keys, valid):
    return pl.pallas_call(
        exchange_kernel,
        out_shape=(
            jax.ShapeDtypeStruct((4, 256, 256), bf16),
            jax.ShapeDtypeStruct((4, 1, D), f32),
            jax.ShapeDtypeStruct((32, 128, 128), bf16),
            jax.ShapeDtypeStruct((SECTIONS, MICRO, 32), i32),
            jax.ShapeDtypeStruct((1, MICRO), i32),
            jax.ShapeDtypeStruct((KEYS, D), f32),
            jax.ShapeDtypeStruct((KEYS, D), f32),
            jax.ShapeDtypeStruct((32, 128), i32),
        ),
        in_specs=[spec(HB)] * 5,
        out_specs=(spec(VM),) * 8,
        scratch_shapes=[
            pltpu.VMEM((4, D, D), f32),
            pltpu.VMEM((MICRO, BLOCK), i32),
            pltpu.VMEM((4, 4, 32), i32),
            pltpu.SemaphoreType.DMA((3, 3)),
            pltpu.SemaphoreType.DMA((3, 3)),
            pltpu.SemaphoreType.DMA((6,)),
        ],
        compiler_params=pltpu.CompilerParams(collective_id=0, has_side_effects=True, vmem_limit_bytes=8 << 20),
        cost_estimate=pl.CostEstimate(flops=40_000_000_000, bytes_accessed=1 << 20, transcendentals=0),
    )(pinned(weight), pinned(bias), pinned(predicates), pinned(keys), pinned(valid))


def sections_kernel(
    rows, keys_in, w2, b, same, words, limits, clear_a, clear_b, v_in, table_a, table_b, lives, ready, keys, valid, sems
):
    fetch = [pltpu.make_async_copy(keys_in, keys, sems.at[0]), pltpu.make_async_copy(v_in, valid, sems.at[1])]
    for copy in fetch:
        copy.start()

    sub = lax.broadcasted_iota(i32, (8, 128), 0)
    lane = lax.broadcasted_iota(i32, (8, 128), 1)
    for m in range(MICRO):
        alive = jnp.where(sub * 128 + lane < limits[0:1, m : m + 1], 1, 0)
        found = jnp.zeros((8, 128), i32)
        for s in range(SECTIONS):
            line = jnp.concatenate([words[s, m : m + 1, :]] * 4, axis=1)
            word = jnp.take_along_axis(
                jnp.broadcast_to(line, (8, 128)), sub * 4 + (lane >> 5), axis=1, mode="promise_in_bounds")
            alive = alive & (word >> (lane & 31))
            found = found + alive
        lives[m * 8 : (m + 1) * 8, :] = found

    def compute(slot, tiles, used=BATCH):
        h = jnp.concatenate([rows[t // 8, pl.ds(pl.multiple_of((t % 8) * TILE, TILE), TILE), :] for t in tiles[:used]], axis=0)
        levels = jnp.concatenate([lives[pl.ds(t, 1), :] for t in tiles], axis=0)
        columns = jnp.transpose(jnp.concatenate([levels] * 16, axis=0))
        alive = jnp.concatenate([jnp.broadcast_to(columns[:, j : j + 1], (128, 128)) for j in range(used)], axis=0)
        total = jnp.zeros((used * TILE, D), f32)
        for s in range(SECTIONS):
            p = jnp.dot(jnp.concatenate(high_low(h), axis=1), w2[s], preferred_element_type=f32)
            h = h + jnp.tanh(p[:, :D] + (p[:, D:] + b[s]))
            total = total + jnp.where(alive > s, h, 0.0)
        both = jnp.concatenate(high_low(total), axis=1)
        for j, t in enumerate(tiles[:used]):
            p = jnp.dot(same[t], both[j * TILE : (j + 1) * TILE], preferred_element_type=f32)
            ready[pl.ds(pl.multiple_of((slot + j) * TILE, TILE), TILE), :] = p[:, :D] + p[:, D:]

    compute(0, [m * 8 + j for m in range(MICRO) for j in range(SURE // TILE)])
    for copy in fetch:
        copy.wait()
    ends = [0]
    for m in range(MICRO):
        ends.append(ends[-1] + (valid[0, m] - SURE + TILE - 1) // TILE)

    def tile_at(i):
        tile = SURE // TILE + i
        for m in range(1, MICRO):
            tile = jnp.where(i >= ends[m], m * 8 + SURE // TILE + i - ends[m], tile)
        return jnp.minimum(tile, 31)

    def batch(n, carry):
        compute(BATCH + n * BATCH, [tile_at(n * BATCH + j) for j in range(BATCH)])
        return carry

    whole = (ends[MICRO] + BATCH // 2 - 1) // BATCH
    lax.fori_loop(0, whole, batch, 0)

    @pl.when(ends[MICRO] > whole * BATCH)
    def _():
        compute(BATCH + whole * BATCH, [tile_at(whole * BATCH + j) for j in range(BATCH)], BATCH // 2)

    tables = (table_a, table_b)

    def scatter(slot, *tiles):
        groups = len(tiles) * TILE // GROUP

        def load(g):
            at = [keys[tiles[g * GROUP // TILE], (g * GROUP + i) % TILE] for i in range(GROUP)]
            return at, [tables[g % 2][pl.ds(k, 1), :] for k in at]

        def store(g, at, held):
            for i, k in enumerate(at):
                tables[g % 2][pl.ds(k, 1), :] = held[i] + ready[pl.ds(slot * TILE + g * GROUP + i, 1), :]

        flying = {g: load(g) for g in range(2)}
        for g in range(groups):
            store(g, *flying.pop(g))
            if g + 2 < groups:
                flying[g + 2] = load(g + 2)

    def sure(m, carry):
        scatter(2 * m, 8 * m, 8 * m + 1)
        return carry

    def rest(i, carry):
        scatter(BATCH + 2 * i, tile_at(2 * i), tile_at(2 * i + 1))
        return carry

    lax.fori_loop(0, MICRO, sure, 0)
    lax.fori_loop(0, ends[MICRO] // 2, rest, 0)

    @pl.when(ends[MICRO] % 2 == 1)
    def _():
        scatter(BATCH + ends[MICRO] - 1, tile_at(ends[MICRO] - 1))


def sections(rows, keys, w, b, same, words, limits, clear_a, clear_b, valid):
    return pl.pallas_call(
        sections_kernel,
        out_shape=(jax.ShapeDtypeStruct((KEYS, D), f32),) * 2 + (jax.ShapeDtypeStruct((32, 128), i32),),
        in_specs=[spec(VM)] * 9 + [spec(HB)],
        out_specs=(spec(VM),) * 3,
        scratch_shapes=[
            pltpu.VMEM((ROWS, D), f32),
            pltpu.SMEM((32, 128), i32),
            pltpu.SMEM((1, MICRO), i32),
            pltpu.SemaphoreType.DMA((2,)),
        ],
        input_output_aliases={7: 0, 8: 1},
        compiler_params=pltpu.CompilerParams(vmem_limit_bytes=12 << 20),
    )(rows, keys, w, b, same, words, limits, clear_a, clear_b, pinned(valid))


ORDERS = ((0, 1, 2), (1, 2, 0), (2, 0, 1))
BAND, PART, COUNTED = 24, 8, 8
N = 9
HEIGHT = 72


def reduce_kernel(table_a, table_b, keys, lives, sums, pair, *scratch):
    held = scratch[0:3]
    near, middle, second, last, third = (scratch[3 + i * N : 3 + (i + 1) * N] for i in range(5))
    core_recv, core_send, near_sems, far_sems = scratch[3 + 5 * N :]
    z = lax.axis_index("section")
    row = lax.axis_index("rows")
    y, x, c = row // 8, (row // 2) % 4, row % 2
    place = (z, y, x)

    def position(axis, k):
        return lax.rem(place[axis] + k, 4)

    def device(axis, k):
        at = list(place)
        at[axis] = position(axis, k)
        return (at[0], at[1] * 8 + at[2] * 2 + c)

    other = (z, y * 8 + x * 2 + (1 - c))
    peers = [device(axis, k) for axis in range(3) for k in (1, 3)] + [other]
    barrier = pltpu.get_barrier_semaphore()
    for peer in peers:
        pl.semaphore_signal(barrier, inc=1, device_id=peer, device_id_type=MESH)

    def join(i, carry):
        at = (i // 16, (i // 4) % 4, i % 4)
        pair[(*at, slice(0, 64))] = table_a[(*at, 1 - c)] + table_b[(*at, 1 - c)]
        return carry

    lax.fori_loop(0, 64, join, 0)
    pl.semaphore_wait(barrier, len(peers))

    def send(src, dst, send_sem, recv_sem, to):
        pltpu.make_async_remote_copy(
            src_ref=src, dst_ref=dst, send_sem=send_sem, recv_sem=recv_sem, device_id=to, device_id_type=MESH
        ).start()

    def wait(ref, sem):
        pltpu.make_async_copy(ref, ref, sem).wait()

    every = [0, 1, 2]

    def where_of(axes, axis, index, half=None):
        where = [slice(None)] * len(axes)
        where[axes.index(axis)] = index
        if half is not None:
            where[1 if axes[0] == axis else 0] = pl.ds(2 * half, 2)
        return tuple(where)

    def keyed(band):
        return BAND - COUNTED if band == 2 else BAND

    def swap(band, index, kind):
        at, size = where_of(every, ORDERS[band][0], index), keyed(band)
        send(
            pair.at[(*at, pl.ds(band * BAND, size))], held[band].at[(*at, pl.ds(0, size))],
            core_send.at[band], core_recv.at[band, kind], other)

    def swapped(band, kind, blocks):
        size = keyed(band)
        wait(held[band].at[0:blocks, :, :, pl.ds(0, size)], core_recv.at[band, kind])
        for k in {0: (2,), 1: (1, 3), 2: (0,)}[kind]:
            at = where_of(every, ORDERS[band][0], position(ORDERS[band][0], k))
            rows = (c, slice(band * BAND, band * BAND + size))
            held[band][(*at, slice(0, size))] += table_a[(*at, *rows)] + table_b[(*at, *rows)]

    for kind, steps in enumerate(((2,), (1, 3), (0,))):
        for band in range(3):
            for k in steps:
                swap(band, position(ORDERS[band][0], k), kind)
    sub64 = lax.broadcasted_iota(i32, (64, 128), 0)
    sub128 = lax.broadcasted_iota(i32, (128, 128), 0)

    def tally(i, found):
        for u in range(4):
            key_row = keys[pl.ds(i * 4 + u, 1), :]
            alive = lives[pl.ds(i * 4 + u, 1), :].astype(f32)
            high = jnp.where((key_row >> 7) == sub64, alive, 0.0).astype(bf16)
            low = jnp.where((key_row & 127) == sub128, 1.0, 0.0).astype(bf16)
            found = found + lax.dot_general(high, low, (((1,), (1,)), ((), ())), preferred_element_type=f32)
        return found

    found = lax.fori_loop(0, 8, tally, jnp.zeros((64, 128), f32))
    for i in range(64):
        pair[i // 16, (i // 4) % 4, i % 4, 64:72, :] = jnp.broadcast_to(found[i : i + 1], (8, 128))
    counted = held[2].at[:, :, :, pl.ds(BAND - COUNTED, COUNTED)]
    send(pair.at[:, :, :, pl.ds(64, COUNTED)], counted, core_send.at[2], core_recv.at[3, 0], other)

    def block_of(n, k, half):
        band, step = n % 3, n // 3
        axis = ORDERS[band][0]
        return held[band].at[(*where_of(every, axis, position(axis, k), half), pl.ds(step * PART, PART))]

    def hop(n, slot, recv, block, k):
        send(block, near[n].at[slot], near_sems.at[n, 3], near_sems.at[n, recv], device(ORDERS[n % 3][0], k))

    def relay(n):
        hop(n, 0, 0, block_of(n, 2, 0), 1)
        hop(n, 1, 1, block_of(n, 2, 1), 3)

    def direct(n):
        hop(n, 2, 2, block_of(n, 1, 1), 1)
        hop(n, 3, 2, block_of(n, 3, 0), 3)

    for band in range(3):
        swapped(band, 0, 1)
        for n in range(band, N - 1 if band == 2 else N, 3):
            relay(n)
    for band in range(3):
        swapped(band, 1, 2)
        for n in range(band, N - 1 if band == 2 else N, 3):
            direct(n)
    wait(counted, core_recv.at[3, 0])
    for i in range(4):
        held[2][i, :, :, BAND - COUNTED :] += pair[i, :, :, 64:72]
    relay(N - 1)
    direct(N - 1)

    def spread(n, stage, source, axes, target):
        axis = ORDERS[n % 3][stage]
        for k in (2, 1, 3):
            send(
                source.at[where_of(axes, axis, position(axis, k))], target.at[k - 1],
                far_sems.at[n, stage - 1, 0], far_sems.at[n, stage - 1, 1], device(axis, k))

    def summed(n, stage, source, axes, target):
        axis = ORDERS[n % 3][stage]
        wait(target, far_sems.at[n, stage - 1, 1])
        return (source[where_of(axes, axis, place[axis])] + target[0]) + (target[1] + target[2])

    for n in range(N):
        if n == 6:
            for band in range(3):
                swapped(band, 2, 1)
        for half, k in ((0, 1), (1, 3)):
            wait(near[n].at[half], near_sems.at[n, half])
            block = block_of(n, k, half)
            block[...] += near[n][half]
            hop(n, 4 + half, 2, block, k)
    for n in range(N):
        axis = ORDERS[n % 3][0]
        wait(near[n].at[2:6], near_sems.at[n, 2])
        middle[n][0:2] = (block_of(n, 0, 0)[...] + near[n][3]) + near[n][4]
        middle[n][2:4] = (block_of(n, 0, 1)[...] + near[n][2]) + near[n][5]
        spread(n, 1, middle[n], [i for i in every if i != axis], second[n])
    for n in range(N):
        axis = ORDERS[n % 3][0]
        last[n][...] = summed(n, 1, middle[n], [i for i in every if i != axis], second[n])
        spread(n, 2, last[n], [ORDERS[n % 3][2]], third[n])
    for n in range(N):
        start = (n % 3) * BAND + (n // 3) * PART
        sums[start : start + PART, :] = summed(n, 2, last[n], [ORDERS[n % 3][2]], third[n])
    for band in range(3):
        wait(held[band], core_send.at[band])
    for n in range(N):
        wait(near[n], near_sems.at[n, 3])
        wait(second[n], far_sems.at[n, 0, 0])
        wait(third[n], far_sems.at[n, 1, 0])


def reduce_to_owner(table_a, table_b, keys, lives):
    buffers = [pltpu.VMEM((4, 4, 4, HEIGHT, D), f32)] + [pltpu.VMEM((4, 4, 4, BAND, D), f32)] * 3
    for lead in ((6, 2, 4), (4, 4), (3, 4), (4,), (3,)):
        buffers += [pltpu.VMEM((*lead, PART, D), f32)] * N
    return pl.pallas_call(
        reduce_kernel,
        out_shape=jax.ShapeDtypeStruct((HEIGHT, D), f32),
        in_specs=[spec(VM)] * 4,
        out_specs=spec(VM),
        scratch_shapes=buffers + [
            pltpu.SemaphoreType.DMA((4, 3)),
            pltpu.SemaphoreType.DMA((3,)),
            pltpu.SemaphoreType.DMA((N, 4)),
            pltpu.SemaphoreType.DMA((N, 2, 2)),
        ],
        compiler_params=pltpu.CompilerParams(collective_id=1, has_side_effects=True, vmem_limit_bytes=20 << 20),
    )(table_a.reshape(4, 4, 4, 2, 64, D), table_b.reshape(4, 4, 4, 2, 64, D), keys, lives)


def means_kernel(sums, means, counts):
    c = lax.axis_index("rows") % 2
    line = sums[64:65, :]
    wide = jnp.transpose(jnp.broadcast_to(line, (128, 128)))
    means[...] = sums[:64] / jnp.maximum(jnp.where(c == 0, wide[:64], wide[64:]), 1.0)
    counts[...] = jnp.where(c == 0, line, pltpu.roll(line, 64, 1))[:, :64]


def means_of(sums):
    return pl.pallas_call(
        means_kernel,
        out_shape=(jax.ShapeDtypeStruct((64, D), f32), jax.ShapeDtypeStruct((1, 64), f32)),
        in_specs=[spec(VM)],
        out_specs=(spec(VM), spec(VM)),
        compiler_params=pltpu.CompilerParams(vmem_limit_bytes=1 << 20),
    )(sums)


def shards(rows_data, row_keys, valid_counts, predicates, section_weight, section_bias):
    w, b, same, words, limits, clear_a, clear_b, key_rows = exchange(
        section_weight, section_bias.reshape(1, 1, D), predicates.reshape(4, MICRO, 32), row_keys, valid_counts.T)
    table_a, table_b, lives = sections(
        rows_data, key_rows, w, b, same, words, limits, clear_a, clear_b, valid_counts.T)
    means, counts = means_of(reduce_to_owner(table_a, table_b, key_rows, lives))
    return means, counts.reshape(64)


def solution(mesh):
    placed = (
        P("section", "rows", None),
        P("section", "rows"),
        P("section", "rows"),
        P("section", None, "rows"),
        P("section", None, None),
        P("section", None),
    )
    return jax.shard_map(
        shards,
        mesh=mesh,
        in_specs=placed,
        out_specs=(P(("section", "rows"), None), P(("section", "rows"))),
        check_vma=False,
    )
```

```python
import functools

import jax
import jax.numpy as jnp
from jax import lax
from jax.experimental import pallas as pl
from jax.experimental.pallas import tpu as pltpu
from jax.sharding import PartitionSpec as P

KEYS = 8192
SECTIONS = 4
D = 128
MICRO = 4
BLOCK = 1024
ROWS = MICRO * BLOCK
GROUP = 8
TILE = 128
BATCH = 8
SURE = 256
f32, bf16, i32 = jnp.float32, jnp.bfloat16, jnp.int32
MESH = pl.DeviceIdType.MESH
VM, SM, HB = pltpu.VMEM, pltpu.SMEM, pltpu.HBM


def spec(space):
    return pl.BlockSpec(memory_space=space)


def pinned(x):
    return pltpu.with_memory_space_constraint(x, HB)


def high_low(x):
    high = x.astype(bf16)
    return high, (x - high.astype(f32)).astype(bf16)


def exchange_kernel(
    w_in, b_in, p_in, k_in, v_in,
    w_twice, b_all, same, words, valid, table_a, table_b, key_rows,
    w_all, keys, flags, send, recv, local,
):
    me = lax.axis_index("section")
    row = lax.axis_index("rows")
    own = [
        pltpu.make_async_copy(src, dst, local.at[n])
        for n, (src, dst) in enumerate((
            (p_in, flags), (p_in.at[me], words.at[me]), (b_in.at[0], b_all.at[me]), (w_in.at[0], w_all.at[me]),
            (k_in, keys), (v_in, valid)))
    ]
    for copy in own:
        copy.start()
    barrier = pltpu.get_barrier_semaphore()
    for k in range(1, 4):
        pl.semaphore_signal(barrier, inc=1, device_id=(lax.rem(me + k, 4), row), device_id_type=MESH)

    def clear(i, carry):
        at = pl.ds(pl.multiple_of(i * 512, 512), 512)
        table_a[at, :] = jnp.zeros((512, D), f32)
        table_b[at, :] = jnp.zeros((512, D), f32)
        return carry

    lax.fori_loop(0, KEYS // 512, clear, 0)
    for copy in own[:4]:
        copy.wait()
    pl.semaphore_wait(barrier, 3)
    copies = []
    for n, k in enumerate((2, 1, 3)):
        to = lax.rem(me + k, 4)
        for a, (src, dst) in enumerate((
            (flags.at[to], words.at[me]), (w_all.at[me], w_all.at[me]), (b_all.at[me], b_all.at[me]),
        )):
            copies.append((a, pltpu.make_async_remote_copy(
                src_ref=src, dst_ref=dst, send_sem=send.at[n, a], recv_sem=recv.at[n, a],
                device_id=(to, row), device_id_type=MESH)))
    for a in range(3):
        for which, copy in copies:
            if which == a:
                copy.start()

    def prepare(origin):
        top = jnp.concatenate(high_low(w_all[origin]), axis=1)
        w_twice[origin] = jnp.concatenate([top, top], axis=0)

    prepare(me)
    own[4].wait()
    own[5].wait()
    group_i = (lax.broadcasted_iota(i32, (1, 128), 1) // GROUP) * KEYS

    for m in range(MICRO):
        for j in range(8):
            key_rows[m * 8 + j : m * 8 + j + 1, :] = keys[m : m + 1, j * 128 : (j + 1) * 128]

    def key_row_at(m, j):
        return key_rows[pl.ds(m * 8 + j, 1), :]

    def sameness(i, carry):
        for u in range(4):
            key_row = key_row_at(i // 2, (i % 2) * 4 + u) + group_i
            key_col = jnp.transpose(jnp.broadcast_to(key_row, (128, 128)))
            same[i * 4 + u] = jnp.where(key_col == key_row, 1.0, 0.0).astype(bf16)
        return carry

    lax.fori_loop(0, 8, sameness, 0)
    for which, copy in copies:
        if which == 0:
            copy.wait()
    for which, copy in copies:
        if which == 2:
            copy.wait()
    for n, k in ((1, 1), (2, 3), (0, 2)):
        copies[3 * n + 1][1].wait()
        prepare(lax.rem(me + 4 - k, 4))


def exchange(weight, bias, predicates, keys, valid):
    return pl.pallas_call(
        exchange_kernel,
        out_shape=(
            jax.ShapeDtypeStruct((4, 256, 256), bf16),
            jax.ShapeDtypeStruct((4, 1, D), f32),
            jax.ShapeDtypeStruct((32, 128, 128), bf16),
            jax.ShapeDtypeStruct((SECTIONS, MICRO, 32), i32),
            jax.ShapeDtypeStruct((1, MICRO), i32),
            jax.ShapeDtypeStruct((KEYS, D), f32),
            jax.ShapeDtypeStruct((KEYS, D), f32),
            jax.ShapeDtypeStruct((32, 128), i32),
        ),
        in_specs=[spec(HB)] * 5,
        out_specs=(spec(VM),) * 8,
        scratch_shapes=[
            pltpu.VMEM((4, D, D), f32),
            pltpu.VMEM((MICRO, BLOCK), i32),
            pltpu.VMEM((4, 4, 32), i32),
            pltpu.SemaphoreType.DMA((3, 3)),
            pltpu.SemaphoreType.DMA((3, 3)),
            pltpu.SemaphoreType.DMA((6,)),
        ],
        compiler_params=pltpu.CompilerParams(collective_id=0, has_side_effects=True, vmem_limit_bytes=8 << 20),
        cost_estimate=pl.CostEstimate(flops=40_000_000_000, bytes_accessed=1 << 20, transcendentals=0),
    )(pinned(weight), pinned(bias), pinned(predicates), pinned(keys), pinned(valid))


def sections_kernel(
    rows, keys_in, w2, b, same, words, limits, clear_a, clear_b, v_in, table_a, table_b, lives, ready, keys, valid, sems
):
    fetch = [pltpu.make_async_copy(keys_in, keys, sems.at[0]), pltpu.make_async_copy(v_in, valid, sems.at[1])]
    for copy in fetch:
        copy.start()

    sub = lax.broadcasted_iota(i32, (8, 128), 0)
    lane = lax.broadcasted_iota(i32, (8, 128), 1)
    for m in range(MICRO):
        alive = jnp.where(sub * 128 + lane < limits[0:1, m : m + 1], 1, 0)
        found = jnp.zeros((8, 128), i32)
        for s in range(SECTIONS):
            line = jnp.concatenate([words[s, m : m + 1, :]] * 4, axis=1)
            word = jnp.take_along_axis(
                jnp.broadcast_to(line, (8, 128)), sub * 4 + (lane >> 5), axis=1, mode="promise_in_bounds")
            alive = alive & (word >> (lane & 31))
            found = found + alive
        lives[m * 8 : (m + 1) * 8, :] = found

    def compute(slot, tiles, used=BATCH):
        h = jnp.concatenate([rows[t // 8, pl.ds(pl.multiple_of((t % 8) * TILE, TILE), TILE), :] for t in tiles[:used]], axis=0)
        levels = jnp.concatenate([lives[pl.ds(t, 1), :] for t in tiles], axis=0)
        columns = jnp.transpose(jnp.concatenate([levels] * 16, axis=0))
        alive = jnp.concatenate([jnp.broadcast_to(columns[:, j : j + 1], (128, 128)) for j in range(used)], axis=0)
        total = jnp.zeros((used * TILE, D), f32)
        for s in range(SECTIONS):
            p = jnp.dot(jnp.concatenate(high_low(h), axis=1), w2[s], preferred_element_type=f32)
            h = h + jnp.tanh(p[:, :D] + (p[:, D:] + b[s]))
            total = total + jnp.where(alive > s, h, 0.0)
        both = jnp.concatenate(high_low(total), axis=1)
        for j, t in enumerate(tiles[:used]):
            p = jnp.dot(same[t], both[j * TILE : (j + 1) * TILE], preferred_element_type=f32)
            ready[pl.ds(pl.multiple_of((slot + j) * TILE, TILE), TILE), :] = p[:, :D] + p[:, D:]

    compute(0, [m * 8 + j for m in range(MICRO) for j in range(SURE // TILE)])
    for copy in fetch:
        copy.wait()
    ends = [0]
    for m in range(MICRO):
        ends.append(ends[-1] + (valid[0, m] - SURE + TILE - 1) // TILE)

    def tile_at(i):
        tile = SURE // TILE + i
        for m in range(1, MICRO):
            tile = jnp.where(i >= ends[m], m * 8 + SURE // TILE + i - ends[m], tile)
        return jnp.minimum(tile, 31)

    def batch(n, carry):
        compute(BATCH + n * BATCH, [tile_at(n * BATCH + j) for j in range(BATCH)])
        return carry

    whole = (ends[MICRO] + BATCH // 2 - 1) // BATCH
    lax.fori_loop(0, whole, batch, 0)

    @pl.when(ends[MICRO] > whole * BATCH)
    def _():
        compute(BATCH + whole * BATCH, [tile_at(whole * BATCH + j) for j in range(BATCH)], BATCH // 2)

    tables = (table_a, table_b)

    def scatter(slot, *tiles):
        groups = len(tiles) * TILE // GROUP

        def load(g):
            at = [keys[tiles[g * GROUP // TILE], (g * GROUP + i) % TILE] for i in range(GROUP)]
            return at, [tables[g % 2][pl.ds(k, 1), :] for k in at]

        def store(g, at, held):
            for i, k in enumerate(at):
                tables[g % 2][pl.ds(k, 1), :] = held[i] + ready[pl.ds(slot * TILE + g * GROUP + i, 1), :]

        flying = {g: load(g) for g in range(2)}
        for g in range(groups):
            store(g, *flying.pop(g))
            if g + 2 < groups:
                flying[g + 2] = load(g + 2)

    def sure(m, carry):
        scatter(2 * m, 8 * m, 8 * m + 1)
        return carry

    def rest(i, carry):
        scatter(BATCH + 2 * i, tile_at(2 * i), tile_at(2 * i + 1))
        return carry

    lax.fori_loop(0, MICRO, sure, 0)
    lax.fori_loop(0, ends[MICRO] // 2, rest, 0)

    @pl.when(ends[MICRO] % 2 == 1)
    def _():
        scatter(BATCH + ends[MICRO] - 1, tile_at(ends[MICRO] - 1))


def sections(rows, keys, w, b, same, words, limits, clear_a, clear_b, valid):
    return pl.pallas_call(
        sections_kernel,
        out_shape=(jax.ShapeDtypeStruct((KEYS, D), f32),) * 2 + (jax.ShapeDtypeStruct((32, 128), i32),),
        in_specs=[spec(VM)] * 9 + [spec(HB)],
        out_specs=(spec(VM),) * 3,
        scratch_shapes=[
            pltpu.VMEM((ROWS, D), f32),
            pltpu.SMEM((32, 128), i32),
            pltpu.SMEM((1, MICRO), i32),
            pltpu.SemaphoreType.DMA((2,)),
        ],
        input_output_aliases={7: 0, 8: 1},
        compiler_params=pltpu.CompilerParams(vmem_limit_bytes=12 << 20),
    )(rows, keys, w, b, same, words, limits, clear_a, clear_b, pinned(valid))


ORDERS = ((0, 1, 2), (1, 2, 0), (2, 0, 1))
BAND, PART, COUNTED = 24, 8, 8
N = 9
HEIGHT = 72


def reduce_kernel(table_a, table_b, keys, lives, sums, pair, *scratch):
    held = scratch[0:3]
    near, middle, second, last, third = (scratch[3 + i * N : 3 + (i + 1) * N] for i in range(5))
    core_recv, core_send, near_sems, far_sems = scratch[3 + 5 * N :]
    z = lax.axis_index("section")
    row = lax.axis_index("rows")
    y, x, c = row // 8, (row // 2) % 4, row % 2
    place = (z, y, x)

    def position(axis, k):
        return lax.rem(place[axis] + k, 4)

    def device(axis, k):
        at = list(place)
        at[axis] = position(axis, k)
        return (at[0], at[1] * 8 + at[2] * 2 + c)

    other = (z, y * 8 + x * 2 + (1 - c))
    peers = [device(axis, k) for axis in range(3) for k in (1, 3)] + [other]
    barrier = pltpu.get_barrier_semaphore()
    for peer in peers:
        pl.semaphore_signal(barrier, inc=1, device_id=peer, device_id_type=MESH)

    def join(i, carry):
        at = (i // 4, i % 4, slice(None))
        pair[(*at, slice(0, 64))] = table_a[(*at, 1 - c)] + table_b[(*at, 1 - c)]
        return carry

    lax.fori_loop(0, 16, join, 0)
    pl.semaphore_wait(barrier, len(peers))

    def send(src, dst, send_sem, recv_sem, to):
        pltpu.make_async_remote_copy(
            src_ref=src, dst_ref=dst, send_sem=send_sem, recv_sem=recv_sem, device_id=to, device_id_type=MESH
        ).start()

    def wait(ref, sem):
        pltpu.make_async_copy(ref, ref, sem).wait()

    every = [0, 1, 2]

    def where_of(axes, axis, index, half=None):
        where = [slice(None)] * len(axes)
        where[axes.index(axis)] = index
        if half is not None:
            where[1 if axes[0] == axis else 0] = pl.ds(2 * half, 2)
        return tuple(where)

    def keyed(band):
        return BAND - COUNTED if band == 2 else BAND

    def swap(band, index, kind):
        at, size = where_of(every, ORDERS[band][0], index), keyed(band)
        send(
            pair.at[(*at, pl.ds(band * BAND, size))], held[band].at[(*at, pl.ds(0, size))],
            core_send.at[band], core_recv.at[band, kind], other)

    def swapped(band, kind, blocks):
        size = keyed(band)
        wait(held[band].at[0:blocks, :, :, pl.ds(0, size)], core_recv.at[band, kind])
        for k in {0: (2,), 1: (1, 3), 2: (0,)}[kind]:
            at = where_of(every, ORDERS[band][0], position(ORDERS[band][0], k))
            rows = (c, slice(band * BAND, band * BAND + size))
            held[band][(*at, slice(0, size))] += table_a[(*at, *rows)] + table_b[(*at, *rows)]

    for kind, steps in enumerate(((2,), (1, 3), (0,))):
        for band in range(3):
            for k in steps:
                swap(band, position(ORDERS[band][0], k), kind)
    sub64 = lax.broadcasted_iota(i32, (64, 128), 0)
    sub128 = lax.broadcasted_iota(i32, (128, 128), 0)

    def tally(i, found):
        for u in range(4):
            key_row = keys[pl.ds(i * 4 + u, 1), :]
            alive = lives[pl.ds(i * 4 + u, 1), :].astype(f32)
            high = jnp.where((key_row >> 7) == sub64, alive, 0.0).astype(bf16)
            low = jnp.where((key_row & 127) == sub128, 1.0, 0.0).astype(bf16)
            found = found + lax.dot_general(high, low, (((1,), (1,)), ((), ())), preferred_element_type=f32)
        return found

    found = lax.fori_loop(0, 8, tally, jnp.zeros((64, 128), f32))
    for i in range(64):
        pair[i // 16, (i // 4) % 4, i % 4, 64:72, :] = jnp.broadcast_to(found[i : i + 1], (8, 128))
    counted = held[2].at[:, :, :, pl.ds(BAND - COUNTED, COUNTED)]
    send(pair.at[:, :, :, pl.ds(64, COUNTED)], counted, core_send.at[2], core_recv.at[3, 0], other)

    def block_of(n, k, half):
        band, step = n % 3, n // 3
        axis = ORDERS[band][0]
        return held[band].at[(*where_of(every, axis, position(axis, k), half), pl.ds(step * PART, PART))]

    def hop(n, slot, recv, block, k):
        send(block, near[n].at[slot], near_sems.at[n, 3], near_sems.at[n, recv], device(ORDERS[n % 3][0], k))

    def relay(n):
        hop(n, 0, 0, block_of(n, 2, 0), 1)
        hop(n, 1, 1, block_of(n, 2, 1), 3)

    def direct(n):
        hop(n, 2, 2, block_of(n, 1, 1), 1)
        hop(n, 3, 2, block_of(n, 3, 0), 3)

    for band in range(3):
        swapped(band, 0, 1)
        for n in range(band, N - 1 if band == 2 else N, 3):
            relay(n)
    for band in range(3):
        swapped(band, 1, 2)
        for n in range(band, N - 1 if band == 2 else N, 3):
            direct(n)
    wait(counted, core_recv.at[3, 0])
    for i in range(4):
        held[2][i, :, :, BAND - COUNTED :] += pair[i, :, :, 64:72]
    relay(N - 1)
    direct(N - 1)

    def spread(n, stage, source, axes, target):
        axis = ORDERS[n % 3][stage]
        for k in (2, 1, 3):
            send(
                source.at[where_of(axes, axis, position(axis, k))], target.at[k - 1],
                far_sems.at[n, stage - 1, 0], far_sems.at[n, stage - 1, 1], device(axis, k))

    def summed(n, stage, source, axes, target):
        axis = ORDERS[n % 3][stage]
        wait(target, far_sems.at[n, stage - 1, 1])
        return (source[where_of(axes, axis, place[axis])] + target[0]) + (target[1] + target[2])

    for n in range(N):
        if n == 6:
            for band in range(3):
                swapped(band, 2, 1)
        for half, k in ((0, 1), (1, 3)):
            wait(near[n].at[half], near_sems.at[n, half])
            block = block_of(n, k, half)
            block[...] += near[n][half]
            hop(n, 4 + half, 2, block, k)
    for n in range(N):
        axis = ORDERS[n % 3][0]
        wait(near[n].at[2:6], near_sems.at[n, 2])
        middle[n][0:2] = (block_of(n, 0, 0)[...] + near[n][3]) + near[n][4]
        middle[n][2:4] = (block_of(n, 0, 1)[...] + near[n][2]) + near[n][5]
        spread(n, 1, middle[n], [i for i in every if i != axis], second[n])
    for n in range(N):
        axis = ORDERS[n % 3][0]
        last[n][...] = summed(n, 1, middle[n], [i for i in every if i != axis], second[n])
        spread(n, 2, last[n], [ORDERS[n % 3][2]], third[n])
    for n in range(N):
        start = (n % 3) * BAND + (n // 3) * PART
        sums[start : start + PART, :] = summed(n, 2, last[n], [ORDERS[n % 3][2]], third[n])
    for band in range(3):
        wait(held[band], core_send.at[band])
    for n in range(N):
        wait(near[n], near_sems.at[n, 3])
        wait(second[n], far_sems.at[n, 0, 0])
        wait(third[n], far_sems.at[n, 1, 0])


def reduce_to_owner(table_a, table_b, keys, lives):
    buffers = [pltpu.VMEM((4, 4, 4, HEIGHT, D), f32)] + [pltpu.VMEM((4, 4, 4, BAND, D), f32)] * 3
    for lead in ((6, 2, 4), (4, 4), (3, 4), (4,), (3,)):
        buffers += [pltpu.VMEM((*lead, PART, D), f32)] * N
    return pl.pallas_call(
        reduce_kernel,
        out_shape=jax.ShapeDtypeStruct((HEIGHT, D), f32),
        in_specs=[spec(VM)] * 4,
        out_specs=spec(VM),
        scratch_shapes=buffers + [
            pltpu.SemaphoreType.DMA((4, 3)),
            pltpu.SemaphoreType.DMA((3,)),
            pltpu.SemaphoreType.DMA((N, 4)),
            pltpu.SemaphoreType.DMA((N, 2, 2)),
        ],
        compiler_params=pltpu.CompilerParams(collective_id=1, has_side_effects=True, vmem_limit_bytes=20 << 20),
    )(table_a.reshape(4, 4, 4, 2, 64, D), table_b.reshape(4, 4, 4, 2, 64, D), keys, lives)


def means_kernel(sums, means, counts):
    c = lax.axis_index("rows") % 2
    line = sums[64:65, :]
    wide = jnp.transpose(jnp.broadcast_to(line, (128, 128)))
    means[...] = sums[:64] / jnp.maximum(jnp.where(c == 0, wide[:64], wide[64:]), 1.0)
    counts[...] = jnp.where(c == 0, line, pltpu.roll(line, 64, 1))[:, :64]


def means_of(sums):
    return pl.pallas_call(
        means_kernel,
        out_shape=(jax.ShapeDtypeStruct((64, D), f32), jax.ShapeDtypeStruct((1, 64), f32)),
        in_specs=[spec(VM)],
        out_specs=(spec(VM), spec(VM)),
        compiler_params=pltpu.CompilerParams(vmem_limit_bytes=1 << 20),
    )(sums)


def shards(rows_data, row_keys, valid_counts, predicates, section_weight, section_bias):
    w, b, same, words, limits, clear_a, clear_b, key_rows = exchange(
        section_weight, section_bias.reshape(1, 1, D), predicates.reshape(4, MICRO, 32), row_keys, valid_counts.T)
    table_a, table_b, lives = sections(
        rows_data, key_rows, w, b, same, words, limits, clear_a, clear_b, valid_counts.T)
    means, counts = means_of(reduce_to_owner(table_a, table_b, key_rows, lives))
    return means, counts.reshape(64)


def solution(mesh):
    placed = (
        P("section", "rows", None),
        P("section", "rows"),
        P("section", "rows"),
        P("section", None, "rows"),
        P("section", None, None),
        P("section", None),
    )
    return jax.shard_map(
        shards,
        mesh=mesh,
        in_specs=placed,
        out_specs=(P(("section", "rows"), None), P(("section", "rows"))),
        check_vma=False,
    )
```
